128 devices in a mesh: row: 2 (over x_lo), col: 4 (over y), layer: 16 (over z, x_hi, core).
Axes of the slice: x: 4 (x_hi: 2, x_lo: 2; x = x_hi * 2 + x_lo), y: 4, z: 4, core: 2. Of those that a mesh axis runs over, the one named last changes fastest.
Arguments:
- object_field: float32 [2, 512, 1024], P(None, 'row', 'col'), may hold values from -6 to 6
- probe_modes: float32 [2, 4, 256, 256], replicated, may hold values from -6 to 6
- amplitudes: float32 [128, 256, 256], P(('row', 'col', 'layer')), may hold values from 0 to 4
- offsets: int32 [128, 2], P(('row', 'col', 'layer')), may hold values from 0 to 768, as said below
Outputs:
- new_object: float32 [2, 512, 1024], P(None, 'row', 'col')
The draws below stay inside these ranges and needn't reach their ends.
Inputs may be any that keep to these rules, and one draw needn't show every extreme that they name: `offsets`: every patch lies inside the 512 x 1024 object. A position held by the device at tile (r, c) has its corner inside that tile: rows r * 256 to (r + 1) * 256 - 1 and columns c * 256 to (c + 1) * 256 - 1. On a device whose tile row is not the last, its first position's patch reaches into the next tile row.
All inputs are finite; a program needn't handle non-finite values.
Results may differ from the reference program's by a relative error of at most 0.0001.
Values sent between devices are 32-bit elements; how exact they have to be, the bound alone decides.
A program may use at most 64 MiB of HBM per device.

```python
import jax
import jax.numpy as jnp
from jax import lax

PATCH = 256
MODES = 4
TILE_R = 256
TILE_C = 256
POS_DEV = 1
OBJ_R = 512
OBJ_C = 1024
POSITIONS = 128
N_ROW = 2
N_COL = 4
N_LAYER = 16


def draw_offsets(key, part):
    index = jnp.arange(POSITIONS, dtype=jnp.int32)
    device = index // POS_DEV
    slot = index % POS_DEV
    tile_row = device // (N_COL * N_LAYER)
    tile_col = device // N_LAYER % N_COL
    key_rows, key_cols = jax.random.split(jax.random.fold_in(key, 17))
    rows_high = jnp.where(tile_row == N_ROW - 1, TILE_R - PATCH + 1, TILE_R)
    rows_low = jnp.where((slot == 0) & (tile_row < N_ROW - 1), TILE_R - PATCH + 1, 0)
    draw_rows = jax.random.randint(key_rows, (POSITIONS,), 0, 1 << 30, dtype=jnp.int32)
    local_rows = rows_low + draw_rows % (rows_high - rows_low)
    cols_high = jnp.where(tile_col == N_COL - 1, TILE_C - PATCH + 1, TILE_C)
    draw_cols = jax.random.randint(key_cols, (POSITIONS,), 0, 1 << 30, dtype=jnp.int32)
    local_cols = draw_cols % cols_high
    return jnp.stack([tile_row * TILE_R + local_rows, tile_col * TILE_C + local_cols], axis=-1).astype(jnp.int32)


def steps_of(stream_key, shape, cuts, low, top_value):
    level = 1.0
    for axis_at, parts in cuts:
        draws = jax.random.uniform(jax.random.fold_in(jax.random.fold_in(stream_key, 6), axis_at), (parts,), jnp.float32, low / len(cuts), top_value / len(cuts))
        level = level * jnp.repeat(jnp.exp(draws), shape[axis_at] // parts).reshape((-1,) + (1,) * (len(shape) - 1 - axis_at))
    return level


def centred(rng, shape, spread, most, shards=(), kind=jnp.bfloat16):
    entries = jax.random.normal(rng, shape, jnp.float32) * spread
    if len(shards) > 0:
        entries = steps_of(rng, shape, shards, -0.22, 0.18) * entries
    return jnp.clip(entries, min=-most, max=most).astype(kind)


def setup_inputs(seed: int = 0) -> dict:
    seeds = jax.random.split(jax.random.key(seed), 5)
    return {
        "object_field": centred(seeds[0], (2, OBJ_R, OBJ_C), 1.0, 6.0, ((1, 2), (2, 4)), jnp.float32),
        "probe_modes": centred(seeds[1], (2, MODES, PATCH, PATCH), 1.0, 6.0, (), jnp.float32),
        "amplitudes": jnp.clip(4.0 * jax.random.uniform(seeds[2], (POSITIONS, PATCH, PATCH), jnp.float32) ** steps_of(seeds[2], (POSITIONS, PATCH, PATCH), ((0, 128),), -0.2, 0.2), 0.0, 4.0),
        "offsets": draw_offsets(jax.random.fold_in(seeds[4], 71), 0),
    }


SOFTEN = 0.05
DAMPING = 0.5

def reference(object_field, probe_modes, amplitudes, offsets):
    probe = lax.complex(probe_modes[0], probe_modes[1])
    power = lax.optimization_barrier(jnp.sum(probe_modes[0] * probe_modes[0] + probe_modes[1] * probe_modes[1], axis=0))
    zero_index = jnp.int32(0)

    def one_position(index, carry):
        numer, denom = carry
        row_at = offsets[index, 0].astype(jnp.int32)
        col_at = offsets[index, 1].astype(jnp.int32)
        patch = lax.dynamic_slice(object_field, (zero_index, row_at, col_at), (2, PATCH, PATCH))
        exit_wave = probe * lax.complex(patch[0], patch[1])[None]
        far = jnp.fft.fft2(exit_wave, norm='ortho')
        intensity = lax.optimization_barrier(jnp.sum(far.real * far.real + far.imag * far.imag, axis=0))
        ratio = amplitudes[index] / (jnp.sqrt(intensity) + SOFTEN)
        revised = jnp.fft.ifft2(far * ratio[None], norm='ortho')
        contrib = lax.optimization_barrier(jnp.sum(jnp.conj(probe) * revised, axis=0))
        block = jnp.stack([contrib.real, contrib.imag])
        old_block = lax.dynamic_slice(numer, (zero_index, row_at, col_at), (2, PATCH, PATCH))
        numer = lax.dynamic_update_slice(numer, old_block + block, (zero_index, row_at, col_at))
        old_power = lax.dynamic_slice(denom, (row_at, col_at), (PATCH, PATCH))
        denom = lax.dynamic_update_slice(denom, old_power + power, (row_at, col_at))
        return (numer, denom)
    numer0 = jnp.zeros(object_field.shape, jnp.float32)
    denom0 = jnp.zeros(object_field.shape[1:], jnp.float32)
    numer, denom = lax.fori_loop(0, POSITIONS, one_position, (numer0, denom0))
    return (numer + DAMPING * object_field) / (denom + DAMPING)[None]
```

```python
import functools
import math

import jax
import jax.numpy as jnp
import numpy as np
from jax import lax
from jax.experimental import pallas as pl
from jax.experimental.pallas import tpu as pltpu
from jax.sharding import PartitionSpec as P

SOFTEN = 0.05
DAMPING = 0.5
MODES = 4
SIDE = 256
HALF = 128
QUART = 64
F32 = jnp.float32
BF16 = jnp.bfloat16
VMEM_SPEC = pl.BlockSpec(memory_space=pltpu.VMEM)
SMEM_SPEC = pl.BlockSpec(memory_space=pltpu.SMEM)
ANY_SPEC = pl.BlockSpec(memory_space=pl.ANY)


def remote(src, dst, send, recv, device):
    return pltpu.make_async_remote_copy(
        src_ref=src,
        dst_ref=dst,
        send_sem=send,
        recv_sem=recv,
        device_id=device,
        device_id_type=pl.DeviceIdType.MESH,
    )


class Place:
    def __init__(self):
        self.row = lax.axis_index("row")
        self.col = lax.axis_index("col")
        layer = lax.axis_index("layer")
        self.layer = layer
        self.z = layer // 4
        self.xh = (layer // 2) % 2
        self.core = layer % 2
        self.partner = self.at(xh=self.xh, core=1 - self.core)
        self.far_x = self.at(xh=1 - self.xh)
        self.cross_xh = (self.xh + self.core) % 2
        self.cross = {"row": 1 - self.row, "layer": self.z * 4 + self.cross_xh * 2 + self.core}
        self.left = {"col": (self.col + 3) % 4}
        self.right = {"col": (self.col + 1) % 4}

    def at(self, z=None, xh=None, core=None):
        z = self.z if z is None else z
        xh = self.xh if xh is None else xh
        core = self.core if core is None else core
        return {"layer": z * 4 + xh * 2 + core}

    def z_peer(self, step):
        return self.at(z=(self.z + step) % 4)

    def meet(self):
        barrier = pltpu.get_barrier_semaphore()
        others = [self.partner, self.far_x, self.cross, self.left, self.right]
        others += [self.z_peer(step) for step in (1, 2, 3)]
        for other in others:
            pl.semaphore_signal(barrier, inc=1, device_id=other, device_id_type=pl.DeviceIdType.MESH)
        pl.semaphore_wait(barrier, len(others))


def rows_of(part, base=0):
    return pl.ds(pl.multiple_of(base + part * QUART, QUART), QUART)


def halo_kernel(
    offsets, obj, ext, spots,
    local_sem, right_send, right_recv, low_send, low_recv, diag_send, diag_recv,
    pair_send, pair_recv, spot_send, spot_recv,
):
    me = Place()
    core = me.core
    loads = []
    for plane in range(2):
        load = pltpu.make_async_copy(obj.at[plane], ext.at[0, plane, pl.ds(0, SIDE)], local_sem.at[plane])
        load.start()
        loads.append(load)
    lanes = lax.broadcasted_iota(jnp.int32, (1, 1, 128), 2)
    line = jnp.where(lanes == 0, offsets[0, 0], jnp.where(lanes == 1, offsets[0, 1], 0))
    spots[pl.ds(me.layer, 1)] = line
    me.meet()
    for load in loads:
        load.wait()

    has_right = me.col < 3
    has_left = me.col > 0
    top = me.row == 0
    bottom = me.row == 1

    def right_copy(part):
        return remote(ext.at[0, core, rows_of(part)], ext.at[1, core, rows_of(part)],
                      right_send.at[part], right_recv.at[part], me.left)

    def low_copy(part):
        return remote(ext.at[0, core, rows_of(part)], ext.at[0, core, rows_of(part, SIDE)],
                      low_send.at[part], low_recv.at[part], me.cross)

    def diag_copy(part):
        return remote(ext.at[1, core, rows_of(part)], ext.at[1, core, rows_of(part, SIDE)],
                      diag_send.at[part], diag_recv.at[part], me.cross)

    def pair_copy(kind, part):
        side, base = ((1, 0), (0, SIDE), (1, SIDE))[kind]
        where = ext.at[side, core, rows_of(part, base)]
        return remote(where, where, pair_send.at[kind, part], pair_recv.at[kind, part], me.partner)

    @pl.when(has_left)
    def _():
        for part in range(4):
            right_copy(part).start()

    @pl.when(bottom)
    def _():
        for part in range(4):
            low_copy(part).start()

    def spot_copy(step):
        if step == 0:
            where = pl.ds(me.layer, 1)
            return remote(spots.at[where], spots.at[where], spot_send.at[0], spot_recv.at[0], me.partner)
        if step == 1:
            where = pl.ds(me.z * 4 + me.xh * 2, 2)
            return remote(spots.at[where], spots.at[where], spot_send.at[1], spot_recv.at[1], me.far_x)
        if step < 5:
            where = pl.ds(me.z * 4, 4)
            return remote(spots.at[where], spots.at[where], spot_send.at[step], spot_recv.at[step],
                          me.z_peer(step - 1))
        if step == 5:
            return remote(spots.at[pl.ds(0, 16)], spots.at[pl.ds(16, 16)], spot_send.at[5], spot_recv.at[5], me.right)
        return remote(spots.at[pl.ds(0, 32)], spots.at[pl.ds(32, 32)], spot_send.at[6], spot_recv.at[6], me.cross)

    def spots_go(stage):
        if stage == 0:
            spot_copy(0).start()
        elif stage == 1:
            spot_copy(0).wait_recv()
            spot_copy(1).start()
        elif stage == 2:
            spot_copy(1).wait_recv()
            for step in (2, 3, 4):
                spot_copy(step).start()
        elif stage == 3:
            for step in (2, 3, 4):
                spot_copy(step).wait_recv()

            @pl.when(has_right)
            def _():
                spot_copy(5).start()
        elif stage == 4:
            @pl.when(has_left)
            def _():
                spot_copy(5).wait_recv()

            @pl.when(top)
            def _():
                spot_copy(6).start()
        else:
            @pl.when(bottom)
            def _():
                spot_copy(6).wait_recv()

    spots_go(0)
    for part in range(4):
        @pl.when(has_right)
        def _():
            right_copy(part).wait_recv()

            @pl.when(bottom)
            def _():
                diag_copy(part).start()

            pair_copy(0, part).start()

        @pl.when(top)
        def _():
            low_copy(part).wait_recv()
            pair_copy(1, part).start()

        spots_go(part + 1)

    @pl.when(jnp.logical_and(top, has_right))
    def _():
        for part in range(4):
            diag_copy(part).wait_recv()
            pair_copy(2, part).start()

    spots_go(5)

    @pl.when(has_left)
    def _():
        for part in range(4):
            right_copy(part).wait_send()

    @pl.when(bottom)
    def _():
        for part in range(4):
            low_copy(part).wait_send()

            @pl.when(has_right)
            def _():
                diag_copy(part).wait_send()

    @pl.when(has_right)
    def _():
        for part in range(4):
            pair_copy(0, part).wait_send()
            other_pair(ext, pair_send, pair_recv, me, 0, part).wait_recv()

    @pl.when(top)
    def _():
        for part in range(4):
            pair_copy(1, part).wait_send()
            other_pair(ext, pair_send, pair_recv, me, 1, part).wait_recv()

            @pl.when(has_right)
            def _():
                pair_copy(2, part).wait_send()
                other_pair(ext, pair_send, pair_recv, me, 2, part).wait_recv()

    for step in range(5):
        spot_copy(step).wait_send()

    @pl.when(has_right)
    def _():
        spot_copy(5).wait_send()

    @pl.when(top)
    def _():
        spot_copy(6).wait_send()


def other_pair(ext, pair_send, pair_recv, me, kind, part):
    side, base = ((1, 0), (0, SIDE), (1, SIDE))[kind]
    where = ext.at[side, 1 - me.core, rows_of(part, base)]
    return remote(where, where, pair_send.at[kind, part], pair_recv.at[kind, part], me.partner)


def halo(offsets, obj):
    sems = pltpu.SemaphoreType.DMA
    return pl.pallas_call(
        halo_kernel,
        out_shape=(
            jax.ShapeDtypeStruct((2, 2, 2 * SIDE, SIDE), F32),
            jax.ShapeDtypeStruct((64, 1, 128), jnp.int32),
        ),
        in_specs=[SMEM_SPEC, ANY_SPEC],
        out_specs=(VMEM_SPEC, VMEM_SPEC),
        scratch_shapes=[
            sems((2,)), sems((4,)), sems((4,)), sems((4,)), sems((4,)), sems((4,)), sems((4,)),
            sems((3, 4)), sems((3, 4)), sems((7,)), sems((7,)),
        ],
        compiler_params=pltpu.CompilerParams(collective_id=0, has_side_effects=True),
        name="halo",
    )(offsets, obj)


def tables():
    steps = np.arange(HALF)
    found = []
    for odd in (0, 1):
        phase = (steps[:, None] * (2 * steps[None, :] + odd)) % SIDE
        angle = phase * (2.0 * math.pi / SIDE)
        real, imag = np.cos(angle) / 16.0, -np.sin(angle) / 16.0
        full = np.block([[real, imag], [-imag, real]]).astype(np.float32)
        for table in (full, np.ascontiguousarray(full.T)):
            high = table.astype(jnp.bfloat16)
            low = (table - high.astype(np.float32)).astype(jnp.bfloat16)
            found += [high, low]
    order = np.zeros((SIDE, SIDE), np.float32)
    order[2 * steps, steps] = 1.0
    order[2 * steps + 1, HALF + steps] = 1.0
    found += [order.astype(jnp.bfloat16), np.ascontiguousarray(order.T).astype(jnp.bfloat16)]
    return np.stack(found)


EVEN, EVEN_T, ODD, ODD_T, ORDER, ORDER_T = 0, 2, 4, 6, 8, 9


def dot(left, right):
    return jnp.dot(left, right, preferred_element_type=F32)


def split(value):
    high = value.astype(BF16)
    return high, (value - high.astype(F32)).astype(BF16)


def on_lanes(value, tabs, which):
    high, low = split(value)
    return dot(high, tabs[which]) + dot(low, tabs[which]) + dot(high, tabs[which + 1])


def on_rows(value, tabs, which):
    high, low = split(value)
    return dot(tabs[which], high) + dot(tabs[which], low) + dot(tabs[which + 1], high)


def side_by_side(left, right):
    return jnp.concatenate([left, right], axis=1)


def on_top(upper, lower):
    return jnp.concatenate([upper, lower], axis=0)


def forward(mode, probe, patch, tabs, far):
    pr, pi = probe[0, mode], probe[1, mode]
    tr, ti = patch[0], patch[1]
    er = pr * tr - pi * ti
    ei = pr * ti + pi * tr
    even = side_by_side(er[:, :HALF] + er[:, HALF:], ei[:, :HALF] + ei[:, HALF:])
    odd = side_by_side(er[:, :HALF] - er[:, HALF:], ei[:, :HALF] - ei[:, HALF:])
    ye = on_lanes(even, tabs, EVEN)
    yo = on_lanes(odd, tabs, ODD)
    for parity, which in ((0, EVEN_T), (1, ODD_T)):
        if parity == 0:
            se, so = ye[:HALF] + ye[HALF:], yo[:HALF] + yo[HALF:]
        else:
            se, so = ye[:HALF] - ye[HALF:], yo[:HALF] - yo[HALF:]
        stack = on_top(side_by_side(se[:, :HALF], so[:, :HALF]), side_by_side(se[:, HALF:], so[:, HALF:]))
        far[mode, parity] = on_rows(stack, tabs, which)


def backward(mode, probe, ratio, tabs, far, block):
    sums = []
    for parity, which in ((0, EVEN), (1, ODD)):
        scale = ratio[parity]
        sums.append(on_rows(far[mode, parity] * on_top(scale, scale), tabs, which))
    upper, lower = sums[0] + sums[1], sums[0] - sums[1]
    even = on_top(side_by_side(upper[:HALF, :HALF], upper[HALF:, :HALF]),
                  side_by_side(lower[:HALF, :HALF], lower[HALF:, :HALF]))
    odd = on_top(side_by_side(upper[:HALF, HALF:], upper[HALF:, HALF:]),
                 side_by_side(lower[:HALF, HALF:], lower[HALF:, HALF:]))
    pe = on_lanes(even, tabs, EVEN_T)
    po = on_lanes(odd, tabs, ODD_T)
    first, second = pe + po, pe - po
    nr = side_by_side(first[:, :HALF], second[:, :HALF])
    ni = side_by_side(first[:, HALF:], second[:, HALF:])
    pr, pi = probe[0, mode], probe[1, mode]
    cr = pr * nr + pi * ni
    ci = pr * ni - pi * nr
    if mode == 0:
        block[0] = cr
        block[1] = ci
    else:
        block[0] = block[0] + cr
        block[1] = block[1] + ci


def rows_from(ref, start, count):
    near = pl.multiple_of(start // 8 * 8, 8)
    wide = ref[pl.ds(near, count + 8), :]
    return pltpu.roll(wide, lax.rem(count + 8 - (start - near), count + 8), 0)[:count]


def local_kernel(
    place, offsets, spots, ext, probe, amp, tabs, frame, share, patch, far, ratio, block, padded
):
    row, col, z = place[0], place[1], place[2]
    row_at = offsets[0, 0] - row * SIDE
    col_at = offsets[0, 1] - col * SIDE
    lanes = lax.broadcasted_iota(jnp.int32, (SIDE, SIDE), 1)
    back = lax.rem(SIDE - col_at, SIDE)
    for plane in range(2):
        here = pltpu.roll(rows_from(ext.at[0, plane], row_at, SIDE), back, 1)
        there = pltpu.roll(rows_from(ext.at[1, plane], row_at, SIDE), back, 1)
        patch[plane] = jnp.where(lanes < SIDE - col_at, here, there)

    rest = amp[...]
    total = None
    for _ in range(3):
        piece = rest.astype(BF16)
        rest = rest - piece.astype(F32)
        moved = dot(dot(tabs[ORDER_T], piece).astype(BF16), tabs[ORDER])
        total = moved if total is None else total + moved
    ratio[0] = total[:HALF]
    ratio[1] = total[HALF:]

    for mode in range(MODES):
        forward(mode, probe, patch, tabs, far)
    for parity in range(2):
        seen = None
        for mode in range(MODES):
            re, im = far[mode, parity, :HALF], far[mode, parity, HALF:]
            term = re * re + im * im
            seen = term if seen is None else seen + term
        ratio[parity] = ratio[parity] / (jnp.sqrt(seen) + SOFTEN)
    for mode in range(MODES):
        backward(mode, probe, ratio, tabs, far, block)

    frame[...] = jnp.zeros_like(frame)
    for plane in range(2):
        turned = pltpu.roll(block[plane], col_at, 1)
        near = pl.multiple_of(row_at // 8 * 8, 8)
        for side, kept in ((0, lanes >= col_at), (1, lanes < col_at)):
            value = on_top(jnp.where(kept, turned, 0.0), jnp.zeros((8, SIDE), F32))
            frame[side, plane, pl.ds(near, SIDE + 8), :] = pltpu.roll(value, row_at - near, 0)

    padded[...] = jnp.zeros_like(padded)
    power = None
    for mode in range(MODES):
        term = probe[0, mode] * probe[0, mode] + probe[1, mode] * probe[1, mode]
        power = term if power is None else power + term
    padded[pl.ds(SIDE, SIDE), :] = power
    share[...] = jnp.zeros_like(share)
    first = row * SIDE + z * QUART
    narrow = lax.broadcasted_iota(jnp.int32, (QUART, SIDE), 1)

    def add_spot(index, carry):
        up = index // 32
        left = (index // 16) % 2
        known = jnp.logical_and(row >= up, col >= left)
        spot_row = spots[index, 0, 0]
        spot_col = spots[index, 0, 1] - (col - left) * SIDE
        start = jnp.where(known, first - spot_row + SIDE, 0)
        turn = jnp.where(known, spot_col, 0)
        turned = pltpu.roll(rows_from(padded, start, QUART), turn, 1)
        kept = jnp.where(left == 0, narrow, SIDE - 1 - narrow) >= jnp.where(left == 0, turn, SIDE - turn)
        share[...] = share[...] + jnp.where(kept, turned, 0.0)
        return carry

    lax.fori_loop(0, 64, add_spot, 0)


def local_work(place, offsets, spots, ext, probe, amp, tabs):
    return pl.pallas_call(
        local_kernel,
        out_shape=(
            jax.ShapeDtypeStruct((2, 2, 2 * SIDE, SIDE), F32),
            jax.ShapeDtypeStruct((QUART, SIDE), F32),
        ),
        in_specs=[SMEM_SPEC, SMEM_SPEC, SMEM_SPEC, VMEM_SPEC, VMEM_SPEC, VMEM_SPEC, VMEM_SPEC],
        out_specs=(VMEM_SPEC, VMEM_SPEC),
        scratch_shapes=[
            pltpu.VMEM((2, SIDE, SIDE), F32),
            pltpu.VMEM((MODES, 2, SIDE, SIDE), F32),
            pltpu.VMEM((2, HALF, SIDE), F32),
            pltpu.VMEM((2, SIDE, SIDE), F32),
            pltpu.VMEM((3 * SIDE, SIDE), F32),
        ],
        compiler_params=pltpu.CompilerParams(),
        name="local",
    )(place, offsets, spots, ext, probe, amp, tabs)


def gather_kernel(
    frame, share, obj, out,
    pair, low_sum, low_in, right_sum, right_in, total, z_in, x_out, x_in,
    pair_send, pair_recv, low_send, low_recv, right_send, right_recv,
    z_send, z_recv, x_send, x_recv, out_send, out_recv, twin_send, twin_recv,
):
    me = Place()
    core = me.core
    has_right = me.col < 3
    has_left = me.col > 0
    top = me.row == 0
    bottom = me.row == 1
    parts = [(me.z + 1 + step) % 4 for step in range(4)]

    def pair_copy(kind, step):
        where = rows_of(parts[step], SIDE * kind)
        return remote(frame.at[:, 1 - core, where], pair.at[:, where],
                      pair_send.at[kind, step], pair_recv.at[kind, step], me.partner)

    def low_copy(step):
        where = rows_of(parts[step])
        return remote(low_sum.at[:, where], low_in.at[:, where], low_send.at[step], low_recv.at[step], me.cross)

    def right_copy(step):
        where = rows_of(parts[step])
        return remote(right_sum.at[where], right_in.at[where], right_send.at[step], right_recv.at[step], me.right)

    def z_copy(step):
        return remote(total.at[rows_of(parts[step])], z_in.at[step], z_send.at[step], z_recv.at[step],
                      me.z_peer(step + 1))

    me.meet()
    for step in range(4):
        @pl.when(top)
        def _():
            pair_copy(1, step).start()

        pair_copy(0, step).start()

    for step in range(4):
        where = rows_of(parts[step])
        under = rows_of(parts[step], SIDE)

        @pl.when(top)
        def _():
            pair_copy(1, step).wait_recv()
            for side in range(2):
                low_sum[side, where] = frame[side, core, under] + pair[side, under]
            low_copy(step).start()

        pair_copy(0, step).wait_recv()
        total[where] = frame[0, core, where] + pair[0, where]
        right_sum[where] = frame[1, core, where] + pair[1, where]

        @pl.when(bottom)
        def _():
            low_copy(step).wait_recv()
            total[where] = total[where] + low_in[0, where]
            right_sum[where] = right_sum[where] + low_in[1, where]

        @pl.when(has_right)
        def _():
            right_copy(step).start()

    for step in range(4):
        where = rows_of(parts[step])

        @pl.when(has_left)
        def _():
            right_copy(step).wait_recv()
            total[where] = total[where] + right_in[where]

        if step < 3:
            z_copy(step).start()

    mine = rows_of(me.z)
    for step in range(3):
        z_copy(step).wait_recv()
    x_out[...] = total[mine] + z_in[0] + z_in[1] + z_in[2]
    x_copy = remote(x_out, x_in, x_send.at[0], x_recv.at[0], me.far_x)
    x_copy.start()
    x_copy.wait_recv()
    whole = x_out[...] + x_in[...]
    out[core, mine] = (whole + DAMPING * obj[core, mine]) / (share[...] + DAMPING)

    def out_copy(step):
        return remote(out.at[core, mine], out.at[core, mine], out_send.at[step], out_recv.at[step], me.z_peer(step + 1))

    def come_copy(step):
        where = out.at[core, rows_of((me.z + 3 - step) % 4)]
        return remote(where, where, out_send.at[step], out_recv.at[step], me.z_peer(step + 1))

    def twin_copy(step, plane):
        part = me.z if step == 3 else (me.z + 3 - step) % 4
        where = out.at[plane, rows_of(part)]
        return remote(where, where, twin_send.at[step], twin_recv.at[step], me.partner)

    for step in (1, 0, 2):
        out_copy(step).start()
    twin_copy(3, core).start()
    for step in (0, 2, 1):
        come_copy(step).wait_recv()
        twin_copy(step, core).start()
    for step in (3, 0, 2, 1):
        twin_copy(step, 1 - core).wait_recv()

    for step in range(4):
        pair_copy(0, step).wait_send()
        twin_copy(step, core).wait_send()

        @pl.when(top)
        def _():
            pair_copy(1, step).wait_send()
            low_copy(step).wait_send()

        @pl.when(has_right)
        def _():
            right_copy(step).wait_send()

        if step < 3:
            z_copy(step).wait_send()
            out_copy(step).wait_send()
    x_copy.wait_send()


def gather(frame, share, obj):
    sems = pltpu.SemaphoreType.DMA
    return pl.pallas_call(
        gather_kernel,
        out_shape=jax.ShapeDtypeStruct((2, SIDE, SIDE), F32),
        in_specs=[VMEM_SPEC] * 3,
        out_specs=VMEM_SPEC,
        scratch_shapes=[
            pltpu.VMEM((2, 2 * SIDE, SIDE), F32),
            pltpu.VMEM((2, SIDE, SIDE), F32),
            pltpu.VMEM((2, SIDE, SIDE), F32),
            pltpu.VMEM((SIDE, SIDE), F32),
            pltpu.VMEM((SIDE, SIDE), F32),
            pltpu.VMEM((SIDE, SIDE), F32),
            pltpu.VMEM((3, QUART, SIDE), F32),
            pltpu.VMEM((QUART, SIDE), F32),
            pltpu.VMEM((QUART, SIDE), F32),
            sems((2, 4)), sems((2, 4)), sems((4,)), sems((4,)), sems((4,)), sems((4,)),
            sems((3,)), sems((3,)), sems((1,)), sems((1,)), sems((3,)), sems((3,)), sems((4,)), sems((4,)),
        ],
        compiler_params=pltpu.CompilerParams(collective_id=1, has_side_effects=True),
        name="gather",
    )(frame, share, obj)


def body(object_field, probe_modes, amplitudes, offsets):
    ext, spots = halo(offsets, object_field)
    place = jnp.stack([lax.axis_index("row"), lax.axis_index("col"), lax.axis_index("layer") // 4]).astype(jnp.int32)
    frame, share = local_work(place, offsets, spots, ext, probe_modes, amplitudes[0], jnp.asarray(tables()))
    return gather(frame, share, object_field)


def solution(mesh):
    placed = (
        P(None, "row", "col"),
        P(),
        P(("row", "col", "layer"), None, None),
        P(("row", "col", "layer"), None),
    )
    return jax.shard_map(
        body, mesh=mesh, in_specs=placed, out_specs=P(None, "row", "col"), check_vma=False
    )
```

```python
import functools
import math

import jax
import jax.numpy as jnp
import numpy as np
from jax import lax
from jax.experimental import pallas as pl
from jax.experimental.pallas import tpu as pltpu
from jax.sharding import PartitionSpec as P

SOFTEN = 0.05
DAMPING = 0.5
MODES = 4
SIDE = 256
HALF = 128
QUART = 64
F32 = jnp.float32
BF16 = jnp.bfloat16
VMEM_SPEC = pl.BlockSpec(memory_space=pltpu.VMEM)
SMEM_SPEC = pl.BlockSpec(memory_space=pltpu.SMEM)
ANY_SPEC = pl.BlockSpec(memory_space=pl.ANY)


def remote(src, dst, send, recv, device):
    return pltpu.make_async_remote_copy(
        src_ref=src,
        dst_ref=dst,
        send_sem=send,
        recv_sem=recv,
        device_id=device,
        device_id_type=pl.DeviceIdType.MESH,
    )


class Place:
    def __init__(self):
        self.row = lax.axis_index("row")
        self.col = lax.axis_index("col")
        layer = lax.axis_index("layer")
        self.layer = layer
        self.z = layer // 4
        self.xh = (layer // 2) % 2
        self.core = layer % 2
        self.partner = self.at(xh=self.xh, core=1 - self.core)
        self.far_x = self.at(xh=1 - self.xh)
        self.cross_xh = (self.xh + self.core) % 2
        self.cross = {"row": 1 - self.row, "layer": self.z * 4 + self.cross_xh * 2 + self.core}
        self.left = {"col": (self.col + 3) % 4}
        self.right = {"col": (self.col + 1) % 4}

    def at(self, z=None, xh=None, core=None):
        z = self.z if z is None else z
        xh = self.xh if xh is None else xh
        core = self.core if core is None else core
        return {"layer": z * 4 + xh * 2 + core}

    def z_peer(self, step):
        return self.at(z=(self.z + step) % 4)

    def meet(self):
        barrier = pltpu.get_barrier_semaphore()
        others = [self.partner, self.far_x, self.cross, self.left, self.right]
        others += [self.z_peer(step) for step in (1, 2, 3)]
        for other in others:
            pl.semaphore_signal(barrier, inc=1, device_id=other, device_id_type=pl.DeviceIdType.MESH)
        pl.semaphore_wait(barrier, len(others))


def rows_of(part, base=0):
    return pl.ds(pl.multiple_of(base + part * QUART, QUART), QUART)


def groups_of(part, base=0):
    return pl.ds(base // 8 + part * (QUART // 8), QUART // 8)


def tables():
    steps = np.arange(HALF)
    found = []
    for odd in (0, 1):
        phase = (steps[:, None] * (2 * steps[None, :] + odd)) % SIDE
        angle = phase * (2.0 * math.pi / SIDE)
        real, imag = np.cos(angle) / 16.0, -np.sin(angle) / 16.0
        full = np.block([[real, imag], [-imag, real]]).astype(np.float32)
        for table in (full, np.ascontiguousarray(full.T)):
            high = table.astype(jnp.bfloat16)
            low = (table - high.astype(np.float32)).astype(jnp.bfloat16)
            found += [high, low]
    order = np.zeros((SIDE, SIDE), np.float32)
    order[2 * steps, steps] = 1.0
    order[2 * steps + 1, HALF + steps] = 1.0
    found += [order.astype(jnp.bfloat16), np.ascontiguousarray(order.T).astype(jnp.bfloat16)]
    return np.stack(found)


EVEN, EVEN_T, ODD, ODD_T, ORDER, ORDER_T = 0, 2, 4, 6, 8, 9


def dot(left, right):
    return jnp.dot(left, right, preferred_element_type=F32)


def split(value):
    high = value.astype(BF16)
    return high, (value - high.astype(F32)).astype(BF16)


def on_lanes(value, tabs, which):
    high, low = split(value)
    return dot(high, tabs[which]) + dot(low, tabs[which]) + dot(high, tabs[which + 1])


def on_rows(value, tabs, which):
    high, low = split(value)
    return dot(tabs[which], high) + dot(tabs[which], low) + dot(tabs[which + 1], high)


def side_by_side(left, right):
    return jnp.concatenate([left, right], axis=1)


def on_top(upper, lower):
    return jnp.concatenate([upper, lower], axis=0)


def halo(me, ext, spots, right_send, right_recv, low_send, low_recv, diag_send, diag_recv, pair_send, pair_recv,
         spot_send, spot_recv, meanwhile):
    core = me.core
    has_right = me.col < 3
    has_left = me.col > 0
    top = me.row == 0
    bottom = me.row == 1

    def right_copy(part):
        return remote(ext.at[0, core, groups_of(part)], ext.at[1, core, groups_of(part)],
                      right_send.at[part], right_recv.at[part], me.left)

    def low_copy(part):
        return remote(ext.at[0, core, groups_of(part)], ext.at[0, core, groups_of(part, SIDE)],
                      low_send.at[part], low_recv.at[part], me.cross)

    def diag_copy(part):
        return remote(ext.at[1, core, groups_of(part)], ext.at[1, core, groups_of(part, SIDE)],
                      diag_send.at[part], diag_recv.at[part], me.cross)

    def pair_copy(kind, part):
        side, base = ((1, 0), (0, SIDE), (1, SIDE))[kind]
        where = ext.at[side, core, groups_of(part, base)]
        return remote(where, where, pair_send.at[kind, part], pair_recv.at[kind, part], me.partner)

    @pl.when(has_left)
    def _():
        for part in range(4):
            right_copy(part).start()

    @pl.when(bottom)
    def _():
        for part in range(4):
            low_copy(part).start()

    def spot_copy(step):
        if step == 0:
            where = pl.ds(me.layer, 1)
            return remote(spots.at[where], spots.at[where], spot_send.at[0], spot_recv.at[0], me.partner)
        if step == 1:
            where = pl.ds(me.z * 4 + me.xh * 2, 2)
            return remote(spots.at[where], spots.at[where], spot_send.at[1], spot_recv.at[1], me.far_x)
        if step < 5:
            where = pl.ds(me.z * 4, 4)
            return remote(spots.at[where], spots.at[where], spot_send.at[step], spot_recv.at[step],
                          me.z_peer(step - 1))
        if step == 5:
            return remote(spots.at[pl.ds(0, 16)], spots.at[pl.ds(16, 16)], spot_send.at[5], spot_recv.at[5], me.right)
        return remote(spots.at[pl.ds(0, 32)], spots.at[pl.ds(32, 32)], spot_send.at[6], spot_recv.at[6], me.cross)

    def spots_go(stage):
        if stage == 0:
            spot_copy(0).start()
        elif stage == 1:
            spot_copy(0).wait_recv()
            spot_copy(1).start()
        elif stage == 2:
            spot_copy(1).wait_recv()
            for step in (2, 3, 4):
                spot_copy(step).start()
        elif stage == 3:
            for step in (2, 3, 4):
                spot_copy(step).wait_recv()

            @pl.when(has_right)
            def _():
                spot_copy(5).start()
        elif stage == 4:
            @pl.when(has_left)
            def _():
                spot_copy(5).wait_recv()

            @pl.when(top)
            def _():
                spot_copy(6).start()
        else:
            @pl.when(bottom)
            def _():
                spot_copy(6).wait_recv()

    spots_go(0)
    meanwhile()
    for part in range(4):
        @pl.when(has_right)
        def _():
            right_copy(part).wait_recv()

            @pl.when(bottom)
            def _():
                diag_copy(part).start()

            pair_copy(0, part).start()

        @pl.when(top)
        def _():
            low_copy(part).wait_recv()
            pair_copy(1, part).start()

        spots_go(part + 1)

    @pl.when(jnp.logical_and(top, has_right))
    def _():
        for part in range(4):
            diag_copy(part).wait_recv()
            pair_copy(2, part).start()

    spots_go(5)

    @pl.when(has_left)
    def _():
        for part in range(4):
            right_copy(part).wait_send()

    @pl.when(bottom)
    def _():
        for part in range(4):
            low_copy(part).wait_send()

            @pl.when(has_right)
            def _():
                diag_copy(part).wait_send()

    @pl.when(has_right)
    def _():
        for part in range(4):
            pair_copy(0, part).wait_send()
            other_pair(ext, pair_send, pair_recv, me, 0, part).wait_recv()

    @pl.when(top)
    def _():
        for part in range(4):
            pair_copy(1, part).wait_send()
            other_pair(ext, pair_send, pair_recv, me, 1, part).wait_recv()

            @pl.when(has_right)
            def _():
                pair_copy(2, part).wait_send()
                other_pair(ext, pair_send, pair_recv, me, 2, part).wait_recv()

    for step in range(5):
        spot_copy(step).wait_send()

    @pl.when(has_right)
    def _():
        spot_copy(5).wait_send()

    @pl.when(top)
    def _():
        spot_copy(6).wait_send()


def other_pair(ext, pair_send, pair_recv, me, kind, part):
    side, base = ((1, 0), (0, SIDE), (1, SIDE))[kind]
    where = ext.at[side, 1 - me.core, groups_of(part, base)]
    return remote(where, where, pair_send.at[kind, part], pair_recv.at[kind, part], me.partner)


def forward(mode, probe, patch, tabs, far):
    pr, pi = probe[0, mode], probe[1, mode]
    tr, ti = patch[0], patch[1]
    er = pr * tr - pi * ti
    ei = pr * ti + pi * tr
    even = side_by_side(er[:, :HALF] + er[:, HALF:], ei[:, :HALF] + ei[:, HALF:])
    odd = side_by_side(er[:, :HALF] - er[:, HALF:], ei[:, :HALF] - ei[:, HALF:])
    ye = on_lanes(even, tabs, EVEN)
    yo = on_lanes(odd, tabs, ODD)
    for parity, which in ((0, EVEN_T), (1, ODD_T)):
        if parity == 0:
            se, so = ye[:HALF] + ye[HALF:], yo[:HALF] + yo[HALF:]
        else:
            se, so = ye[:HALF] - ye[HALF:], yo[:HALF] - yo[HALF:]
        stack = on_top(side_by_side(se[:, :HALF], so[:, :HALF]), side_by_side(se[:, HALF:], so[:, HALF:]))
        far[mode, parity] = on_rows(stack, tabs, which)


def backward_rows(mode, ratio, tabs, far):
    sums = []
    for parity, which in ((0, EVEN), (1, ODD)):
        scale = ratio[parity]
        sums.append(on_rows(far[mode, parity] * on_top(scale, scale), tabs, which))
    far[mode, 0] = sums[0] + sums[1]
    far[mode, 1] = sums[0] - sums[1]


def backward_lanes(half, probe, tabs, far, block):
    even = [side_by_side(far[mode, half, :HALF, :HALF], far[mode, half, HALF:, :HALF]) for mode in range(MODES)]
    odd = [side_by_side(far[mode, half, :HALF, HALF:], far[mode, half, HALF:, HALF:]) for mode in range(MODES)]
    pe = on_lanes(jnp.concatenate(even, axis=0), tabs, EVEN_T)
    po = on_lanes(jnp.concatenate(odd, axis=0), tabs, ODD_T)
    first, second = pe + po, pe - po
    where = slice(half * HALF, half * HALF + HALF)
    cr = ci = None
    for mode in range(MODES):
        part = slice(mode * HALF, mode * HALF + HALF)
        nr = side_by_side(first[part, :HALF], second[part, :HALF])
        ni = side_by_side(first[part, HALF:], second[part, HALF:])
        pr, pi = probe[0, mode, where], probe[1, mode, where]
        tr = pr * nr + pi * ni
        ti = pr * ni - pi * nr
        cr = tr if cr is None else cr + tr
        ci = ti if ci is None else ci + ti
    block[0, where] = cr
    block[1, where] = ci


def rows_from(ref, start, count):
    group = lax.shift_right_arithmetic(start, 3)
    wide = ref[pl.ds(group, count // 8 + 1)].reshape(count + 8, SIDE)
    return pltpu.roll(wide, lax.rem(count + 8 - (start - group * 8), count + 8), 0)[:count]


def inside(value):
    return jnp.clip(value, 0, SIDE - 1)


def grouped(value):
    return value.reshape(value.shape[0] // 8, 8, SIDE)


def sort_amplitudes(amp, tabs, ratio):
    rest = amp[...]
    total = None
    for _ in range(3):
        piece = rest.astype(BF16)
        rest = rest - piece.astype(F32)
        moved = dot(dot(tabs[ORDER_T], piece).astype(BF16), tabs[ORDER])
        total = moved if total is None else total + moved
    ratio[0] = total[:HALF]
    ratio[1] = total[HALF:]


def sum_power(probe, padded, share):
    power = None
    for mode in range(MODES):
        term = probe[0, mode] * probe[0, mode] + probe[1, mode] * probe[1, mode]
        power = term if power is None else power + term
    padded[pl.ds(0, 32)] = jnp.zeros((32, 8, SIDE), F32)
    padded[pl.ds(32, 32)] = grouped(power)
    padded[pl.ds(64, 33)] = jnp.zeros((33, 8, SIDE), F32)
    share[...] = jnp.zeros_like(share)


def cut_patch(row_at, col_at, ext, patch):
    lanes = lax.broadcasted_iota(jnp.int32, (SIDE, SIDE), 1)
    back = lax.rem(SIDE - col_at, SIDE)
    for plane in range(2):
        here = pltpu.roll(rows_from(ext.at[0, plane], row_at, SIDE), back, 1)
        there = pltpu.roll(rows_from(ext.at[1, plane], row_at, SIDE), back, 1)
        patch[plane] = jnp.where(lanes < SIDE - col_at, here, there)


def make_ratio(far, ratio):
    for parity in range(2):
        seen = None
        for mode in range(MODES):
            re, im = far[mode, parity, :HALF], far[mode, parity, HALF:]
            term = re * re + im * im
            seen = term if seen is None else seen + term
        ratio[parity] = ratio[parity] / (jnp.sqrt(seen) + SOFTEN)


TOGETHER = 4


def add_spots(me, group, spots, padded, share):
    up, left = group // 2, group % 2
    known = jnp.logical_and(me.row >= up, me.col >= left)
    first = up * SIDE + me.z * QUART + SIDE
    row_base = (me.row - up) * SIDE
    col_base = (me.col - left) * SIDE
    lanes = lax.broadcasted_iota(jnp.int32, (QUART, SIDE), 1)

    def some(index, carry):
        total = share[...]
        for step in range(TOGETHER):
            spot = group * 16 + index * TOGETHER + step
            start = jnp.where(known, first - inside(spots[spot, 0, 0] - row_base), 0)
            turn = jnp.where(known, inside(spots[spot, 0, 1] - col_base), 0)
            turned = pltpu.roll(rows_from(padded, start, QUART), turn, 1)
            kept = lanes >= turn if left == 0 else lanes < turn
            total = total + jnp.where(kept, turned, 0.0)
        share[...] = total
        return carry

    lax.fori_loop(0, 16 // TOGETHER, some, 0)


def put_tall(value, col_at, tall):
    lanes = lax.broadcasted_iota(jnp.int32, (SIDE, SIDE), 1)
    turned = pltpu.roll(value, col_at, 1)
    tall[0, pl.ds(32, 32)] = grouped(jnp.where(lanes >= col_at, turned, 0.0))
    tall[1, pl.ds(32, 32)] = grouped(jnp.where(lanes < col_at, turned, 0.0))


def whole_kernel(
    offsets, obj_hbm, probe_hbm, amp_hbm, tabs_hbm, out,
    ext, spots, spot_words, probe, amp, tabs, patch, far, ratio, block, padded, share,
    twin_block, tall, low_sum, low_in, right_sum, right_in, total, z_in, x_out, x_in,
    load_sem,
    h_right_send, h_right_recv, h_low_send, h_low_recv, h_diag_send, h_diag_recv,
    h_pair_send, h_pair_recv, spot_send, spot_recv,
    pair_send, pair_recv, low_send, low_recv, right_send, right_recv,
    z_send, z_recv, x_send, x_recv, out_send, out_recv, twin_send, twin_recv,
):
    me = Place()
    core = me.core
    loads = [
        pltpu.make_async_copy(obj_hbm.at[0], ext.at[0, 0, pl.ds(0, SIDE // 8)], load_sem.at[0]),
        pltpu.make_async_copy(obj_hbm.at[1], ext.at[0, 1, pl.ds(0, SIDE // 8)], load_sem.at[1]),
        pltpu.make_async_copy(tabs_hbm, tabs, load_sem.at[2]),
        pltpu.make_async_copy(amp_hbm, amp, load_sem.at[3]),
        pltpu.make_async_copy(probe_hbm, probe, load_sem.at[4]),
    ]
    for load in loads:
        load.start()
    lanes = lax.broadcasted_iota(jnp.int32, (1, 1, 128), 2)
    line = jnp.where(lanes == 0, offsets[0, 0], jnp.where(lanes == 1, offsets[0, 1], 0))
    spots[pl.ds(me.layer, 1)] = line
    me.meet()
    loads[0].wait()
    loads[1].wait()

    def meanwhile():
        loads[2].wait()
        loads[3].wait()
        sort_amplitudes(amp, tabs, ratio)
        for source in range(2):
            for side in range(2):
                tall[source, side, pl.ds(0, 32)] = jnp.zeros((32, 8, SIDE), F32)
                tall[source, side, pl.ds(64, 33)] = jnp.zeros((33, 8, SIDE), F32)
        loads[4].wait()
        sum_power(probe, padded, share)

    halo(me, ext, spots, h_right_send, h_right_recv, h_low_send, h_low_recv, h_diag_send, h_diag_recv,
         h_pair_send, h_pair_recv, spot_send, spot_recv, meanwhile)
    words = pltpu.make_async_copy(spots, spot_words, load_sem.at[5])
    words.start()

    row_at = inside(offsets[0, 0] - me.row * SIDE)
    col_at = inside(offsets[0, 1] - me.col * SIDE)
    cut_patch(row_at, col_at, ext, patch)
    for mode in range(MODES):
        forward(mode, probe, patch, tabs, far)
    make_ratio(far, ratio)
    for mode in range(MODES):
        backward_rows(mode, ratio, tabs, far)
    words.wait()
    twin_layer = me.layer + 1 - 2 * core
    twin_row = inside(spot_words[twin_layer, 0, 0] - me.row * SIDE)
    twin_col = inside(spot_words[twin_layer, 0, 1] - me.col * SIDE)

    def pair_copy(half):
        where = pl.ds(half * HALF, HALF)
        return remote(block.at[1 - core, where], twin_block.at[where],
                      pair_send.at[half], pair_recv.at[half], me.partner)

    for half in range(2):
        backward_lanes(half, probe, tabs, far, block)
        pair_copy(half).start()

    has_right = me.col < 3
    has_left = me.col > 0
    top = me.row == 0
    bottom = me.row == 1
    parts = [(me.z + 1 + step) % 4 for step in range(4)]

    def low_copy(step):
        where = rows_of(parts[step])
        return remote(low_sum.at[:, where], low_in.at[:, where], low_send.at[step], low_recv.at[step], me.cross)

    def right_copy(step):
        where = rows_of(parts[step])
        return remote(right_sum.at[where], right_in.at[where], right_send.at[step], right_recv.at[step], me.right)

    def z_copy(step):
        return remote(total.at[rows_of(parts[step])], z_in.at[step], z_send.at[step], z_recv.at[step],
                      me.z_peer(step + 1))

    put_tall(block[core], col_at, tall.at[0])
    for half in range(2):
        pair_copy(half).wait_recv()
    put_tall(twin_block[...], twin_col, tall.at[1])

    def both(side, part, base):
        first = SIDE + base + part * QUART
        return (rows_from(tall.at[0, side], first - row_at, QUART)
                + rows_from(tall.at[1, side], first - twin_row, QUART))

    for step in range(4):
        where = rows_of(parts[step])

        @pl.when(top)
        def _():
            for side in range(2):
                low_sum[side, where] = both(side, parts[step], SIDE)
            low_copy(step).start()

        total[where] = both(0, parts[step], 0)
        right_sum[where] = both(1, parts[step], 0)

        @pl.when(bottom)
        def _():
            low_copy(step).wait_recv()
            total[where] = total[where] + low_in[0, where]
            right_sum[where] = right_sum[where] + low_in[1, where]

        @pl.when(has_right)
        def _():
            right_copy(step).start()

        add_spots(me, step, spot_words, padded, share)

    for step in range(4):
        where = rows_of(parts[step])

        @pl.when(has_left)
        def _():
            right_copy(step).wait_recv()
            total[where] = total[where] + right_in[where]

        if step < 3:
            z_copy(step).start()

    mine = rows_of(me.z)
    for step in range(3):
        z_copy(step).wait_recv()
    x_out[...] = total[mine] + z_in[0] + z_in[1] + z_in[2]
    x_copy = remote(x_out, x_in, x_send.at[0], x_recv.at[0], me.far_x)
    x_copy.start()
    x_copy.wait_recv()
    whole = x_out[...] + x_in[...]
    out[core, mine] = (whole + DAMPING * ext[0, core, groups_of(me.z)].reshape(QUART, SIDE)) / (share[...] + DAMPING)

    def out_copy(step):
        return remote(out.at[core, mine], out.at[core, mine], out_send.at[step], out_recv.at[step], me.z_peer(step + 1))

    def come_copy(step):
        where = out.at[core, rows_of((me.z + 3 - step) % 4)]
        return remote(where, where, out_send.at[step], out_recv.at[step], me.z_peer(step + 1))

    def twin_copy(step, plane):
        part = me.z if step == 3 else (me.z + 3 - step) % 4
        where = out.at[plane, rows_of(part)]
        return remote(where, where, twin_send.at[step], twin_recv.at[step], me.partner)

    for step in (1, 0, 2):
        out_copy(step).start()
    twin_copy(3, core).start()
    for step in (0, 2, 1):
        come_copy(step).wait_recv()
        twin_copy(step, core).start()
    for step in (3, 0, 2, 1):
        twin_copy(step, 1 - core).wait_recv()

    for half in range(2):
        pair_copy(half).wait_send()
    for step in range(4):
        twin_copy(step, core).wait_send()

        @pl.when(top)
        def _():
            low_copy(step).wait_send()

        @pl.when(has_right)
        def _():
            right_copy(step).wait_send()

        if step < 3:
            z_copy(step).wait_send()
            out_copy(step).wait_send()
    x_copy.wait_send()


def body(object_field, probe_modes, amplitudes, offsets):
    sems = pltpu.SemaphoreType.DMA
    return pl.pallas_call(
        whole_kernel,
        out_shape=jax.ShapeDtypeStruct((2, SIDE, SIDE), F32),
        in_specs=[SMEM_SPEC] + [ANY_SPEC] * 4,
        out_specs=VMEM_SPEC,
        scratch_shapes=[
            pltpu.VMEM((2, 2, 64, 8, SIDE), F32),
            pltpu.VMEM((64, 1, 128), jnp.int32),
            pltpu.SMEM((64, 1, 128), jnp.int32),
            pltpu.VMEM((2, MODES, SIDE, SIDE), F32),
            pltpu.VMEM((SIDE, SIDE), F32),
            pltpu.VMEM((10, SIDE, SIDE), BF16),
            pltpu.VMEM((2, SIDE, SIDE), F32),
            pltpu.VMEM((MODES, 2, SIDE, SIDE), F32),
            pltpu.VMEM((2, HALF, SIDE), F32),
            pltpu.VMEM((2, SIDE, SIDE), F32),
            pltpu.VMEM((97, 8, SIDE), F32),
            pltpu.VMEM((QUART, SIDE), F32),
            pltpu.VMEM((SIDE, SIDE), F32),
            pltpu.VMEM((2, 2, 97, 8, SIDE), F32),
            pltpu.VMEM((2, SIDE, SIDE), F32),
            pltpu.VMEM((2, SIDE, SIDE), F32),
            pltpu.VMEM((SIDE, SIDE), F32),
            pltpu.VMEM((SIDE, SIDE), F32),
            pltpu.VMEM((SIDE, SIDE), F32),
            pltpu.VMEM((3, QUART, SIDE), F32),
            pltpu.VMEM((QUART, SIDE), F32),
            pltpu.VMEM((QUART, SIDE), F32),
            sems((6,)),
            sems((4,)), sems((4,)), sems((4,)), sems((4,)), sems((4,)), sems((4,)),
            sems((3, 4)), sems((3, 4)), sems((7,)), sems((7,)),
            sems((2,)), sems((2,)), sems((4,)), sems((4,)), sems((4,)), sems((4,)),
            sems((3,)), sems((3,)), sems((1,)), sems((1,)), sems((3,)), sems((3,)), sems((4,)), sems((4,)),
        ],
        compiler_params=pltpu.CompilerParams(collective_id=0, has_side_effects=True),
        name="whole",
    )(offsets, object_field.reshape(2, 32, 8, SIDE), probe_modes, amplitudes[0], jnp.asarray(tables()))


def solution(mesh):
    placed = (
        P(None, "row", "col"),
        P(),
        P(("row", "col", "layer"), None, None),
        P(("row", "col", "layer"), None),
    )
    return jax.shard_map(
        body, mesh=mesh, in_specs=placed, out_specs=P(None, "row", "col"), check_vma=False
    )
```

```python
import functools
import math

import jax
import jax.numpy as jnp
import numpy as np
from jax import lax
from jax.experimental import pallas as pl
from jax.experimental.pallas import tpu as pltpu
from jax.sharding import PartitionSpec as P

SOFTEN = 0.05
DAMPING = 0.5
MODES = 4
SIDE = 256
HALF = 128
QUART = 64
F32 = jnp.float32
BF16 = jnp.bfloat16
VMEM_SPEC = pl.BlockSpec(memory_space=pltpu.VMEM)
SMEM_SPEC = pl.BlockSpec(memory_space=pltpu.SMEM)
ANY_SPEC = pl.BlockSpec(memory_space=pl.ANY)


def remote(src, dst, send, recv, device):
    return pltpu.make_async_remote_copy(
        src_ref=src,
        dst_ref=dst,
        send_sem=send,
        recv_sem=recv,
        device_id=device,
        device_id_type=pl.DeviceIdType.MESH,
    )


class Place:
    def __init__(self):
        self.row = lax.axis_index("row")
        self.col = lax.axis_index("col")
        layer = lax.axis_index("layer")
        self.layer = layer
        self.z = layer // 4
        self.xh = (layer // 2) % 2
        self.core = layer % 2
        self.partner = self.at(xh=self.xh, core=1 - self.core)
        self.far_x = self.at(xh=1 - self.xh)
        self.cross_xh = (self.xh + self.core) % 2
        self.cross = {"row": 1 - self.row, "layer": self.z * 4 + self.cross_xh * 2 + self.core}
        self.left = {"col": (self.col + 3) % 4}
        self.right = {"col": (self.col + 1) % 4}

    def at(self, z=None, xh=None, core=None):
        z = self.z if z is None else z
        xh = self.xh if xh is None else xh
        core = self.core if core is None else core
        return {"layer": z * 4 + xh * 2 + core}

    def z_peer(self, step):
        return self.at(z=(self.z + step) % 4)

    def meet(self):
        barrier = pltpu.get_barrier_semaphore()
        others = [self.partner, self.far_x, self.cross, self.left, self.right]
        others += [self.z_peer(step) for step in (1, 2, 3)]
        for other in others:
            pl.semaphore_signal(barrier, inc=1, device_id=other, device_id_type=pl.DeviceIdType.MESH)
        pl.semaphore_wait(barrier, len(others))


def rows_of(part, base=0):
    return pl.ds(pl.multiple_of(base + part * QUART, QUART), QUART)


def groups_of(part, base=0):
    return pl.ds(base // 8 + part * (QUART // 8), QUART // 8)


def tables():
    steps = np.arange(HALF)
    found = []
    for odd in (0, 1):
        phase = (steps[:, None] * (2 * steps[None, :] + odd)) % SIDE
        angle = phase * (2.0 * math.pi / SIDE)
        real, imag = np.cos(angle) / 16.0, -np.sin(angle) / 16.0
        full = np.block([[real, imag], [-imag, real]]).astype(np.float32)
        for table in (full, np.ascontiguousarray(full.T)):
            high = table.astype(jnp.bfloat16)
            low = (table - high.astype(np.float32)).astype(jnp.bfloat16)
            found += [high, low]
    order = np.zeros((SIDE, SIDE), np.float32)
    order[2 * steps, steps] = 1.0
    order[2 * steps + 1, HALF + steps] = 1.0
    found += [order.astype(jnp.bfloat16), np.ascontiguousarray(order.T).astype(jnp.bfloat16)]
    return np.stack(found)


EVEN, EVEN_T, ODD, ODD_T, ORDER, ORDER_T = 0, 2, 4, 6, 8, 9


def dot(left, right):
    return jnp.dot(left, right, preferred_element_type=F32)


def split(value):
    high = value.astype(BF16)
    return high, (value - high.astype(F32)).astype(BF16)


def on_lanes(value, tabs, which):
    high, low = split(value)
    return dot(high, tabs[which]) + dot(low, tabs[which]) + dot(high, tabs[which + 1])


def on_rows(value, tabs, which):
    high, low = split(value)
    return dot(tabs[which], high) + dot(tabs[which], low) + dot(tabs[which + 1], high)


def side_by_side(left, right):
    return jnp.concatenate([left, right], axis=1)


def on_top(upper, lower):
    return jnp.concatenate([upper, lower], axis=0)


def halo(me, ext, right_send, right_recv, share_send, share_recv, low_send, low_recv, diag_send, diag_recv,
         pair_send, pair_recv, meanwhile):
    core = me.core
    has_right = me.col < 3
    has_left = me.col > 0
    top = me.row == 0
    bottom = me.row == 1

    def piece(index, base=0):
        if index == 0:
            return pl.ds(base + me.z * 4, 4)
        if index < 3:
            return pl.ds(base + 8 + index * 8, 8)
        return pl.ds(base + ((me.z + 6 - index) % 4) * 4, 4)

    def right_copy(index):
        return remote(ext.at[0, core, piece(index)], ext.at[1, core, piece(index)],
                      right_send.at[index], right_recv.at[index], me.left)

    def share_copy(step):
        where = ext.at[1, core, piece(0)]
        return remote(where, where, share_send.at[step - 1], share_recv.at[step - 1], me.z_peer(step))

    def low_copy(part):
        return remote(ext.at[0, core, groups_of(part)], ext.at[0, core, groups_of(part, SIDE)],
                      low_send.at[part], low_recv.at[part], me.cross)

    def diag_copy(index):
        return remote(ext.at[1, core, piece(index)], ext.at[1, core, piece(index, 32)],
                      diag_send.at[index], diag_recv.at[index], me.cross)

    def pair_copy(kind, index, plane):
        if kind == 1:
            where = ext.at[0, plane, groups_of(index, SIDE)]
        else:
            where = ext.at[1, plane, piece(index, 32 if kind == 2 else 0)]
        sem = (0, 6, 10)[kind] + index
        return remote(where, where, pair_send.at[sem], pair_recv.at[sem], me.partner)

    @pl.when(has_left)
    def _():
        for index in range(3):
            right_copy(index).start()

    @pl.when(bottom)
    def _():
        for part in range(4):
            low_copy(part).start()

    meanwhile()

    def pass_on(index):
        @pl.when(bottom)
        def _():
            diag_copy(index).start()

        pair_copy(0, index, core).start()

    def low_here(part):
        @pl.when(top)
        def _():
            low_copy(part).wait_recv()
            pair_copy(1, part, core).start()

    @pl.when(has_right)
    def _():
        right_copy(0).wait_recv()
        for step in (2, 1, 3):
            share_copy(step).start()
        pass_on(0)

    low_here(0)
    low_here(1)

    @pl.when(has_right)
    def _():
        right_copy(1).wait_recv()
        pass_on(1)

    low_here(2)
    low_here(3)

    @pl.when(has_right)
    def _():
        right_copy(2).wait_recv()
        pass_on(2)
        for step in (1, 3, 2):
            share_copy(step).wait_recv()
            pass_on(step + 2)

    order = (0, 1, 2, 3, 5, 4)

    @pl.when(jnp.logical_and(top, has_right))
    def _():
        for index in order:
            diag_copy(index).wait_recv()
            pair_copy(2, index, core).start()

    @pl.when(has_right)
    def _():
        for index in order:
            pair_copy(0, index, 1 - core).wait_recv()

    @pl.when(top)
    def _():
        for part in range(4):
            pair_copy(1, part, 1 - core).wait_recv()

        @pl.when(has_right)
        def _():
            for index in order:
                pair_copy(2, index, 1 - core).wait_recv()

    def all_sent():
        @pl.when(has_left)
        def _():
            for index in range(3):
                right_copy(index).wait_send()

        @pl.when(bottom)
        def _():
            for part in range(4):
                low_copy(part).wait_send()

            @pl.when(has_right)
            def _():
                for index in range(6):
                    diag_copy(index).wait_send()

        @pl.when(has_right)
        def _():
            for step in (1, 2, 3):
                share_copy(step).wait_send()
            for index in range(6):
                pair_copy(0, index, core).wait_send()

        @pl.when(top)
        def _():
            for part in range(4):
                pair_copy(1, part, core).wait_send()

            @pl.when(has_right)
            def _():
                for index in range(6):
                    pair_copy(2, index, core).wait_send()

    return all_sent


def spot_chain(me, spots, spot_words, spot_send, spot_recv, word_sem):
    has_right = me.col < 3
    has_left = me.col > 0
    top = me.row == 0
    bottom = me.row == 1

    def spot_copy(step):
        if step == 0:
            where = pl.ds(me.layer, 1)
            return remote(spots.at[where], spots.at[where], spot_send.at[0], spot_recv.at[0], me.partner)
        if step == 1:
            where = pl.ds(me.z * 4 + me.xh * 2, 2)
            return remote(spots.at[where], spots.at[where], spot_send.at[1], spot_recv.at[1], me.far_x)
        if step < 5:
            where = pl.ds(me.z * 4, 4)
            return remote(spots.at[where], spots.at[where], spot_send.at[step], spot_recv.at[step],
                          me.z_peer(step - 1))
        if step == 5:
            return remote(spots.at[pl.ds(0, 16)], spots.at[pl.ds(16, 16)], spot_send.at[5], spot_recv.at[5], me.right)
        return remote(spots.at[pl.ds(0, 32)], spots.at[pl.ds(32, 32)], spot_send.at[6], spot_recv.at[6], me.cross)

    near = pltpu.make_async_copy(spots.at[pl.ds(0, 16)], spot_words.at[pl.ds(0, 16)], word_sem.at[0])
    others = pltpu.make_async_copy(spots.at[pl.ds(16, 48)], spot_words.at[pl.ds(16, 48)], word_sem.at[1])

    def go(stage):
        if stage == 0:
            spot_copy(0).start()
        elif stage == 1:
            spot_copy(0).wait_recv()
            spot_copy(1).start()
        elif stage == 2:
            spot_copy(1).wait_recv()
            for step in (2, 3, 4):
                spot_copy(step).start()
        elif stage == 3:
            for step in (2, 3, 4):
                spot_copy(step).wait_recv()
            near.start()

            @pl.when(has_right)
            def _():
                spot_copy(5).start()
        elif stage == 4:
            @pl.when(has_left)
            def _():
                spot_copy(5).wait_recv()

            @pl.when(top)
            def _():
                spot_copy(6).start()
        elif stage == 5:
            @pl.when(bottom)
            def _():
                spot_copy(6).wait_recv()

            others.start()
        else:
            for step in range(5):
                spot_copy(step).wait_send()

            @pl.when(has_right)
            def _():
                spot_copy(5).wait_send()

            @pl.when(top)
            def _():
                spot_copy(6).wait_send()

    return go, near, others


def forward(mode, probe, patch, tabs, far):
    pr, pi = probe[0, mode], probe[1, mode]
    tr, ti = patch[0], patch[1]
    er = pr * tr - pi * ti
    ei = pr * ti + pi * tr
    even = side_by_side(er[:, :HALF] + er[:, HALF:], ei[:, :HALF] + ei[:, HALF:])
    odd = side_by_side(er[:, :HALF] - er[:, HALF:], ei[:, :HALF] - ei[:, HALF:])
    ye = on_lanes(even, tabs, EVEN)
    yo = on_lanes(odd, tabs, ODD)
    for parity, which in ((0, EVEN_T), (1, ODD_T)):
        if parity == 0:
            se, so = ye[:HALF] + ye[HALF:], yo[:HALF] + yo[HALF:]
        else:
            se, so = ye[:HALF] - ye[HALF:], yo[:HALF] - yo[HALF:]
        stack = on_top(side_by_side(se[:, :HALF], so[:, :HALF]), side_by_side(se[:, HALF:], so[:, HALF:]))
        far[mode, parity] = on_rows(stack, tabs, which)


def backward_rows(mode, ratio, tabs, far):
    sums = []
    for parity, which in ((0, EVEN), (1, ODD)):
        scale = ratio[parity]
        sums.append(on_rows(far[mode, parity] * on_top(scale, scale), tabs, which))
    far[mode, 0] = sums[0] + sums[1]
    far[mode, 1] = sums[0] - sums[1]


def backward_lanes(half, probe, tabs, far, block):
    even = [side_by_side(far[mode, half, :HALF, :HALF], far[mode, half, HALF:, :HALF]) for mode in range(MODES)]
    odd = [side_by_side(far[mode, half, :HALF, HALF:], far[mode, half, HALF:, HALF:]) for mode in range(MODES)]
    pe = on_lanes(jnp.concatenate(even, axis=0), tabs, EVEN_T)
    po = on_lanes(jnp.concatenate(odd, axis=0), tabs, ODD_T)
    first, second = pe + po, pe - po
    where = slice(half * HALF, half * HALF + HALF)
    cr = ci = None
    for mode in range(MODES):
        part = slice(mode * HALF, mode * HALF + HALF)
        nr = side_by_side(first[part, :HALF], second[part, :HALF])
        ni = side_by_side(first[part, HALF:], second[part, HALF:])
        pr, pi = probe[0, mode, where], probe[1, mode, where]
        tr = pr * nr + pi * ni
        ti = pr * ni - pi * nr
        cr = tr if cr is None else cr + tr
        ci = ti if ci is None else ci + ti
    block[0, where] = cr
    block[1, where] = ci


def rows_from(ref, start, count):
    group = lax.shift_right_arithmetic(start, 3)
    wide = ref[pl.ds(group, count // 8 + 1)].reshape(count + 8, SIDE)
    return pltpu.roll(wide, lax.rem(count + 8 - (start - group * 8), count + 8), 0)[:count]


def inside(value):
    return jnp.clip(value, 0, SIDE - 1)


def grouped(value):
    return value.reshape(value.shape[0] // 8, 8, SIDE)


def sort_amplitudes(amp, tabs, ratio):
    rest = amp[...]
    total = None
    for _ in range(3):
        piece = rest.astype(BF16)
        rest = rest - piece.astype(F32)
        moved = dot(dot(tabs[ORDER_T], piece).astype(BF16), tabs[ORDER])
        total = moved if total is None else total + moved
    ratio[0] = total[:HALF]
    ratio[1] = total[HALF:]


def sum_power(probe, padded, share):
    power = None
    for mode in range(MODES):
        term = probe[0, mode] * probe[0, mode] + probe[1, mode] * probe[1, mode]
        power = term if power is None else power + term
    padded[pl.ds(0, 32)] = jnp.zeros((32, 8, SIDE), F32)
    padded[pl.ds(32, 32)] = grouped(power)
    padded[pl.ds(64, 33)] = jnp.zeros((33, 8, SIDE), F32)
    share[...] = jnp.zeros_like(share)


def cut_patch(row_at, col_at, ext, patch):
    lanes = lax.broadcasted_iota(jnp.int32, (SIDE, SIDE), 1)
    back = lax.rem(SIDE - col_at, SIDE)
    for plane in range(2):
        here = pltpu.roll(rows_from(ext.at[0, plane], row_at, SIDE), back, 1)
        there = pltpu.roll(rows_from(ext.at[1, plane], row_at, SIDE), back, 1)
        patch[plane] = jnp.where(lanes < SIDE - col_at, here, there)


def make_ratio(far, ratio):
    for parity in range(2):
        seen = None
        for mode in range(MODES):
            re, im = far[mode, parity, :HALF], far[mode, parity, HALF:]
            term = re * re + im * im
            seen = term if seen is None else seen + term
        ratio[parity] = ratio[parity] / (jnp.sqrt(seen) + SOFTEN)


TOGETHER = 4


def add_spots(me, group, spots, padded, share):
    up, left = group // 2, group % 2
    known = jnp.logical_and(me.row >= up, me.col >= left)
    first = up * SIDE + me.z * QUART + SIDE
    row_base = (me.row - up) * SIDE
    col_base = (me.col - left) * SIDE
    lanes = lax.broadcasted_iota(jnp.int32, (QUART, SIDE), 1)

    def some(index, carry):
        total = share[...]
        for step in range(TOGETHER):
            spot = group * 16 + index * TOGETHER + step
            start = jnp.where(known, first - inside(spots[spot, 0, 0] - row_base), 0)
            turn = jnp.where(known, inside(spots[spot, 0, 1] - col_base), 0)
            turned = pltpu.roll(rows_from(padded, start, QUART), turn, 1)
            kept = lanes >= turn if left == 0 else lanes < turn
            total = total + jnp.where(kept, turned, 0.0)
        share[...] = total
        return carry

    lax.fori_loop(0, 16 // TOGETHER, some, 0)


def put_tall(value, col_at, tall):
    lanes = lax.broadcasted_iota(jnp.int32, (SIDE, SIDE), 1)
    turned = pltpu.roll(value, col_at, 1)
    tall[0, pl.ds(32, 32)] = grouped(jnp.where(lanes >= col_at, turned, 0.0))
    tall[1, pl.ds(32, 32)] = grouped(jnp.where(lanes < col_at, turned, 0.0))


def whole_kernel(
    offsets, obj_hbm, probe_hbm, amp_hbm, tabs_hbm, out,
    ext, spots, spot_words, probe, amp, tabs, patch, far, ratio, block, padded, share,
    twin_block, tall, low_sum, low_in, right_sum, right_in, total, z_in, x_out, x_in,
    load_sem, word_sem,
    h_right_send, h_right_recv, h_share_send, h_share_recv, h_low_send, h_low_recv, h_diag_send, h_diag_recv,
    h_pair_send, h_pair_recv, spot_send, spot_recv,
    pair_send, pair_recv, low_send, low_recv, right_send, right_recv,
    z_send, z_recv, x_send, x_recv, out_send, out_recv, twin_send, twin_recv,
):
    me = Place()
    core = me.core
    loads = [
        pltpu.make_async_copy(obj_hbm.at[0], ext.at[0, 0, pl.ds(0, SIDE // 8)], load_sem.at[0]),
        pltpu.make_async_copy(obj_hbm.at[1], ext.at[0, 1, pl.ds(0, SIDE // 8)], load_sem.at[1]),
        pltpu.make_async_copy(tabs_hbm, tabs, load_sem.at[2]),
        pltpu.make_async_copy(amp_hbm, amp, load_sem.at[3]),
        pltpu.make_async_copy(probe_hbm, probe, load_sem.at[4]),
    ]
    for load in loads:
        load.start()
    lanes = lax.broadcasted_iota(jnp.int32, (1, 1, 128), 2)
    line = jnp.where(lanes == 0, offsets[0, 0], jnp.where(lanes == 1, offsets[0, 1], 0))
    spots[pl.ds(me.layer, 1)] = line
    me.meet()
    loads[0].wait()
    loads[1].wait()

    def meanwhile():
        loads[2].wait()
        loads[3].wait()
        sort_amplitudes(amp, tabs, ratio)
        for source in range(2):
            for side in range(2):
                tall[source, side, pl.ds(0, 32)] = jnp.zeros((32, 8, SIDE), F32)
                tall[source, side, pl.ds(64, 33)] = jnp.zeros((33, 8, SIDE), F32)
        loads[4].wait()
        sum_power(probe, padded, share)

    spots_go, near_words, other_words = spot_chain(me, spots, spot_words, spot_send, spot_recv, word_sem)
    spots_go(0)
    halo_sent = halo(me, ext, h_right_send, h_right_recv, h_share_send, h_share_recv, h_low_send, h_low_recv,
                     h_diag_send, h_diag_recv, h_pair_send, h_pair_recv, meanwhile)
    spots_go(1)

    row_at = inside(offsets[0, 0] - me.row * SIDE)
    col_at = inside(offsets[0, 1] - me.col * SIDE)
    cut_patch(row_at, col_at, ext, patch)
    spots_go(2)
    for mode in range(MODES):
        forward(mode, probe, patch, tabs, far)
    spots_go(3)
    make_ratio(far, ratio)
    for mode in range(MODES):
        backward_rows(mode, ratio, tabs, far)
    spots_go(4)
    near_words.wait()
    twin_layer = me.layer + 1 - 2 * core
    twin_row = inside(spot_words[twin_layer, 0, 0] - me.row * SIDE)
    twin_col = inside(spot_words[twin_layer, 0, 1] - me.col * SIDE)

    def pair_copy(half):
        where = pl.ds(half * HALF, HALF)
        return remote(block.at[1 - core, where], twin_block.at[where],
                      pair_send.at[half], pair_recv.at[half], me.partner)

    for half in range(2):
        backward_lanes(half, probe, tabs, far, block)
        pair_copy(half).start()
    spots_go(5)

    has_right = me.col < 3
    has_left = me.col > 0
    top = me.row == 0
    bottom = me.row == 1
    parts = [(me.z + 1 + step) % 4 for step in range(4)]

    def low_copy(step):
        where = rows_of(parts[step])
        return remote(low_sum.at[:, where], low_in.at[:, where], low_send.at[step], low_recv.at[step], me.cross)

    def right_copy(step):
        where = rows_of(parts[step])
        return remote(right_sum.at[where], right_in.at[where], right_send.at[step], right_recv.at[step], me.right)

    def z_copy(step):
        return remote(total.at[rows_of(parts[step])], z_in.at[step], z_send.at[step], z_recv.at[step],
                      me.z_peer(step + 1))

    put_tall(block[core], col_at, tall.at[0])
    for half in range(2):
        pair_copy(half).wait_recv()
    put_tall(twin_block[...], twin_col, tall.at[1])
    other_words.wait()

    def both(side, part, base):
        first = SIDE + base + part * QUART
        return (rows_from(tall.at[0, side], first - row_at, QUART)
                + rows_from(tall.at[1, side], first - twin_row, QUART))

    for step in range(4):
        where = rows_of(parts[step])

        @pl.when(top)
        def _():
            for side in range(2):
                low_sum[side, where] = both(side, parts[step], SIDE)
            low_copy(step).start()

        total[where] = both(0, parts[step], 0)
        right_sum[where] = both(1, parts[step], 0)

        @pl.when(bottom)
        def _():
            low_copy(step).wait_recv()
            total[where] = total[where] + low_in[0, where]
            right_sum[where] = right_sum[where] + low_in[1, where]

        @pl.when(has_right)
        def _():
            right_copy(step).start()

        add_spots(me, step, spot_words, padded, share)

    for step in range(4):
        where = rows_of(parts[step])

        @pl.when(has_left)
        def _():
            right_copy(step).wait_recv()
            total[where] = total[where] + right_in[where]

        if step < 3:
            z_copy(step).start()

    mine = rows_of(me.z)
    for step in range(3):
        z_copy(step).wait_recv()
    x_out[...] = total[mine] + z_in[0] + z_in[1] + z_in[2]
    x_copy = remote(x_out, x_in, x_send.at[0], x_recv.at[0], me.far_x)
    x_copy.start()
    x_copy.wait_recv()
    whole = x_out[...] + x_in[...]
    out[core, mine] = (whole + DAMPING * ext[0, core, groups_of(me.z)].reshape(QUART, SIDE)) / (share[...] + DAMPING)

    def out_copy(step):
        return remote(out.at[core, mine], out.at[core, mine], out_send.at[step], out_recv.at[step], me.z_peer(step + 1))

    def come_copy(step):
        where = out.at[core, rows_of((me.z + 3 - step) % 4)]
        return remote(where, where, out_send.at[step], out_recv.at[step], me.z_peer(step + 1))

    def twin_copy(step, plane):
        part = me.z if step == 3 else (me.z + 3 - step) % 4
        where = out.at[plane, rows_of(part)]
        return remote(where, where, twin_send.at[step], twin_recv.at[step], me.partner)

    for step in (1, 0, 2):
        out_copy(step).start()
    twin_copy(3, core).start()
    for step in (0, 2, 1):
        come_copy(step).wait_recv()
        twin_copy(step, core).start()
    for step in (3, 0, 2, 1):
        twin_copy(step, 1 - core).wait_recv()

    for half in range(2):
        pair_copy(half).wait_send()
    for step in range(4):
        twin_copy(step, core).wait_send()

        @pl.when(top)
        def _():
            low_copy(step).wait_send()

        @pl.when(has_right)
        def _():
            right_copy(step).wait_send()

        if step < 3:
            z_copy(step).wait_send()
            out_copy(step).wait_send()
    x_copy.wait_send()
    halo_sent()
    spots_go(6)


def body(object_field, probe_modes, amplitudes, offsets):
    sems = pltpu.SemaphoreType.DMA
    return pl.pallas_call(
        whole_kernel,
        out_shape=jax.ShapeDtypeStruct((2, SIDE, SIDE), F32),
        in_specs=[SMEM_SPEC] + [ANY_SPEC] * 4,
        out_specs=VMEM_SPEC,
        scratch_shapes=[
            pltpu.VMEM((2, 2, 64, 8, SIDE), F32),
            pltpu.VMEM((64, 1, 128), jnp.int32),
            pltpu.SMEM((64, 1, 128), jnp.int32),
            pltpu.VMEM((2, MODES, SIDE, SIDE), F32),
            pltpu.VMEM((SIDE, SIDE), F32),
            pltpu.VMEM((10, SIDE, SIDE), BF16),
            pltpu.VMEM((2, SIDE, SIDE), F32),
            pltpu.VMEM((MODES, 2, SIDE, SIDE), F32),
            pltpu.VMEM((2, HALF, SIDE), F32),
            pltpu.VMEM((2, SIDE, SIDE), F32),
            pltpu.VMEM((97, 8, SIDE), F32),
            pltpu.VMEM((QUART, SIDE), F32),
            pltpu.VMEM((SIDE, SIDE), F32),
            pltpu.VMEM((2, 2, 97, 8, SIDE), F32),
            pltpu.VMEM((2, SIDE, SIDE), F32),
            pltpu.VMEM((2, SIDE, SIDE), F32),
            pltpu.VMEM((SIDE, SIDE), F32),
            pltpu.VMEM((SIDE, SIDE), F32),
            pltpu.VMEM((SIDE, SIDE), F32),
            pltpu.VMEM((3, QUART, SIDE), F32),
            pltpu.VMEM((QUART, SIDE), F32),
            pltpu.VMEM((QUART, SIDE), F32),
            sems((5,)), sems((2,)),
            sems((3,)), sems((3,)), sems((3,)), sems((3,)), sems((4,)), sems((4,)), sems((6,)), sems((6,)),
            sems((16,)), sems((16,)), sems((7,)), sems((7,)),
            sems((2,)), sems((2,)), sems((4,)), sems((4,)), sems((4,)), sems((4,)),
            sems((3,)), sems((3,)), sems((1,)), sems((1,)), sems((3,)), sems((3,)), sems((4,)), sems((4,)),
        ],
        compiler_params=pltpu.CompilerParams(collective_id=0, has_side_effects=True),
        name="whole",
    )(offsets, object_field.reshape(2, 32, 8, SIDE), probe_modes, amplitudes[0], jnp.asarray(tables()))


def solution(mesh):
    placed = (
        P(None, "row", "col"),
        P(),
        P(("row", "col", "layer"), None, None),
        P(("row", "col", "layer"), None),
    )
    return jax.shard_map(
        body, mesh=mesh, in_specs=placed, out_specs=P(None, "row", "col"), check_vma=False
    )
```

```python
import functools
import math

import jax
import jax.numpy as jnp
import numpy as np
from jax import lax
from jax.experimental import pallas as pl
from jax.experimental.pallas import tpu as pltpu
from jax.sharding import PartitionSpec as P

SOFTEN = 0.05
DAMPING = 0.5
MODES = 4
SIDE = 256
HALF = 128
QUART = 64
F32 = jnp.float32
BF16 = jnp.bfloat16
VMEM_SPEC = pl.BlockSpec(memory_space=pltpu.VMEM)
SMEM_SPEC = pl.BlockSpec(memory_space=pltpu.SMEM)
HBM_SPEC = pl.BlockSpec(memory_space=pltpu.HBM)


def remote(src, dst, send, recv, device):
    return pltpu.make_async_remote_copy(
        src_ref=src,
        dst_ref=dst,
        send_sem=send,
        recv_sem=recv,
        device_id=device,
        device_id_type=pl.DeviceIdType.MESH,
    )


class Place:
    def __init__(self):
        self.row = lax.axis_index("row")
        self.col = lax.axis_index("col")
        layer = lax.axis_index("layer")
        self.layer = layer
        self.z = layer // 4
        self.xh = (layer // 2) % 2
        self.core = layer % 2
        self.partner = self.at(xh=self.xh, core=1 - self.core)
        self.far_x = self.at(xh=1 - self.xh)
        self.cross_xh = (self.xh + self.core) % 2
        self.cross = {"row": 1 - self.row, "layer": self.z * 4 + self.cross_xh * 2 + self.core}
        self.left = {"col": (self.col + 3) % 4}
        self.right = {"col": (self.col + 1) % 4}

    def at(self, z=None, xh=None, core=None):
        z = self.z if z is None else z
        xh = self.xh if xh is None else xh
        core = self.core if core is None else core
        return {"layer": z * 4 + xh * 2 + core}

    def z_peer(self, step):
        return self.at(z=(self.z + step) % 4)

    def meet(self):
        barrier = pltpu.get_barrier_semaphore()
        others = [self.partner, self.far_x, self.cross, self.left, self.right]
        others += [self.z_peer(step) for step in (1, 2, 3)]
        others += [self.at(z=(self.z + step) % 4, xh=1 - self.xh) for step in (1, 2, 3)]
        for other in others:
            pl.semaphore_signal(barrier, inc=1, device_id=other, device_id_type=pl.DeviceIdType.MESH)
        pl.semaphore_wait(barrier, len(others))


def rows_of(part, base=0):
    return pl.ds(pl.multiple_of(base + part * QUART, QUART), QUART)


def groups_of(part, base=0):
    return pl.ds(base // 8 + part * (QUART // 8), QUART // 8)


def tables():
    steps = np.arange(HALF)
    found = []
    for odd in (0, 1):
        phase = (steps[:, None] * (2 * steps[None, :] + odd)) % SIDE
        angle = phase * (2.0 * math.pi / SIDE)
        real, imag = np.cos(angle) / 16.0, -np.sin(angle) / 16.0
        full = np.block([[real, imag], [-imag, real]]).astype(np.float32)
        for table in (full, np.ascontiguousarray(full.T)):
            high = table.astype(jnp.bfloat16)
            low = (table - high.astype(np.float32)).astype(jnp.bfloat16)
            found += [high, low]
    order = np.zeros((SIDE, SIDE), np.float32)
    order[2 * steps, steps] = 1.0
    order[2 * steps + 1, HALF + steps] = 1.0
    found += [order.astype(jnp.bfloat16), np.ascontiguousarray(order.T).astype(jnp.bfloat16)]
    return np.stack(found)


EVEN, EVEN_T, ODD, ODD_T, ORDER, ORDER_T = 0, 2, 4, 6, 8, 9


def dot(left, right):
    return jnp.dot(left, right, preferred_element_type=F32)


def split(value):
    high = value.astype(BF16)
    return high, (value - high.astype(F32)).astype(BF16)


def on_lanes(value, tabs, which):
    high, low = split(value)
    return dot(high, tabs[which]) + dot(low, tabs[which]) + dot(high, tabs[which + 1])


def on_rows(value, tabs, which):
    high, low = split(value)
    return dot(tabs[which], high) + dot(tabs[which], low) + dot(tabs[which + 1], high)


def side_by_side(left, right):
    return jnp.concatenate([left, right], axis=1)


def on_top(upper, lower):
    return jnp.concatenate([upper, lower], axis=0)


OWN = 5
PIECES = 8
ORDER_IN = (0, 1, 2, 5, 7, 3, 6, 4)


def halo(me, ext, right_send, right_recv, share_send, share_recv, low_send, low_recv, diag_send, diag_recv,
         pair_send, pair_recv, meanwhile, spots_go):
    core = me.core
    has_right = me.col < 3
    has_left = me.col > 0
    top = me.row == 0
    bottom = me.row == 1

    def piece(index, base=0):
        if index == 0:
            return pl.ds(base + me.z * 2, 2)
        if index < OWN:
            return pl.ds(base + (0, 8, 16, 24, 28)[index], (0, 8, 8, 4, 4)[index])
        return pl.ds(base + ((me.z + 3 + OWN - index) % 4) * 2, 2)

    def right_copy(index):
        return remote(ext.at[0, core, piece(index)], ext.at[1, core, piece(index)],
                      right_send.at[index], right_recv.at[index], me.left)

    def share_copy(step):
        where = ext.at[1, core, piece(0)]
        return remote(where, where, share_send.at[step - 1], share_recv.at[step - 1], me.z_peer(step))

    def low_copy(part):
        return remote(ext.at[0, core, groups_of(part)], ext.at[0, core, groups_of(part, SIDE)],
                      low_send.at[part], low_recv.at[part], me.cross)

    def diag_copy(index):
        return remote(ext.at[1, core, piece(index)], ext.at[1, core, piece(index, 32)],
                      diag_send.at[index], diag_recv.at[index], me.cross)

    def pair_copy(kind, index, plane):
        if kind == 1:
            where = ext.at[0, plane, groups_of(index, SIDE)]
        else:
            where = ext.at[1, plane, piece(index, 32 if kind == 2 else 0)]
        sem = (0, PIECES, PIECES + 4)[kind] + index
        return remote(where, where, pair_send.at[sem], pair_recv.at[sem], me.partner)

    @pl.when(has_left)
    def _():
        for index in range(OWN):
            right_copy(index).start()

    @pl.when(bottom)
    def _():
        for part in range(4):
            low_copy(part).start()

    meanwhile()
    spots_go(1)

    def pass_on(index):
        @pl.when(bottom)
        def _():
            diag_copy(index).start()

        pair_copy(0, index, core).start()

    def low_here(part):
        @pl.when(top)
        def _():
            low_copy(part).wait_recv()
            pair_copy(1, part, core).start()

    @pl.when(has_right)
    def _():
        right_copy(0).wait_recv()
        for step in (2, 1, 3):
            share_copy(step).start()
        pass_on(0)

    low_here(0)
    low_here(1)

    @pl.when(has_right)
    def _():
        right_copy(1).wait_recv()
        pass_on(1)

    spots_go(2)
    low_here(2)
    low_here(3)

    @pl.when(has_right)
    def _():
        for index in ORDER_IN[2:]:
            if index < OWN:
                right_copy(index).wait_recv()
            else:
                share_copy(index - OWN + 1).wait_recv()
            pass_on(index)

    @pl.when(jnp.logical_and(top, has_right))
    def _():
        for index in ORDER_IN:
            diag_copy(index).wait_recv()
            pair_copy(2, index, core).start()

    @pl.when(has_right)
    def _():
        for index in ORDER_IN:
            pair_copy(0, index, 1 - core).wait_recv()

    @pl.when(top)
    def _():
        for part in range(4):
            pair_copy(1, part, 1 - core).wait_recv()

        @pl.when(has_right)
        def _():
            for index in ORDER_IN:
                pair_copy(2, index, 1 - core).wait_recv()

    def all_sent():
        @pl.when(has_left)
        def _():
            for index in range(OWN):
                right_copy(index).wait_send()

        @pl.when(bottom)
        def _():
            for part in range(4):
                low_copy(part).wait_send()

            @pl.when(has_right)
            def _():
                for index in range(PIECES):
                    diag_copy(index).wait_send()

        @pl.when(has_right)
        def _():
            for step in (1, 2, 3):
                share_copy(step).wait_send()
            for index in range(PIECES):
                pair_copy(0, index, core).wait_send()

        @pl.when(top)
        def _():
            for part in range(4):
                pair_copy(1, part, core).wait_send()

            @pl.when(has_right)
            def _():
                for index in range(PIECES):
                    pair_copy(2, index, core).wait_send()

    return all_sent


def spot_chain(me, spots, spot_words, spot_send, spot_recv, word_sem):
    has_right = me.col < 3
    has_left = me.col > 0
    top = me.row == 0
    bottom = me.row == 1

    def spot_copy(step):
        if step == 0:
            where = pl.ds(me.layer, 1)
            return remote(spots.at[where], spots.at[where], spot_send.at[0], spot_recv.at[0], me.partner)
        if step == 1:
            where = pl.ds(me.z * 4 + me.xh * 2, 2)
            return remote(spots.at[where], spots.at[where], spot_send.at[1], spot_recv.at[1], me.far_x)
        if step < 5:
            where = pl.ds(me.z * 4, 4)
            return remote(spots.at[where], spots.at[where], spot_send.at[step], spot_recv.at[step],
                          me.z_peer(step - 1))
        if step == 5:
            return remote(spots.at[pl.ds(0, 16)], spots.at[pl.ds(16, 16)], spot_send.at[5], spot_recv.at[5], me.right)
        return remote(spots.at[pl.ds(0, 32)], spots.at[pl.ds(32, 32)], spot_send.at[6], spot_recv.at[6], me.cross)

    near = pltpu.make_async_copy(spots.at[pl.ds(0, 16)], spot_words.at[pl.ds(0, 16)], word_sem.at[0])
    others = pltpu.make_async_copy(spots.at[pl.ds(16, 48)], spot_words.at[pl.ds(16, 48)], word_sem.at[1])

    def go(stage):
        if stage == 0:
            spot_copy(0).start()
        elif stage == 1:
            spot_copy(0).wait_recv()
            spot_copy(1).start()
        elif stage == 2:
            spot_copy(1).wait_recv()
            for step in (2, 3, 4):
                spot_copy(step).start()
        elif stage == 3:
            for step in (2, 3, 4):
                spot_copy(step).wait_recv()
            near.start()

            @pl.when(has_right)
            def _():
                spot_copy(5).start()
        elif stage == 4:
            @pl.when(has_left)
            def _():
                spot_copy(5).wait_recv()

            @pl.when(top)
            def _():
                spot_copy(6).start()
        elif stage == 5:
            @pl.when(bottom)
            def _():
                spot_copy(6).wait_recv()

            others.start()
        else:
            for step in range(5):
                spot_copy(step).wait_send()

            @pl.when(has_right)
            def _():
                spot_copy(5).wait_send()

            @pl.when(top)
            def _():
                spot_copy(6).wait_send()

    return go, near, others


def forward(mode, probe, patch, tabs, far):
    pr, pi = probe[0, mode], probe[1, mode]
    tr, ti = patch[0], patch[1]
    er = pr * tr - pi * ti
    ei = pr * ti + pi * tr
    even = side_by_side(er[:, :HALF] + er[:, HALF:], ei[:, :HALF] + ei[:, HALF:])
    odd = side_by_side(er[:, :HALF] - er[:, HALF:], ei[:, :HALF] - ei[:, HALF:])
    ye = on_lanes(even, tabs, EVEN)
    yo = on_lanes(odd, tabs, ODD)
    for parity, which in ((0, EVEN_T), (1, ODD_T)):
        if parity == 0:
            se, so = ye[:HALF] + ye[HALF:], yo[:HALF] + yo[HALF:]
        else:
            se, so = ye[:HALF] - ye[HALF:], yo[:HALF] - yo[HALF:]
        stack = on_top(side_by_side(se[:, :HALF], so[:, :HALF]), side_by_side(se[:, HALF:], so[:, HALF:]))
        far[mode, parity] = on_rows(stack, tabs, which)


def backward_rows(mode, ratio, tabs, far):
    sums = []
    for parity, which in ((0, EVEN), (1, ODD)):
        scale = ratio[parity]
        sums.append(on_rows(far[mode, parity] * on_top(scale, scale), tabs, which))
    far[mode, 0] = sums[0] + sums[1]
    far[mode, 1] = sums[0] - sums[1]


def backward_lanes(half, probe, tabs, far, block):
    even = [side_by_side(far[mode, half, :HALF, :HALF], far[mode, half, HALF:, :HALF]) for mode in range(MODES)]
    odd = [side_by_side(far[mode, half, :HALF, HALF:], far[mode, half, HALF:, HALF:]) for mode in range(MODES)]
    pe = on_lanes(jnp.concatenate(even, axis=0), tabs, EVEN_T)
    po = on_lanes(jnp.concatenate(odd, axis=0), tabs, ODD_T)
    first, second = pe + po, pe - po
    where = slice(half * HALF, half * HALF + HALF)
    cr = ci = None
    for mode in range(MODES):
        part = slice(mode * HALF, mode * HALF + HALF)
        nr = side_by_side(first[part, :HALF], second[part, :HALF])
        ni = side_by_side(first[part, HALF:], second[part, HALF:])
        pr, pi = probe[0, mode, where], probe[1, mode, where]
        tr = pr * nr + pi * ni
        ti = pr * ni - pi * nr
        cr = tr if cr is None else cr + tr
        ci = ti if ci is None else ci + ti
    block[0, where] = cr
    block[1, where] = ci


def rows_from(ref, start, count):
    group = lax.shift_right_arithmetic(start, 3)
    wide = ref[pl.ds(group, count // 8 + 1)].reshape(count + 8, SIDE)
    return pltpu.roll(wide, lax.rem(count + 8 - (start - group * 8), count + 8), 0)[:count]


def inside(value):
    return jnp.clip(value, 0, SIDE - 1)


def grouped(value):
    return value.reshape(value.shape[0] // 8, 8, SIDE)


def sort_amplitudes(amp, tabs, ratio):
    rest = amp[...]
    total = None
    for _ in range(3):
        piece = rest.astype(BF16)
        rest = rest - piece.astype(F32)
        moved = dot(dot(tabs[ORDER_T], piece).astype(BF16), tabs[ORDER])
        total = moved if total is None else total + moved
    ratio[0] = total[:HALF]
    ratio[1] = total[HALF:]


def sum_power(probe, padded, share):
    power = None
    for mode in range(MODES):
        term = probe[0, mode] * probe[0, mode] + probe[1, mode] * probe[1, mode]
        power = term if power is None else power + term
    padded[pl.ds(0, 32)] = jnp.zeros((32, 8, SIDE), F32)
    padded[pl.ds(32, 32)] = grouped(power)
    padded[pl.ds(64, 33)] = jnp.zeros((33, 8, SIDE), F32)
    share[...] = jnp.zeros_like(share)


def cut_patch(row_at, col_at, ext, patch):
    lanes = lax.broadcasted_iota(jnp.int32, (SIDE, SIDE), 1)
    back = lax.rem(SIDE - col_at, SIDE)
    for plane in range(2):
        here = pltpu.roll(rows_from(ext.at[0, plane], row_at, SIDE), back, 1)
        there = pltpu.roll(rows_from(ext.at[1, plane], row_at, SIDE), back, 1)
        patch[plane] = jnp.where(lanes < SIDE - col_at, here, there)


def make_ratio(far, ratio):
    for parity in range(2):
        seen = None
        for mode in range(MODES):
            re, im = far[mode, parity, :HALF], far[mode, parity, HALF:]
            term = re * re + im * im
            seen = term if seen is None else seen + term
        ratio[parity] = ratio[parity] / (jnp.sqrt(seen) + SOFTEN)


TOGETHER = 4


def add_spots(me, group, spots, padded, share):
    up, left = group // 2, group % 2
    known = jnp.logical_and(me.row >= up, me.col >= left)
    first = up * SIDE + me.z * QUART + SIDE
    row_base = (me.row - up) * SIDE
    col_base = (me.col - left) * SIDE
    lanes = lax.broadcasted_iota(jnp.int32, (QUART, SIDE), 1)

    def some(index, carry):
        total = share[...]
        for step in range(TOGETHER):
            spot = group * 16 + index * TOGETHER + step
            start = jnp.where(known, first - inside(spots[spot, 0, 0] - row_base), 0)
            turn = jnp.where(known, inside(spots[spot, 0, 1] - col_base), 0)
            turned = pltpu.roll(rows_from(padded, start, QUART), turn, 1)
            kept = lanes >= turn if left == 0 else lanes < turn
            total = total + jnp.where(kept, turned, 0.0)
        share[...] = total
        return carry

    lax.fori_loop(0, 16 // TOGETHER, some, 0)


def put_tall(value, col_at, tall):
    lanes = lax.broadcasted_iota(jnp.int32, (SIDE, SIDE), 1)
    turned = pltpu.roll(value, col_at, 1)
    tall[0, pl.ds(32, 32)] = grouped(jnp.where(lanes >= col_at, turned, 0.0))
    tall[1, pl.ds(32, 32)] = grouped(jnp.where(lanes < col_at, turned, 0.0))


def whole_kernel(
    offsets, obj_hbm, probe_hbm, amp_hbm, tabs_hbm, out,
    ext, spots, spot_words, probe, amp, tabs, patch, far, ratio, block, padded, share,
    twin_block, tall, low_sum, low_in, right_sum, right_in, total, z_in, far_in,
    load_sem, word_sem,
    h_right_send, h_right_recv, h_share_send, h_share_recv, h_low_send, h_low_recv, h_diag_send, h_diag_recv,
    h_pair_send, h_pair_recv, spot_send, spot_recv,
    pair_send, pair_recv, low_send, low_recv, right_send, right_recv,
    z_send, z_recv, far_send, far_recv, out_send, out_recv, twin_send, twin_recv,
):
    me = Place()
    core = me.core
    loads = [
        pltpu.make_async_copy(obj_hbm.at[0], ext.at[0, 0, pl.ds(0, SIDE // 8)], load_sem.at[0]),
        pltpu.make_async_copy(obj_hbm.at[1], ext.at[0, 1, pl.ds(0, SIDE // 8)], load_sem.at[1]),
        pltpu.make_async_copy(tabs_hbm, tabs, load_sem.at[2]),
        pltpu.make_async_copy(amp_hbm, amp, load_sem.at[3]),
        pltpu.make_async_copy(probe_hbm, probe, load_sem.at[4]),
    ]
    for load in loads:
        load.start()
    lanes = lax.broadcasted_iota(jnp.int32, (1, 1, 128), 2)
    line = jnp.where(lanes == 0, offsets[0, 0], jnp.where(lanes == 1, offsets[0, 1], 0))
    spots[pl.ds(me.layer, 1)] = line
    me.meet()
    loads[0].wait()
    loads[1].wait()

    def meanwhile():
        loads[2].wait()
        loads[3].wait()
        sort_amplitudes(amp, tabs, ratio)
        for source in range(2):
            for side in range(2):
                tall[source, side, pl.ds(0, 32)] = jnp.zeros((32, 8, SIDE), F32)
                tall[source, side, pl.ds(64, 33)] = jnp.zeros((33, 8, SIDE), F32)
        loads[4].wait()
        sum_power(probe, padded, share)

    spots_go, near_words, other_words = spot_chain(me, spots, spot_words, spot_send, spot_recv, word_sem)
    spots_go(0)
    halo_sent = halo(me, ext, h_right_send, h_right_recv, h_share_send, h_share_recv, h_low_send, h_low_recv,
                     h_diag_send, h_diag_recv, h_pair_send, h_pair_recv, meanwhile, spots_go)
    spots_go(3)

    row_at = inside(offsets[0, 0] - me.row * SIDE)
    col_at = inside(offsets[0, 1] - me.col * SIDE)
    cut_patch(row_at, col_at, ext, patch)
    for mode in range(MODES):
        forward(mode, probe, patch, tabs, far)
    spots_go(4)
    make_ratio(far, ratio)
    for mode in range(MODES):
        backward_rows(mode, ratio, tabs, far)
    near_words.wait()
    twin_layer = me.layer + 1 - 2 * core
    twin_row = inside(spot_words[twin_layer, 0, 0] - me.row * SIDE)
    twin_col = inside(spot_words[twin_layer, 0, 1] - me.col * SIDE)

    def pair_copy(half):
        where = pl.ds(half * HALF, HALF)
        return remote(block.at[1 - core, where], twin_block.at[where],
                      pair_send.at[half], pair_recv.at[half], me.partner)

    for half in range(2):
        backward_lanes(half, probe, tabs, far, block)
        pair_copy(half).start()
    spots_go(5)

    has_right = me.col < 3
    has_left = me.col > 0
    top = me.row == 0
    bottom = me.row == 1
    parts = [(me.z + 1 + step) % 4 for step in range(4)]

    def low_copy(side, step):
        where = rows_of(parts[step])
        return remote(low_sum.at[side, where], low_in.at[side, where],
                      low_send.at[side, step], low_recv.at[side, step], me.cross)

    def right_copy(step):
        where = rows_of(parts[step])
        return remote(right_sum.at[where], right_in.at[where], right_send.at[step], right_recv.at[step], me.right)

    def z_copy(step):
        return remote(total.at[rows_of(parts[step])], z_in.at[step], z_send.at[step], z_recv.at[step],
                      me.z_peer(step + 1))

    def far_copy(step):
        return remote(total.at[rows_of(parts[step])], far_in.at[step], far_send.at[step], far_recv.at[step],
                      me.at(z=parts[step], xh=1 - me.xh))

    put_tall(block[core], col_at, tall.at[0])
    for half in range(2):
        pair_copy(half).wait_recv()
    put_tall(twin_block[...], twin_col, tall.at[1])
    other_words.wait()

    def both(side, part, base):
        first = SIDE + base + part * QUART
        return (rows_from(tall.at[0, side], first - row_at, QUART)
                + rows_from(tall.at[1, side], first - twin_row, QUART))

    def send_low(side):
        @pl.when(top)
        def _():
            for step in range(4):
                low_sum[side, rows_of(parts[step])] = both(side, parts[step], SIDE)
                low_copy(side, step).start()

    send_low(1)
    for step in range(4):
        where = rows_of(parts[step])
        right_sum[where] = both(1, parts[step], 0)

        @pl.when(jnp.logical_and(top, has_right))
        def _():
            right_copy(step).start()

    send_low(0)
    for step in range(4):
        total[rows_of(parts[step])] = both(0, parts[step], 0)
    for group in range(2):
        add_spots(me, group, spot_words, padded, share)

    @pl.when(bottom)
    def _():
        for step in range(4):
            where = rows_of(parts[step])
            low_copy(1, step).wait_recv()
            right_sum[where] = right_sum[where] + low_in[1, where]

            @pl.when(has_right)
            def _():
                right_copy(step).start()

    for group in range(2, 4):
        add_spots(me, group, spot_words, padded, share)

    for step in range(4):
        where = rows_of(parts[step])

        @pl.when(bottom)
        def _():
            low_copy(0, step).wait_recv()
            total[where] = total[where] + low_in[0, where]

        @pl.when(has_left)
        def _():
            right_copy(step).wait_recv()
            total[where] = total[where] + right_in[where]

        if step < 3:
            z_copy(step).start()
        far_copy(step).start()

    mine = rows_of(me.z)
    for step in range(3):
        z_copy(step).wait_recv()
    near_sum = total[mine] + z_in[0] + z_in[1] + z_in[2]
    for step in range(4):
        far_copy(step).wait_recv()
    far_sum = far_in[3] + far_in[0] + far_in[1] + far_in[2]
    whole = near_sum + far_sum
    out[core, mine] = (whole + DAMPING * ext[0, core, groups_of(me.z)].reshape(QUART, SIDE)) / (share[...] + DAMPING)

    def out_copy(step):
        return remote(out.at[core, mine], out.at[core, mine], out_send.at[step], out_recv.at[step], me.z_peer(step + 1))

    def come_copy(step):
        where = out.at[core, rows_of((me.z + 3 - step) % 4)]
        return remote(where, where, out_send.at[step], out_recv.at[step], me.z_peer(step + 1))

    def twin_copy(step, plane):
        part = me.z if step == 3 else (me.z + 3 - step) % 4
        where = out.at[plane, rows_of(part)]
        return remote(where, where, twin_send.at[step], twin_recv.at[step], me.partner)

    for step in (1, 0, 2):
        out_copy(step).start()
    twin_copy(3, core).start()
    for step in (0, 2, 1):
        come_copy(step).wait_recv()
        twin_copy(step, core).start()
    for step in (3, 0, 2, 1):
        twin_copy(step, 1 - core).wait_recv()

    for half in range(2):
        pair_copy(half).wait_send()
    for step in range(4):
        twin_copy(step, core).wait_send()

        far_copy(step).wait_send()

        @pl.when(top)
        def _():
            for side in range(2):
                low_copy(side, step).wait_send()

        @pl.when(has_right)
        def _():
            right_copy(step).wait_send()

        if step < 3:
            z_copy(step).wait_send()
            out_copy(step).wait_send()
    halo_sent()
    spots_go(6)


def body(object_field, probe_modes, amplitudes, offsets):
    sems = pltpu.SemaphoreType.DMA
    return pl.pallas_call(
        whole_kernel,
        out_shape=pltpu.VMEM((2, SIDE, SIDE), F32),
        in_specs=[SMEM_SPEC] + [HBM_SPEC] * 4,
        out_specs=VMEM_SPEC,
        scratch_shapes=[
            pltpu.VMEM((2, 2, 64, 8, SIDE), F32),
            pltpu.VMEM((64, 1, 128), jnp.int32),
            pltpu.SMEM((64, 1, 128), jnp.int32),
            pltpu.VMEM((2, MODES, SIDE, SIDE), F32),
            pltpu.VMEM((SIDE, SIDE), F32),
            pltpu.VMEM((10, SIDE, SIDE), BF16),
            pltpu.VMEM((2, SIDE, SIDE), F32),
            pltpu.VMEM((MODES, 2, SIDE, SIDE), F32),
            pltpu.VMEM((2, HALF, SIDE), F32),
            pltpu.VMEM((2, SIDE, SIDE), F32),
            pltpu.VMEM((97, 8, SIDE), F32),
            pltpu.VMEM((QUART, SIDE), F32),
            pltpu.VMEM((SIDE, SIDE), F32),
            pltpu.VMEM((2, 2, 97, 8, SIDE), F32),
            pltpu.VMEM((2, SIDE, SIDE), F32),
            pltpu.VMEM((2, SIDE, SIDE), F32),
            pltpu.VMEM((SIDE, SIDE), F32),
            pltpu.VMEM((SIDE, SIDE), F32),
            pltpu.VMEM((SIDE, SIDE), F32),
            pltpu.VMEM((3, QUART, SIDE), F32),
            pltpu.VMEM((4, QUART, SIDE), F32),
            sems((5,)), sems((2,)),
            sems((OWN,)), sems((OWN,)), sems((3,)), sems((3,)), sems((4,)), sems((4,)),
            sems((PIECES,)), sems((PIECES,)), sems((2 * PIECES + 4,)), sems((2 * PIECES + 4,)), sems((7,)), sems((7,)),
            sems((2,)), sems((2,)), sems((2, 4)), sems((2, 4)), sems((4,)), sems((4,)),
            sems((3,)), sems((3,)), sems((4,)), sems((4,)), sems((3,)), sems((3,)), sems((4,)), sems((4,)),
        ],
        compiler_params=pltpu.CompilerParams(
            collective_id=0, has_side_effects=True
        ),
        name="whole",
    )(offsets, object_field.reshape(2, 32, 8, SIDE), probe_modes, amplitudes[0], jnp.asarray(tables()))


def solution(mesh):
    placed = (
        P(None, "row", "col"),
        P(),
        P(("row", "col", "layer"), None, None),
        P(("row", "col", "layer"), None),
    )
    return jax.shard_map(
        body, mesh=mesh, in_specs=placed, out_specs=P(None, "row", "col"), check_vma=False
    )
```

```python
import functools
import math

import jax
import jax.numpy as jnp
import numpy as np
from jax import lax
from jax.experimental import pallas as pl
from jax.experimental.pallas import tpu as pltpu
from jax.sharding import PartitionSpec as P

SOFTEN = 0.05
DAMPING = 0.5
MODES = 4
SIDE = 256
HALF = 128
QUART = 64
F32 = jnp.float32
BF16 = jnp.bfloat16
VMEM_SPEC = pl.BlockSpec(memory_space=pltpu.VMEM)
SMEM_SPEC = pl.BlockSpec(memory_space=pltpu.SMEM)
HBM_SPEC = pl.BlockSpec(memory_space=pltpu.HBM)


def remote(src, dst, send, recv, device):
    return pltpu.make_async_remote_copy(
        src_ref=src,
        dst_ref=dst,
        send_sem=send,
        recv_sem=recv,
        device_id=device,
        device_id_type=pl.DeviceIdType.MESH,
    )


class Place:
    def __init__(self):
        self.row = lax.axis_index("row")
        self.col = lax.axis_index("col")
        layer = lax.axis_index("layer")
        self.layer = layer
        self.z = layer // 4
        self.xh = (layer // 2) % 2
        self.core = layer % 2
        self.partner = self.at(xh=self.xh, core=1 - self.core)
        self.far_x = self.at(xh=1 - self.xh)
        self.cross_xh = (self.xh + self.core) % 2
        self.cross = {"row": 1 - self.row, "layer": self.z * 4 + self.cross_xh * 2 + self.core}
        self.left = {"col": (self.col + 3) % 4}
        self.right = {"col": (self.col + 1) % 4}

    def at(self, z=None, xh=None, core=None):
        z = self.z if z is None else z
        xh = self.xh if xh is None else xh
        core = self.core if core is None else core
        return {"layer": z * 4 + xh * 2 + core}

    def z_peer(self, step):
        return self.at(z=(self.z + step) % 4)

    def meet(self):
        barrier = pltpu.get_barrier_semaphore()
        others = [self.partner, self.far_x, self.cross, self.left, self.right]
        others += [self.z_peer(step) for step in (1, 2, 3)]
        for other in others:
            pl.semaphore_signal(barrier, inc=1, device_id=other, device_id_type=pl.DeviceIdType.MESH)
        pl.semaphore_wait(barrier, len(others))


def rows_of(part, base=0):
    return pl.ds(pl.multiple_of(base + part * QUART, QUART), QUART)


def groups_of(part, base=0):
    return pl.ds(base // 8 + part * (QUART // 8), QUART // 8)


def tables():
    steps = np.arange(HALF)
    found = []
    for odd in (0, 1):
        phase = (steps[:, None] * (2 * steps[None, :] + odd)) % SIDE
        angle = phase * (2.0 * math.pi / SIDE)
        real, imag = np.cos(angle) / 16.0, -np.sin(angle) / 16.0
        full = np.block([[real, imag], [-imag, real]]).astype(np.float32)
        for table in (full, np.ascontiguousarray(full.T)):
            high = table.astype(jnp.bfloat16)
            low = (table - high.astype(np.float32)).astype(jnp.bfloat16)
            found += [high, low]
    order = np.zeros((SIDE, SIDE), np.float32)
    order[2 * steps, steps] = 1.0
    order[2 * steps + 1, HALF + steps] = 1.0
    found += [order.astype(jnp.bfloat16), np.ascontiguousarray(order.T).astype(jnp.bfloat16)]
    return np.stack(found)


EVEN, EVEN_T, ODD, ODD_T, ORDER, ORDER_T = 0, 2, 4, 6, 8, 9


def dot(left, right):
    return jnp.dot(left, right, preferred_element_type=F32)


def split(value):
    high = value.astype(BF16)
    return high, (value - high.astype(F32)).astype(BF16)


def on_lanes(value, tabs, which):
    high, low = split(value)
    return dot(high, tabs[which]) + dot(low, tabs[which]) + dot(high, tabs[which + 1])


def on_rows(value, tabs, which):
    high, low = split(value)
    return dot(tabs[which], high) + dot(tabs[which], low) + dot(tabs[which + 1], high)


def side_by_side(left, right):
    return jnp.concatenate([left, right], axis=1)


def on_top(upper, lower):
    return jnp.concatenate([upper, lower], axis=0)


OWN = 5
PIECES = 6
ORDER_IN = (0, 1, 2, 3, 4, 5)


def halo(me, ext, right_send, right_recv, share_send, share_recv, low_send, low_recv, diag_send, diag_recv,
         pair_send, pair_recv, meanwhile, spots_go):
    core = me.core
    has_right = me.col < 3
    has_left = me.col > 0
    top = me.row == 0
    bottom = me.row == 1

    odd = me.z % 2
    z_mate = me.at(z=me.z + 1 - 2 * odd)

    def piece(index, base=0):
        if index == 0:
            return pl.ds(base + odd * 6, 6)
        if index < OWN:
            return pl.ds(base + (0, 12, 20, 26, 30)[index], (0, 8, 6, 4, 2)[index])
        return pl.ds(base + (1 - odd) * 6, 6)

    def right_copy(index):
        return remote(ext.at[0, core, piece(index)], ext.at[1, core, piece(index)],
                      right_send.at[index], right_recv.at[index], me.left)

    def share_copy():
        where = ext.at[1, core, piece(0)]
        return remote(where, where, share_send.at[0], share_recv.at[0], z_mate)

    def low_copy(part):
        return remote(ext.at[0, core, groups_of(part)], ext.at[0, core, groups_of(part, SIDE)],
                      low_send.at[part], low_recv.at[part], me.cross)

    def diag_copy(index):
        return remote(ext.at[1, core, piece(index)], ext.at[1, core, piece(index, 32)],
                      diag_send.at[index], diag_recv.at[index], me.cross)

    def pair_copy(kind, index, plane):
        if kind == 1:
            where = ext.at[0, plane, groups_of(index, SIDE)]
        else:
            where = ext.at[1, plane, piece(index, 32 if kind == 2 else 0)]
        sem = (0, PIECES, PIECES + 4)[kind] + index
        return remote(where, where, pair_send.at[sem], pair_recv.at[sem], me.partner)

    @pl.when(has_left)
    def _():
        for index in range(OWN):
            right_copy(index).start()

    @pl.when(bottom)
    def _():
        for part in range(4):
            low_copy(part).start()

    meanwhile()
    spots_go(1)

    def pass_on(index):
        @pl.when(bottom)
        def _():
            diag_copy(index).start()

        pair_copy(0, index, core).start()

    def low_here(part):
        @pl.when(top)
        def _():
            low_copy(part).wait_recv()
            pair_copy(1, part, core).start()

    @pl.when(has_right)
    def _():
        right_copy(0).wait_recv()
        share_copy().start()
        pass_on(0)

    low_here(0)
    low_here(1)

    @pl.when(has_right)
    def _():
        right_copy(1).wait_recv()
        pass_on(1)

    spots_go(2)
    low_here(2)
    low_here(3)

    @pl.when(has_right)
    def _():
        for index in ORDER_IN[2:]:
            if index < OWN:
                right_copy(index).wait_recv()
            else:
                share_copy().wait_recv()
            pass_on(index)

    @pl.when(jnp.logical_and(top, has_right))
    def _():
        for index in ORDER_IN:
            diag_copy(index).wait_recv()
            pair_copy(2, index, core).start()

    @pl.when(has_right)
    def _():
        for index in ORDER_IN:
            pair_copy(0, index, 1 - core).wait_recv()

    @pl.when(top)
    def _():
        for part in range(4):
            pair_copy(1, part, 1 - core).wait_recv()

        @pl.when(has_right)
        def _():
            for index in ORDER_IN:
                pair_copy(2, index, 1 - core).wait_recv()

    def all_sent():
        @pl.when(has_left)
        def _():
            for index in range(OWN):
                right_copy(index).wait_send()

        @pl.when(bottom)
        def _():
            for part in range(4):
                low_copy(part).wait_send()

            @pl.when(has_right)
            def _():
                for index in range(PIECES):
                    diag_copy(index).wait_send()

        @pl.when(has_right)
        def _():
            share_copy().wait_send()
            for index in range(PIECES):
                pair_copy(0, index, core).wait_send()

        @pl.when(top)
        def _():
            for part in range(4):
                pair_copy(1, part, core).wait_send()

            @pl.when(has_right)
            def _():
                for index in range(PIECES):
                    pair_copy(2, index, core).wait_send()

    return all_sent


def spot_chain(me, spots, spot_words, spot_send, spot_recv, word_sem):
    has_right = me.col < 3
    has_left = me.col > 0
    top = me.row == 0
    bottom = me.row == 1

    def spot_copy(step):
        if step == 0:
            where = pl.ds(me.layer, 1)
            return remote(spots.at[where], spots.at[where], spot_send.at[0], spot_recv.at[0], me.partner)
        if step == 1:
            where = pl.ds(me.z * 4 + me.xh * 2, 2)
            return remote(spots.at[where], spots.at[where], spot_send.at[1], spot_recv.at[1], me.far_x)
        if step < 5:
            where = pl.ds(me.z * 4, 4)
            return remote(spots.at[where], spots.at[where], spot_send.at[step], spot_recv.at[step],
                          me.z_peer(step - 1))
        if step == 5:
            return remote(spots.at[pl.ds(0, 16)], spots.at[pl.ds(16, 16)], spot_send.at[5], spot_recv.at[5], me.right)
        return remote(spots.at[pl.ds(0, 32)], spots.at[pl.ds(32, 32)], spot_send.at[6], spot_recv.at[6], me.cross)

    near = pltpu.make_async_copy(spots.at[pl.ds(0, 16)], spot_words.at[pl.ds(0, 16)], word_sem.at[0])
    others = pltpu.make_async_copy(spots.at[pl.ds(16, 48)], spot_words.at[pl.ds(16, 48)], word_sem.at[1])

    def go(stage):
        if stage == 0:
            spot_copy(0).start()
        elif stage == 1:
            spot_copy(0).wait_recv()
            spot_copy(1).start()
        elif stage == 2:
            spot_copy(1).wait_recv()
            for step in (2, 3, 4):
                spot_copy(step).start()
        elif stage == 3:
            for step in (2, 3, 4):
                spot_copy(step).wait_recv()
            near.start()

            @pl.when(has_right)
            def _():
                spot_copy(5).start()
        elif stage == 4:
            @pl.when(has_left)
            def _():
                spot_copy(5).wait_recv()

            @pl.when(top)
            def _():
                spot_copy(6).start()
        elif stage == 5:
            @pl.when(bottom)
            def _():
                spot_copy(6).wait_recv()

            others.start()
        else:
            for step in range(5):
                spot_copy(step).wait_send()

            @pl.when(has_right)
            def _():
                spot_copy(5).wait_send()

            @pl.when(top)
            def _():
                spot_copy(6).wait_send()

    return go, near, others


def forward(mode, probe, patch, tabs, far):
    pr, pi = probe[0, mode], probe[1, mode]
    tr, ti = patch[0], patch[1]
    er = pr * tr - pi * ti
    ei = pr * ti + pi * tr
    even = side_by_side(er[:, :HALF] + er[:, HALF:], ei[:, :HALF] + ei[:, HALF:])
    odd = side_by_side(er[:, :HALF] - er[:, HALF:], ei[:, :HALF] - ei[:, HALF:])
    ye = on_lanes(even, tabs, EVEN)
    yo = on_lanes(odd, tabs, ODD)
    for parity, which in ((0, EVEN_T), (1, ODD_T)):
        if parity == 0:
            se, so = ye[:HALF] + ye[HALF:], yo[:HALF] + yo[HALF:]
        else:
            se, so = ye[:HALF] - ye[HALF:], yo[:HALF] - yo[HALF:]
        stack = on_top(side_by_side(se[:, :HALF], so[:, :HALF]), side_by_side(se[:, HALF:], so[:, HALF:]))
        far[mode, parity] = on_rows(stack, tabs, which)


def backward_rows(mode, ratio, tabs, far):
    sums = []
    for parity, which in ((0, EVEN), (1, ODD)):
        scale = ratio[parity]
        sums.append(on_rows(far[mode, parity] * on_top(scale, scale), tabs, which))
    far[mode, 0] = sums[0] + sums[1]
    far[mode, 1] = sums[0] - sums[1]


def backward_lanes(half, probe, tabs, far, block):
    even = [side_by_side(far[mode, half, :HALF, :HALF], far[mode, half, HALF:, :HALF]) for mode in range(MODES)]
    odd = [side_by_side(far[mode, half, :HALF, HALF:], far[mode, half, HALF:, HALF:]) for mode in range(MODES)]
    pe = on_lanes(jnp.concatenate(even, axis=0), tabs, EVEN_T)
    po = on_lanes(jnp.concatenate(odd, axis=0), tabs, ODD_T)
    first, second = pe + po, pe - po
    where = slice(half * HALF, half * HALF + HALF)
    cr = ci = None
    for mode in range(MODES):
        part = slice(mode * HALF, mode * HALF + HALF)
        nr = side_by_side(first[part, :HALF], second[part, :HALF])
        ni = side_by_side(first[part, HALF:], second[part, HALF:])
        pr, pi = probe[0, mode, where], probe[1, mode, where]
        tr = pr * nr + pi * ni
        ti = pr * ni - pi * nr
        cr = tr if cr is None else cr + tr
        ci = ti if ci is None else ci + ti
    block[0, where] = cr
    block[1, where] = ci


def rows_from(ref, start, count):
    group = lax.shift_right_arithmetic(start, 3)
    wide = ref[pl.ds(group, count // 8 + 1)].reshape(count + 8, SIDE)
    return pltpu.roll(wide, lax.rem(count + 8 - (start - group * 8), count + 8), 0)[:count]


def inside(value):
    return jnp.clip(value, 0, SIDE - 1)


def grouped(value):
    return value.reshape(value.shape[0] // 8, 8, SIDE)


def sort_amplitudes(amp, tabs, ratio):
    rest = amp[...]
    total = None
    for _ in range(3):
        piece = rest.astype(BF16)
        rest = rest - piece.astype(F32)
        moved = dot(dot(tabs[ORDER_T], piece).astype(BF16), tabs[ORDER])
        total = moved if total is None else total + moved
    ratio[0] = total[:HALF]
    ratio[1] = total[HALF:]


def sum_power(probe, padded, share):
    power = None
    for mode in range(MODES):
        term = probe[0, mode] * probe[0, mode] + probe[1, mode] * probe[1, mode]
        power = term if power is None else power + term
    padded[pl.ds(0, 32)] = jnp.zeros((32, 8, SIDE), F32)
    padded[pl.ds(32, 32)] = grouped(power)
    padded[pl.ds(64, 33)] = jnp.zeros((33, 8, SIDE), F32)
    share[...] = jnp.zeros_like(share)


def cut_patch(row_at, col_at, ext, patch):
    lanes = lax.broadcasted_iota(jnp.int32, (SIDE, SIDE), 1)
    back = lax.rem(SIDE - col_at, SIDE)
    for plane in range(2):
        here = pltpu.roll(rows_from(ext.at[0, plane], row_at, SIDE), back, 1)
        there = pltpu.roll(rows_from(ext.at[1, plane], row_at, SIDE), back, 1)
        patch[plane] = jnp.where(lanes < SIDE - col_at, here, there)


def make_ratio(far, ratio):
    for parity in range(2):
        seen = None
        for mode in range(MODES):
            re, im = far[mode, parity, :HALF], far[mode, parity, HALF:]
            term = re * re + im * im
            seen = term if seen is None else seen + term
        ratio[parity] = ratio[parity] / (jnp.sqrt(seen) + SOFTEN)


TOGETHER = 4


def add_spots(me, group, spots, padded, share):
    up, left = group // 2, group % 2
    known = jnp.logical_and(me.row >= up, me.col >= left)
    first = up * SIDE + me.z * QUART + SIDE
    row_base = (me.row - up) * SIDE
    col_base = (me.col - left) * SIDE
    lanes = lax.broadcasted_iota(jnp.int32, (QUART, SIDE), 1)

    def some(index, carry):
        total = share[...]
        for step in range(TOGETHER):
            spot = group * 16 + index * TOGETHER + step
            start = jnp.where(known, first - inside(spots[spot, 0, 0] - row_base), 0)
            turn = jnp.where(known, inside(spots[spot, 0, 1] - col_base), 0)
            turned = pltpu.roll(rows_from(padded, start, QUART), turn, 1)
            kept = lanes >= turn if left == 0 else lanes < turn
            total = total + jnp.where(kept, turned, 0.0)
        share[...] = total
        return carry

    lax.fori_loop(0, 16 // TOGETHER, some, 0)


def put_tall(value, col_at, tall):
    lanes = lax.broadcasted_iota(jnp.int32, (SIDE, SIDE), 1)
    turned = pltpu.roll(value, col_at, 1)
    tall[0, pl.ds(32, 32)] = grouped(jnp.where(lanes >= col_at, turned, 0.0))
    tall[1, pl.ds(32, 32)] = grouped(jnp.where(lanes < col_at, turned, 0.0))


def whole_kernel(
    offsets, obj_hbm, probe_hbm, amp_hbm, tabs_hbm, out,
    ext, spots, spot_words, probe, amp, tabs, patch, far, ratio, block, padded, share,
    twin_block, tall, low_sum, low_in, right_sum, right_in, total, z_in, far_in,
    load_sem, word_sem,
    h_right_send, h_right_recv, h_share_send, h_share_recv, h_low_send, h_low_recv, h_diag_send, h_diag_recv,
    h_pair_send, h_pair_recv, spot_send, spot_recv,
    pair_send, pair_recv, low_send, low_recv, right_send, right_recv,
    z_send, z_recv, far_send, far_recv, out_send, out_recv, twin_send, twin_recv,
):
    me = Place()
    core = me.core
    loads = [
        pltpu.make_async_copy(obj_hbm.at[0], ext.at[0, 0, pl.ds(0, SIDE // 8)], load_sem.at[0]),
        pltpu.make_async_copy(obj_hbm.at[1], ext.at[0, 1, pl.ds(0, SIDE // 8)], load_sem.at[1]),
        pltpu.make_async_copy(tabs_hbm, tabs, load_sem.at[2]),
        pltpu.make_async_copy(amp_hbm, amp, load_sem.at[3]),
        pltpu.make_async_copy(probe_hbm, probe, load_sem.at[4]),
    ]
    for load in loads:
        load.start()
    lanes = lax.broadcasted_iota(jnp.int32, (1, 1, 128), 2)
    line = jnp.where(lanes == 0, offsets[0, 0], jnp.where(lanes == 1, offsets[0, 1], 0))
    spots[pl.ds(me.layer, 1)] = line
    me.meet()
    loads[0].wait()
    loads[1].wait()

    def meanwhile():
        loads[2].wait()
        loads[3].wait()
        sort_amplitudes(amp, tabs, ratio)
        for source in range(2):
            for side in range(2):
                tall[source, side, pl.ds(0, 32)] = jnp.zeros((32, 8, SIDE), F32)
                tall[source, side, pl.ds(64, 33)] = jnp.zeros((33, 8, SIDE), F32)
        loads[4].wait()
        sum_power(probe, padded, share)

    spots_go, near_words, other_words = spot_chain(me, spots, spot_words, spot_send, spot_recv, word_sem)
    spots_go(0)
    halo_sent = halo(me, ext, h_right_send, h_right_recv, h_share_send, h_share_recv, h_low_send, h_low_recv,
                     h_diag_send, h_diag_recv, h_pair_send, h_pair_recv, meanwhile, spots_go)
    spots_go(3)

    row_at = inside(offsets[0, 0] - me.row * SIDE)
    col_at = inside(offsets[0, 1] - me.col * SIDE)
    cut_patch(row_at, col_at, ext, patch)
    for mode in range(MODES):
        forward(mode, probe, patch, tabs, far)
    spots_go(4)
    make_ratio(far, ratio)
    for mode in range(MODES):
        backward_rows(mode, ratio, tabs, far)
    near_words.wait()
    twin_layer = me.layer + 1 - 2 * core
    twin_row = inside(spot_words[twin_layer, 0, 0] - me.row * SIDE)
    twin_col = inside(spot_words[twin_layer, 0, 1] - me.col * SIDE)

    def pair_copy(half):
        where = pl.ds(half * HALF, HALF)
        return remote(block.at[1 - core, where], twin_block.at[where],
                      pair_send.at[half], pair_recv.at[half], me.partner)

    for half in range(2):
        backward_lanes(half, probe, tabs, far, block)
        pair_copy(half).start()
    spots_go(5)

    has_right = me.col < 3
    has_left = me.col > 0
    top = me.row == 0
    bottom = me.row == 1
    parts = [(me.z + 1 + step) % 4 for step in range(4)]

    def low_copy(side, step):
        where = rows_of(parts[step])
        return remote(low_sum.at[side, where], low_in.at[side, where],
                      low_send.at[side, step], low_recv.at[side, step], me.cross)

    def right_copy(step):
        where = rows_of(parts[step])
        return remote(right_sum.at[where], right_in.at[where], right_send.at[step], right_recv.at[step], me.right)

    def z_copy(step):
        return remote(total.at[rows_of(parts[step])], z_in.at[step], z_send.at[step], z_recv.at[step],
                      me.z_peer(step + 1))

    def far_copy(step):
        return remote(total.at[rows_of(parts[step])], far_in.at[step], far_send.at[step], far_recv.at[step],
                      me.at(z=parts[step], xh=1 - me.xh))

    put_tall(block[core], col_at, tall.at[0])
    for half in range(2):
        pair_copy(half).wait_recv()
    put_tall(twin_block[...], twin_col, tall.at[1])
    other_words.wait()

    def both(side, part, base):
        first = SIDE + base + part * QUART
        return (rows_from(tall.at[0, side], first - row_at, QUART)
                + rows_from(tall.at[1, side], first - twin_row, QUART))

    def send_low(side):
        @pl.when(top)
        def _():
            for step in range(4):
                low_sum[side, rows_of(parts[step])] = both(side, parts[step], SIDE)
                low_copy(side, step).start()

    send_low(1)
    for step in range(4):
        where = rows_of(parts[step])
        right_sum[where] = both(1, parts[step], 0)

        @pl.when(jnp.logical_and(top, has_right))
        def _():
            right_copy(step).start()

    send_low(0)
    for step in range(4):
        total[rows_of(parts[step])] = both(0, parts[step], 0)
    for group in range(2):
        add_spots(me, group, spot_words, padded, share)

    @pl.when(bottom)
    def _():
        for step in range(4):
            where = rows_of(parts[step])
            low_copy(1, step).wait_recv()
            right_sum[where] = right_sum[where] + low_in[1, where]

            @pl.when(has_right)
            def _():
                right_copy(step).start()

    for group in range(2, 4):
        add_spots(me, group, spot_words, padded, share)

    for step in range(4):
        where = rows_of(parts[step])

        @pl.when(bottom)
        def _():
            low_copy(0, step).wait_recv()
            total[where] = total[where] + low_in[0, where]

        @pl.when(has_left)
        def _():
            right_copy(step).wait_recv()
            total[where] = total[where] + right_in[where]

        if step < 3:
            z_copy(step).start()
        far_copy(step).start()

    mine = rows_of(me.z)
    for step in range(3):
        z_copy(step).wait_recv()
    near_sum = total[mine] + z_in[0] + z_in[1] + z_in[2]
    for step in range(4):
        far_copy(step).wait_recv()
    far_sum = far_in[3] + far_in[0] + far_in[1] + far_in[2]
    whole = near_sum + far_sum
    out[core, mine] = (whole + DAMPING * ext[0, core, groups_of(me.z)].reshape(QUART, SIDE)) / (share[...] + DAMPING)

    def out_copy(step):
        return remote(out.at[core, mine], out.at[core, mine], out_send.at[step], out_recv.at[step], me.z_peer(step + 1))

    def come_copy(step):
        where = out.at[core, rows_of((me.z + 3 - step) % 4)]
        return remote(where, where, out_send.at[step], out_recv.at[step], me.z_peer(step + 1))

    def twin_copy(step, plane):
        part = me.z if step == 3 else (me.z + 3 - step) % 4
        where = out.at[plane, rows_of(part)]
        return remote(where, where, twin_send.at[step], twin_recv.at[step], me.partner)

    for step in (1, 0, 2):
        out_copy(step).start()
    twin_copy(3, core).start()
    for step in (0, 2, 1):
        come_copy(step).wait_recv()
        twin_copy(step, core).start()
    for step in (3, 0, 2, 1):
        twin_copy(step, 1 - core).wait_recv()

    for half in range(2):
        pair_copy(half).wait_send()
    for step in range(4):
        twin_copy(step, core).wait_send()

        far_copy(step).wait_send()

        @pl.when(top)
        def _():
            for side in range(2):
                low_copy(side, step).wait_send()

        @pl.when(has_right)
        def _():
            right_copy(step).wait_send()

        if step < 3:
            z_copy(step).wait_send()
            out_copy(step).wait_send()
    halo_sent()
    spots_go(6)


def body(object_field, probe_modes, amplitudes, offsets):
    sems = pltpu.SemaphoreType.DMA
    return pl.pallas_call(
        whole_kernel,
        out_shape=pltpu.VMEM((2, SIDE, SIDE), F32),
        in_specs=[SMEM_SPEC] + [HBM_SPEC] * 4,
        out_specs=VMEM_SPEC,
        scratch_shapes=[
            pltpu.VMEM((2, 2, 64, 8, SIDE), F32),
            pltpu.VMEM((64, 1, 128), jnp.int32),
            pltpu.SMEM((64, 1, 128), jnp.int32),
            pltpu.VMEM((2, MODES, SIDE, SIDE), F32),
            pltpu.VMEM((SIDE, SIDE), F32),
            pltpu.VMEM((10, SIDE, SIDE), BF16),
            pltpu.VMEM((2, SIDE, SIDE), F32),
            pltpu.VMEM((MODES, 2, SIDE, SIDE), F32),
            pltpu.VMEM((2, HALF, SIDE), F32),
            pltpu.VMEM((2, SIDE, SIDE), F32),
            pltpu.VMEM((97, 8, SIDE), F32),
            pltpu.VMEM((QUART, SIDE), F32),
            pltpu.VMEM((SIDE, SIDE), F32),
            pltpu.VMEM((2, 2, 97, 8, SIDE), F32),
            pltpu.VMEM((2, SIDE, SIDE), F32),
            pltpu.VMEM((2, SIDE, SIDE), F32),
            pltpu.VMEM((SIDE, SIDE), F32),
            pltpu.VMEM((SIDE, SIDE), F32),
            pltpu.VMEM((SIDE, SIDE), F32),
            pltpu.VMEM((3, QUART, SIDE), F32),
            pltpu.VMEM((4, QUART, SIDE), F32),
            sems((5,)), sems((2,)),
            sems((OWN,)), sems((OWN,)), sems((1,)), sems((1,)), sems((4,)), sems((4,)),
            sems((PIECES,)), sems((PIECES,)), sems((2 * PIECES + 4,)), sems((2 * PIECES + 4,)), sems((7,)), sems((7,)),
            sems((2,)), sems((2,)), sems((2, 4)), sems((2, 4)), sems((4,)), sems((4,)),
            sems((3,)), sems((3,)), sems((4,)), sems((4,)), sems((3,)), sems((3,)), sems((4,)), sems((4,)),
        ],
        compiler_params=pltpu.CompilerParams(
            collective_id=0, has_side_effects=True
        ),
        name="whole",
    )(offsets, object_field.reshape(2, 32, 8, SIDE), probe_modes, amplitudes[0], jnp.asarray(tables()))


def solution(mesh):
    placed = (
        P(None, "row", "col"),
        P(),
        P(("row", "col", "layer"), None, None),
        P(("row", "col", "layer"), None),
    )
    return jax.shard_map(
        body, mesh=mesh, in_specs=placed, out_specs=P(None, "row", "col"), check_vma=False
    )
```

```python
import functools
import math

import jax
import jax.numpy as jnp
import numpy as np
from jax import lax
from jax.experimental import pallas as pl
from jax.experimental.pallas import tpu as pltpu
from jax.sharding import PartitionSpec as P

SOFTEN = 0.05
DAMPING = 0.5
MODES = 4
SIDE = 256
HALF = 128
QUART = 64
EIGHTH = 32
F32 = jnp.float32
BF16 = jnp.bfloat16
VMEM_SPEC = pl.BlockSpec(memory_space=pltpu.VMEM)
SMEM_SPEC = pl.BlockSpec(memory_space=pltpu.SMEM)
HBM_SPEC = pl.BlockSpec(memory_space=pltpu.HBM)


def remote(src, dst, send, recv, device):
    return pltpu.make_async_remote_copy(
        src_ref=src,
        dst_ref=dst,
        send_sem=send,
        recv_sem=recv,
        device_id=device,
        device_id_type=pl.DeviceIdType.MESH,
    )


class Place:
    def __init__(self):
        self.row = lax.axis_index("row")
        self.col = lax.axis_index("col")
        layer = lax.axis_index("layer")
        self.layer = layer
        self.z = layer // 4
        self.xh = (layer // 2) % 2
        self.core = layer % 2
        self.partner = self.at(xh=self.xh, core=1 - self.core)
        self.far_x = self.at(xh=1 - self.xh)
        self.far_twin = self.at(xh=1 - self.xh, core=1 - self.core)
        self.cross_xh = (self.xh + self.core) % 2
        self.cross = {"row": 1 - self.row, "layer": self.z * 4 + self.cross_xh * 2 + self.core}
        self.left = {"col": (self.col + 3) % 4}
        self.right = {"col": (self.col + 1) % 4}

    def at(self, z=None, xh=None, core=None):
        z = self.z if z is None else z
        xh = self.xh if xh is None else xh
        core = self.core if core is None else core
        return {"layer": z * 4 + xh * 2 + core}

    def z_peer(self, step):
        return self.at(z=(self.z + step) % 4)

    def meet(self):
        barrier = pltpu.get_barrier_semaphore()
        others = [self.partner, self.far_x, self.far_twin, self.cross, self.left, self.right]
        others += [self.z_peer(step) for step in (1, 2, 3)]
        for other in others:
            pl.semaphore_signal(barrier, inc=1, device_id=other, device_id_type=pl.DeviceIdType.MESH)
        pl.semaphore_wait(barrier, len(others))


def rows_of(part, base=0):
    return pl.ds(pl.multiple_of(base + part * QUART, QUART), QUART)


def groups_of(part, base=0):
    return pl.ds(base // 8 + part * (QUART // 8), QUART // 8)


def tables():
    steps = np.arange(HALF)
    found = []
    for odd in (0, 1):
        phase = (steps[:, None] * (2 * steps[None, :] + odd)) % SIDE
        angle = phase * (2.0 * math.pi / SIDE)
        real, imag = np.cos(angle) / 16.0, -np.sin(angle) / 16.0
        full = np.block([[real, imag], [-imag, real]]).astype(np.float32)
        for table in (full, np.ascontiguousarray(full.T)):
            high = table.astype(jnp.bfloat16)
            low = (table - high.astype(np.float32)).astype(jnp.bfloat16)
            found += [high, low]
    order = np.zeros((SIDE, SIDE), np.float32)
    order[2 * steps, steps] = 1.0
    order[2 * steps + 1, HALF + steps] = 1.0
    found += [order.astype(jnp.bfloat16), np.ascontiguousarray(order.T).astype(jnp.bfloat16)]
    return np.stack(found)


EVEN, EVEN_T, ODD, ODD_T, ORDER, ORDER_T = 0, 2, 4, 6, 8, 9


def dot(left, right):
    return jnp.dot(left, right, preferred_element_type=F32)


def split(value):
    high = value.astype(BF16)
    return high, (value - high.astype(F32)).astype(BF16)


def on_lanes(value, tabs, which):
    high, low = split(value)
    return dot(high, tabs[which]) + dot(low, tabs[which]) + dot(high, tabs[which + 1])


def on_rows(value, tabs, which):
    high, low = split(value)
    return dot(tabs[which], high) + dot(tabs[which], low) + dot(tabs[which + 1], high)


def side_by_side(left, right):
    return jnp.concatenate([left, right], axis=1)


def on_top(upper, lower):
    return jnp.concatenate([upper, lower], axis=0)


OWN = 5
PIECES = 6
ORDER_IN = (0, 1, 2, 3, 4, 5)


def halo(me, ext, right_send, right_recv, share_send, share_recv, low_send, low_recv, diag_send, diag_recv,
         pair_send, pair_recv, meanwhile, spots_go):
    core = me.core
    has_right = me.col < 3
    has_left = me.col > 0
    top = me.row == 0
    bottom = me.row == 1

    odd = me.z % 2
    z_mate = me.at(z=me.z + 1 - 2 * odd)

    def piece(index, base=0):
        if index == 0:
            return pl.ds(base + odd * 6, 6)
        if index < OWN:
            return pl.ds(base + (0, 12, 20, 26, 30)[index], (0, 8, 6, 4, 2)[index])
        return pl.ds(base + (1 - odd) * 6, 6)

    def right_copy(index):
        return remote(ext.at[0, core, piece(index)], ext.at[1, core, piece(index)],
                      right_send.at[index], right_recv.at[index], me.left)

    def share_copy():
        where = ext.at[1, core, piece(0)]
        return remote(where, where, share_send.at[0], share_recv.at[0], z_mate)

    def low_copy(part):
        return remote(ext.at[0, core, groups_of(part)], ext.at[0, core, groups_of(part, SIDE)],
                      low_send.at[part], low_recv.at[part], me.cross)

    def diag_copy(index):
        return remote(ext.at[1, core, piece(index)], ext.at[1, core, piece(index, 32)],
                      diag_send.at[index], diag_recv.at[index], me.cross)

    def pair_copy(kind, index, plane):
        if kind == 1:
            where = ext.at[0, plane, groups_of(index, SIDE)]
        else:
            where = ext.at[1, plane, piece(index, 32 if kind == 2 else 0)]
        sem = (0, PIECES, PIECES + 4)[kind] + index
        return remote(where, where, pair_send.at[sem], pair_recv.at[sem], me.partner)

    @pl.when(has_left)
    def _():
        for index in range(OWN):
            right_copy(index).start()

    @pl.when(bottom)
    def _():
        for part in range(4):
            low_copy(part).start()

    meanwhile()

    def pass_on(index):
        @pl.when(bottom)
        def _():
            diag_copy(index).start()

        pair_copy(0, index, core).start()

    def low_here(part):
        @pl.when(top)
        def _():
            low_copy(part).wait_recv()
            pair_copy(1, part, core).start()

    @pl.when(has_right)
    def _():
        right_copy(0).wait_recv()
        share_copy().start()
        pass_on(0)

    low_here(0)
    low_here(1)

    @pl.when(has_right)
    def _():
        right_copy(1).wait_recv()
        pass_on(1)

    spots_go(2)
    low_here(2)
    low_here(3)

    @pl.when(has_right)
    def _():
        for index in ORDER_IN[2:]:
            if index < OWN:
                right_copy(index).wait_recv()
            else:
                share_copy().wait_recv()
            pass_on(index)

    @pl.when(jnp.logical_and(top, has_right))
    def _():
        for index in ORDER_IN:
            diag_copy(index).wait_recv()
            pair_copy(2, index, core).start()

    @pl.when(has_right)
    def _():
        for index in ORDER_IN:
            pair_copy(0, index, 1 - core).wait_recv()

    @pl.when(top)
    def _():
        for part in range(4):
            pair_copy(1, part, 1 - core).wait_recv()

        @pl.when(has_right)
        def _():
            for index in ORDER_IN:
                pair_copy(2, index, 1 - core).wait_recv()

    def all_sent():
        @pl.when(has_left)
        def _():
            for index in range(OWN):
                right_copy(index).wait_send()

        @pl.when(bottom)
        def _():
            for part in range(4):
                low_copy(part).wait_send()

            @pl.when(has_right)
            def _():
                for index in range(PIECES):
                    diag_copy(index).wait_send()

        @pl.when(has_right)
        def _():
            share_copy().wait_send()
            for index in range(PIECES):
                pair_copy(0, index, core).wait_send()

        @pl.when(top)
        def _():
            for part in range(4):
                pair_copy(1, part, core).wait_send()

            @pl.when(has_right)
            def _():
                for index in range(PIECES):
                    pair_copy(2, index, core).wait_send()

    return all_sent


def spot_chain(me, spots, spot_words, spot_send, spot_recv, word_sem):
    has_right = me.col < 3
    has_left = me.col > 0
    top = me.row == 0
    bottom = me.row == 1

    def spot_copy(step):
        if step in (0, 1, 7):
            where = pl.ds(me.layer, 1)
            other = {0: me.partner, 1: me.far_x, 7: me.far_twin}[step]
            return remote(spots.at[where], spots.at[where], spot_send.at[step], spot_recv.at[step], other)
        if step < 5:
            where = pl.ds(me.z * 4, 4)
            return remote(spots.at[where], spots.at[where], spot_send.at[step], spot_recv.at[step],
                          me.z_peer(step - 1))
        if step == 5:
            return remote(spots.at[pl.ds(0, 16)], spots.at[pl.ds(16, 16)], spot_send.at[5], spot_recv.at[5], me.right)
        return remote(spots.at[pl.ds(0, 32)], spots.at[pl.ds(32, 32)], spot_send.at[6], spot_recv.at[6], me.cross)

    near = pltpu.make_async_copy(spots.at[pl.ds(0, 16)], spot_words.at[pl.ds(0, 16)], word_sem.at[0])
    others = pltpu.make_async_copy(spots.at[pl.ds(16, 48)], spot_words.at[pl.ds(16, 48)], word_sem.at[1])

    def go(stage):
        if stage == 0:
            for step in (1, 7, 0):
                spot_copy(step).start()
        elif stage == 2:
            for step in (0, 1, 7):
                spot_copy(step).wait_recv()
            for step in (2, 3, 4):
                spot_copy(step).start()
        elif stage == 3:
            for step in (2, 3, 4):
                spot_copy(step).wait_recv()
            near.start()

            @pl.when(has_right)
            def _():
                spot_copy(5).start()
        elif stage == 4:
            @pl.when(has_left)
            def _():
                spot_copy(5).wait_recv()

            @pl.when(top)
            def _():
                spot_copy(6).start()
        elif stage == 5:
            @pl.when(bottom)
            def _():
                spot_copy(6).wait_recv()

            others.start()
        else:
            for step in (0, 1, 2, 3, 4, 7):
                spot_copy(step).wait_send()

            @pl.when(has_right)
            def _():
                spot_copy(5).wait_send()

            @pl.when(top)
            def _():
                spot_copy(6).wait_send()

    return go, near, others


def forward(mode, probe, patch, tabs, far):
    pr, pi = probe[0, mode], probe[1, mode]
    tr, ti = patch[0], patch[1]
    er = pr * tr - pi * ti
    ei = pr * ti + pi * tr
    even = side_by_side(er[:, :HALF] + er[:, HALF:], ei[:, :HALF] + ei[:, HALF:])
    odd = side_by_side(er[:, :HALF] - er[:, HALF:], ei[:, :HALF] - ei[:, HALF:])
    ye = on_lanes(even, tabs, EVEN)
    yo = on_lanes(odd, tabs, ODD)
    for parity, which in ((0, EVEN_T), (1, ODD_T)):
        if parity == 0:
            se, so = ye[:HALF] + ye[HALF:], yo[:HALF] + yo[HALF:]
        else:
            se, so = ye[:HALF] - ye[HALF:], yo[:HALF] - yo[HALF:]
        stack = on_top(side_by_side(se[:, :HALF], so[:, :HALF]), side_by_side(se[:, HALF:], so[:, HALF:]))
        far[mode, parity] = on_rows(stack, tabs, which)


def backward_rows(mode, ratio, tabs, far):
    sums = []
    for parity, which in ((0, EVEN), (1, ODD)):
        scale = ratio[parity]
        sums.append(on_rows(far[mode, parity] * on_top(scale, scale), tabs, which))
    far[mode, 0] = sums[0] + sums[1]
    far[mode, 1] = sums[0] - sums[1]


def backward_lanes(half, probe, tabs, far, block):
    even = [side_by_side(far[mode, half, :HALF, :HALF], far[mode, half, HALF:, :HALF]) for mode in range(MODES)]
    odd = [side_by_side(far[mode, half, :HALF, HALF:], far[mode, half, HALF:, HALF:]) for mode in range(MODES)]
    pe = on_lanes(jnp.concatenate(even, axis=0), tabs, EVEN_T)
    po = on_lanes(jnp.concatenate(odd, axis=0), tabs, ODD_T)
    first, second = pe + po, pe - po
    where = slice(half * HALF, half * HALF + HALF)
    cr = ci = None
    for mode in range(MODES):
        part = slice(mode * HALF, mode * HALF + HALF)
        nr = side_by_side(first[part, :HALF], second[part, :HALF])
        ni = side_by_side(first[part, HALF:], second[part, HALF:])
        pr, pi = probe[0, mode, where], probe[1, mode, where]
        tr = pr * nr + pi * ni
        ti = pr * ni - pi * nr
        cr = tr if cr is None else cr + tr
        ci = ti if ci is None else ci + ti
    block[0, where] = cr
    block[1, where] = ci


def rows_from(ref, start, count):
    group = lax.shift_right_arithmetic(start, 3)
    wide = ref[pl.ds(group, count // 8 + 1)].reshape(count + 8, SIDE)
    return pltpu.roll(wide, lax.rem(count + 8 - (start - group * 8), count + 8), 0)[:count]


def inside(value):
    return jnp.clip(value, 0, SIDE - 1)


def grouped(value):
    return value.reshape(value.shape[0] // 8, 8, SIDE)


def sort_amplitudes(amp, tabs, ratio):
    rest = amp[...]
    total = None
    for _ in range(3):
        piece = rest.astype(BF16)
        rest = rest - piece.astype(F32)
        moved = dot(dot(tabs[ORDER_T], piece).astype(BF16), tabs[ORDER])
        total = moved if total is None else total + moved
    ratio[0] = total[:HALF]
    ratio[1] = total[HALF:]


def sum_power(probe, padded, share):
    power = None
    for mode in range(MODES):
        term = probe[0, mode] * probe[0, mode] + probe[1, mode] * probe[1, mode]
        power = term if power is None else power + term
    padded[pl.ds(0, 32)] = jnp.zeros((32, 8, SIDE), F32)
    padded[pl.ds(32, 32)] = grouped(power)
    padded[pl.ds(64, 33)] = jnp.zeros((33, 8, SIDE), F32)
    share[...] = jnp.zeros_like(share)


def cut_patch(row_at, col_at, ext, patch):
    lanes = lax.broadcasted_iota(jnp.int32, (SIDE, SIDE), 1)
    back = lax.rem(SIDE - col_at, SIDE)
    for plane in range(2):
        here = pltpu.roll(rows_from(ext.at[0, plane], row_at, SIDE), back, 1)
        there = pltpu.roll(rows_from(ext.at[1, plane], row_at, SIDE), back, 1)
        patch[plane] = jnp.where(lanes < SIDE - col_at, here, there)


def make_ratio(far, ratio):
    for parity in range(2):
        seen = None
        for mode in range(MODES):
            re, im = far[mode, parity, :HALF], far[mode, parity, HALF:]
            term = re * re + im * im
            seen = term if seen is None else seen + term
        ratio[parity] = ratio[parity] / (jnp.sqrt(seen) + SOFTEN)


TOGETHER = 4


def add_spots(me, group, spots, padded, share):
    up, left = group // 2, group % 2
    known = jnp.logical_and(me.row >= up, me.col >= left)
    first = up * SIDE + me.z * QUART + SIDE
    row_base = (me.row - up) * SIDE
    col_base = (me.col - left) * SIDE
    lanes = lax.broadcasted_iota(jnp.int32, (QUART, SIDE), 1)

    def some(index, carry):
        total = share[...]
        for step in range(TOGETHER):
            spot = group * 16 + index * TOGETHER + step
            start = jnp.where(known, first - inside(spots[spot, 0, 0] - row_base), 0)
            turn = jnp.where(known, inside(spots[spot, 0, 1] - col_base), 0)
            turned = pltpu.roll(rows_from(padded, start, QUART), turn, 1)
            kept = lanes >= turn if left == 0 else lanes < turn
            total = total + jnp.where(kept, turned, 0.0)
        share[...] = total
        return carry

    lax.fori_loop(0, 16 // TOGETHER, some, 0)


def put_tall(value, col_at, tall):
    lanes = lax.broadcasted_iota(jnp.int32, (SIDE, SIDE), 1)
    turned = pltpu.roll(value, col_at, 1)
    tall[0, pl.ds(32, 32)] = grouped(jnp.where(lanes >= col_at, turned, 0.0))
    tall[1, pl.ds(32, 32)] = grouped(jnp.where(lanes < col_at, turned, 0.0))


def whole_kernel(
    offsets, obj_hbm, probe_hbm, amp_hbm, tabs_hbm, out,
    ext, spots, spot_words, probe, amp, tabs, patch, far, ratio, block, padded, share,
    twin_block, tall, low_sum, low_in, right_sum, right_in, total, z_in, far_in,
    load_sem, word_sem,
    h_right_send, h_right_recv, h_share_send, h_share_recv, h_low_send, h_low_recv, h_diag_send, h_diag_recv,
    h_pair_send, h_pair_recv, spot_send, spot_recv,
    pair_send, pair_recv, low_send, low_recv, right_send, right_recv,
    z_send, z_recv, far_send, far_recv, out_send, out_recv, twin_send, twin_recv,
):
    me = Place()
    core = me.core
    loads = [
        pltpu.make_async_copy(obj_hbm.at[0], ext.at[0, 0, pl.ds(0, SIDE // 8)], load_sem.at[0]),
        pltpu.make_async_copy(obj_hbm.at[1], ext.at[0, 1, pl.ds(0, SIDE // 8)], load_sem.at[1]),
        pltpu.make_async_copy(tabs_hbm, tabs, load_sem.at[2]),
        pltpu.make_async_copy(amp_hbm, amp, load_sem.at[3]),
        pltpu.make_async_copy(probe_hbm, probe, load_sem.at[4]),
    ]
    for load in loads:
        load.start()
    lanes = lax.broadcasted_iota(jnp.int32, (1, 1, 128), 2)
    line = jnp.where(lanes == 0, offsets[0, 0], jnp.where(lanes == 1, offsets[0, 1], 0))
    spots[pl.ds(me.layer, 1)] = line
    me.meet()
    loads[0].wait()
    loads[1].wait()

    def meanwhile():
        loads[2].wait()
        loads[3].wait()
        sort_amplitudes(amp, tabs, ratio)
        for source in range(2):
            for side in range(2):
                tall[source, side, pl.ds(0, 32)] = jnp.zeros((32, 8, SIDE), F32)
                tall[source, side, pl.ds(64, 33)] = jnp.zeros((33, 8, SIDE), F32)
        loads[4].wait()
        sum_power(probe, padded, share)

    spots_go, near_words, other_words = spot_chain(me, spots, spot_words, spot_send, spot_recv, word_sem)
    spots_go(0)
    halo_sent = halo(me, ext, h_right_send, h_right_recv, h_share_send, h_share_recv, h_low_send, h_low_recv,
                     h_diag_send, h_diag_recv, h_pair_send, h_pair_recv, meanwhile, spots_go)
    spots_go(3)

    row_at = inside(offsets[0, 0] - me.row * SIDE)
    col_at = inside(offsets[0, 1] - me.col * SIDE)
    cut_patch(row_at, col_at, ext, patch)
    for mode in range(MODES):
        forward(mode, probe, patch, tabs, far)
    spots_go(4)
    make_ratio(far, ratio)
    for mode in range(MODES):
        backward_rows(mode, ratio, tabs, far)
    near_words.wait()
    twin_layer = me.layer + 1 - 2 * core
    twin_row = inside(spot_words[twin_layer, 0, 0] - me.row * SIDE)
    twin_col = inside(spot_words[twin_layer, 0, 1] - me.col * SIDE)

    def pair_copy(half):
        where = pl.ds(half * HALF, HALF)
        return remote(block.at[1 - core, where], twin_block.at[where],
                      pair_send.at[half], pair_recv.at[half], me.partner)

    for half in range(2):
        backward_lanes(half, probe, tabs, far, block)
        pair_copy(half).start()

    has_right = me.col < 3
    has_left = me.col > 0
    top = me.row == 0
    bottom = me.row == 1
    parts = [(me.z + 1 + step) % 4 for step in range(4)]

    def rows_at(step):
        return pl.ds(pl.multiple_of(parts[step // 2] * QUART + step % 2 * EIGHTH, EIGHTH), EIGHTH)

    def low_copy(side, step):
        where = rows_at(step) if side == 1 else rows_of(parts[step])
        return remote(low_sum.at[side, where], low_in.at[side, where],
                      low_send.at[side, step], low_recv.at[side, step], me.cross)

    def right_copy(step):
        where = rows_at(step)
        return remote(right_sum.at[where], right_in.at[where], right_send.at[step], right_recv.at[step], me.right)

    def z_copy(step):
        return remote(total.at[rows_at(step)], z_in.at[step], z_send.at[step], z_recv.at[step],
                      me.z_peer(step // 2 + 1))

    def far_copy(step):
        return remote(total.at[rows_at(step)], far_in.at[step], far_send.at[step], far_recv.at[step],
                      me.at(z=parts[step // 2], xh=1 - me.xh))

    put_tall(block[core], col_at, tall.at[0])
    for half in range(2):
        pair_copy(half).wait_recv()
    put_tall(twin_block[...], twin_col, tall.at[1])

    def both(side, first, count):
        return (rows_from(tall.at[0, side], SIDE + first - row_at, count)
                + rows_from(tall.at[1, side], SIDE + first - twin_row, count))

    def first_of(step):
        return parts[step // 2] * QUART + step % 2 * EIGHTH

    @pl.when(top)
    def _():
        for step in range(8):
            low_sum[1, rows_at(step)] = both(1, SIDE + first_of(step), EIGHTH)
            low_copy(1, step).start()

    for step in range(8):
        right_sum[rows_at(step)] = both(1, first_of(step), EIGHTH)

        @pl.when(jnp.logical_and(top, has_right))
        def _():
            right_copy(step).start()

    @pl.when(top)
    def _():
        for step in range(4):
            low_sum[0, rows_of(parts[step])] = both(0, SIDE + parts[step] * QUART, QUART)
            low_copy(0, step).start()

    for step in range(4):
        total[rows_of(parts[step])] = both(0, parts[step] * QUART, QUART)
    add_spots(me, 0, spot_words, padded, share)

    @pl.when(bottom)
    def _():
        for step in range(8):
            where = rows_at(step)
            low_copy(1, step).wait_recv()
            right_sum[where] = right_sum[where] + low_in[1, where]

            @pl.when(has_right)
            def _():
                right_copy(step).start()

    spots_go(5)
    other_words.wait()
    for group in range(1, 4):
        add_spots(me, group, spot_words, padded, share)

    for step in range(8):
        where = rows_at(step)
        if step % 2 == 0:
            @pl.when(bottom)
            def _():
                low_copy(0, step // 2).wait_recv()
                lower = rows_of(parts[step // 2])
                total[lower] = total[lower] + low_in[0, lower]

        @pl.when(has_left)
        def _():
            right_copy(step).wait_recv()
            total[where] = total[where] + right_in[where]

        far_copy(step).start()
        if step < 6:
            z_copy(step).start()

    def out_rows(part, half):
        return pl.ds(pl.multiple_of(part * QUART + half * EIGHTH, EIGHTH), EIGHTH)

    def out_copy(step, half):
        where = out.at[core, out_rows(me.z, half)]
        return remote(where, where, out_send.at[step, half], out_recv.at[step, half], me.z_peer(step + 1))

    def come_copy(step, half):
        where = out.at[core, out_rows((me.z + 3 - step) % 4, half)]
        return remote(where, where, out_send.at[step, half], out_recv.at[step, half], me.z_peer(step + 1))

    def twin_copy(step, half, plane):
        part = me.z if step == 3 else (me.z + 3 - step) % 4
        where = out.at[plane, out_rows(part, half)]
        return remote(where, where, twin_send.at[step, half], twin_recv.at[step, half], me.partner)

    for half in range(2):
        mine = out_rows(me.z, half)
        for step in range(3):
            z_copy(2 * step + half).wait_recv()
        near_sum = total[mine] + z_in[half] + z_in[2 + half] + z_in[4 + half]
        for step in range(4):
            far_copy(2 * step + half).wait_recv()
        far_sum = far_in[6 + half] + far_in[half] + far_in[2 + half] + far_in[4 + half]
        own = ext[0, core, pl.ds(me.z * 8 + half * 4, 4)].reshape(EIGHTH, SIDE)
        below = share[half * EIGHTH : half * EIGHTH + EIGHTH] + DAMPING
        out[core, mine] = (near_sum + far_sum + DAMPING * own) / below
        for step in (1, 0, 2):
            out_copy(step, half).start()
        twin_copy(3, half, core).start()

    for half in range(2):
        for step in (0, 2, 1):
            come_copy(step, half).wait_recv()
            twin_copy(step, half, core).start()
    for half in range(2):
        for step in (3, 0, 2, 1):
            twin_copy(step, half, 1 - core).wait_recv()

    for half in range(2):
        pair_copy(half).wait_send()
        for step in range(4):
            twin_copy(step, half, core).wait_send()
            if step < 3:
                out_copy(step, half).wait_send()
    for step in range(8):
        far_copy(step).wait_send()
        if step < 6:
            z_copy(step).wait_send()

        @pl.when(top)
        def _():
            low_copy(1, step).wait_send()
            if step < 4:
                low_copy(0, step).wait_send()

        @pl.when(has_right)
        def _():
            right_copy(step).wait_send()
    halo_sent()
    spots_go(6)


def body(object_field, probe_modes, amplitudes, offsets):
    sems = pltpu.SemaphoreType.DMA
    return pl.pallas_call(
        whole_kernel,
        out_shape=pltpu.VMEM((2, SIDE, SIDE), F32),
        in_specs=[SMEM_SPEC] + [HBM_SPEC] * 4,
        out_specs=VMEM_SPEC,
        scratch_shapes=[
            pltpu.VMEM((2, 2, 64, 8, SIDE), F32),
            pltpu.VMEM((64, 1, 128), jnp.int32),
            pltpu.SMEM((64, 1, 128), jnp.int32),
            pltpu.VMEM((2, MODES, SIDE, SIDE), F32),
            pltpu.VMEM((SIDE, SIDE), F32),
            pltpu.VMEM((10, SIDE, SIDE), BF16),
            pltpu.VMEM((2, SIDE, SIDE), F32),
            pltpu.VMEM((MODES, 2, SIDE, SIDE), F32),
            pltpu.VMEM((2, HALF, SIDE), F32),
            pltpu.VMEM((2, SIDE, SIDE), F32),
            pltpu.VMEM((97, 8, SIDE), F32),
            pltpu.VMEM((QUART, SIDE), F32),
            pltpu.VMEM((SIDE, SIDE), F32),
            pltpu.VMEM((2, 2, 97, 8, SIDE), F32),
            pltpu.VMEM((2, SIDE, SIDE), F32),
            pltpu.VMEM((2, SIDE, SIDE), F32),
            pltpu.VMEM((SIDE, SIDE), F32),
            pltpu.VMEM((SIDE, SIDE), F32),
            pltpu.VMEM((SIDE, SIDE), F32),
            pltpu.VMEM((6, EIGHTH, SIDE), F32),
            pltpu.VMEM((8, EIGHTH, SIDE), F32),
            sems((5,)), sems((2,)),
            sems((OWN,)), sems((OWN,)), sems((1,)), sems((1,)), sems((4,)), sems((4,)),
            sems((PIECES,)), sems((PIECES,)), sems((2 * PIECES + 4,)), sems((2 * PIECES + 4,)), sems((8,)), sems((8,)),
            sems((2,)), sems((2,)), sems((2, 8)), sems((2, 8)), sems((8,)), sems((8,)),
            sems((6,)), sems((6,)), sems((8,)), sems((8,)), sems((3, 2)), sems((3, 2)), sems((4, 2)), sems((4, 2)),
        ],
        compiler_params=pltpu.CompilerParams(
            collective_id=0, has_side_effects=True
        ),
        name="whole",
    )(offsets, object_field.reshape(2, 32, 8, SIDE), probe_modes, amplitudes[0], jnp.asarray(tables()))


def solution(mesh):
    placed = (
        P(None, "row", "col"),
        P(),
        P(("row", "col", "layer"), None, None),
        P(("row", "col", "layer"), None),
    )
    return jax.shard_map(
        body, mesh=mesh, in_specs=placed, out_specs=P(None, "row", "col"), check_vma=False
    )
```

```python
import functools
import math

import jax
import jax.numpy as jnp
import numpy as np
from jax import lax
from jax.experimental import pallas as pl
from jax.experimental.pallas import tpu as pltpu
from jax.sharding import PartitionSpec as P

SOFTEN = 0.05
DAMPING = 0.5
MODES = 4
SIDE = 256
HALF = 128
QUART = 64
EIGHTH = 32
F32 = jnp.float32
BF16 = jnp.bfloat16
VMEM_SPEC = pl.BlockSpec(memory_space=pltpu.VMEM)
SMEM_SPEC = pl.BlockSpec(memory_space=pltpu.SMEM)
HBM_SPEC = pl.BlockSpec(memory_space=pltpu.HBM)


def remote(src, dst, send, recv, device):
    return pltpu.make_async_remote_copy(
        src_ref=src,
        dst_ref=dst,
        send_sem=send,
        recv_sem=recv,
        device_id=device,
        device_id_type=pl.DeviceIdType.MESH,
    )


class Place:
    def __init__(self):
        self.row = lax.axis_index("row")
        self.col = lax.axis_index("col")
        layer = lax.axis_index("layer")
        self.layer = layer
        self.z = layer // 4
        self.xh = (layer // 2) % 2
        self.core = layer % 2
        self.partner = self.at(xh=self.xh, core=1 - self.core)
        self.far_x = self.at(xh=1 - self.xh)
        self.far_twin = self.at(xh=1 - self.xh, core=1 - self.core)
        self.cross_xh = (self.xh + self.core) % 2
        self.cross = {"row": 1 - self.row, "layer": self.z * 4 + self.cross_xh * 2 + self.core}
        self.left = {"col": (self.col + 3) % 4}
        self.right = {"col": (self.col + 1) % 4}

    def at(self, z=None, xh=None, core=None):
        z = self.z if z is None else z
        xh = self.xh if xh is None else xh
        core = self.core if core is None else core
        return {"layer": z * 4 + xh * 2 + core}

    def z_peer(self, step):
        return self.at(z=(self.z + step) % 4)

    def meet(self):
        barrier = pltpu.get_barrier_semaphore()
        others = [self.partner, self.far_x, self.far_twin, self.cross, self.left, self.right]
        others += [self.z_peer(step) for step in (1, 2, 3)]
        for other in others:
            pl.semaphore_signal(barrier, inc=1, device_id=other, device_id_type=pl.DeviceIdType.MESH)
        pl.semaphore_wait(barrier, len(others))


def rows_of(part, base=0):
    return pl.ds(pl.multiple_of(base + part * QUART, QUART), QUART)


def groups_of(part, base=0):
    return pl.ds(base // 8 + part * (QUART // 8), QUART // 8)


def tables():
    steps = np.arange(HALF)
    found = []
    for odd in (0, 1):
        phase = (steps[:, None] * (2 * steps[None, :] + odd)) % SIDE
        angle = phase * (2.0 * math.pi / SIDE)
        real, imag = np.cos(angle) / 16.0, -np.sin(angle) / 16.0
        full = np.block([[real, imag], [-imag, real]]).astype(np.float32)
        for table in (full, np.ascontiguousarray(full.T)):
            high = table.astype(jnp.bfloat16)
            low = (table - high.astype(np.float32)).astype(jnp.bfloat16)
            found += [high, low]
    order = np.zeros((SIDE, SIDE), np.float32)
    order[2 * steps, steps] = 1.0
    order[2 * steps + 1, HALF + steps] = 1.0
    found += [order.astype(jnp.bfloat16), np.ascontiguousarray(order.T).astype(jnp.bfloat16)]
    return np.stack(found)


EVEN, EVEN_T, ODD, ODD_T, ORDER, ORDER_T = 0, 2, 4, 6, 8, 9


def dot(left, right):
    return jnp.dot(left, right, preferred_element_type=F32)


def split(value):
    high = value.astype(BF16)
    return high, (value - high.astype(F32)).astype(BF16)


def on_lanes(value, tabs, which):
    high, low = split(value)
    return dot(high, tabs[which]) + dot(low, tabs[which]) + dot(high, tabs[which + 1])


def on_rows(value, tabs, which):
    high, low = split(value)
    return dot(tabs[which], high) + dot(tabs[which], low) + dot(tabs[which + 1], high)


def side_by_side(left, right):
    return jnp.concatenate([left, right], axis=1)


def on_top(upper, lower):
    return jnp.concatenate([upper, lower], axis=0)


OWN = 5
PIECES = 6
ORDER_IN = (0, 1, 2, 3, 4, 5)


def halo(me, ext, right_send, right_recv, share_send, share_recv, low_send, low_recv, diag_send, diag_recv,
         pair_send, pair_recv, meanwhile, spots_go):
    core = me.core
    has_right = me.col < 3
    has_left = me.col > 0
    top = me.row == 0
    bottom = me.row == 1

    odd = me.z % 2
    z_mate = me.at(z=me.z + 1 - 2 * odd)

    def piece(index, base=0):
        if index == 0:
            return pl.ds(base + odd * 6, 6)
        if index < OWN:
            return pl.ds(base + (0, 12, 20, 26, 30)[index], (0, 8, 6, 4, 2)[index])
        return pl.ds(base + (1 - odd) * 6, 6)

    def right_copy(index):
        return remote(ext.at[0, core, piece(index)], ext.at[1, core, piece(index)],
                      right_send.at[index], right_recv.at[index], me.left)

    def share_copy():
        where = ext.at[1, core, piece(0)]
        return remote(where, where, share_send.at[0], share_recv.at[0], z_mate)

    def low_copy(part):
        return remote(ext.at[0, core, groups_of(part)], ext.at[0, core, groups_of(part, SIDE)],
                      low_send.at[part], low_recv.at[part], me.cross)

    def diag_copy(index):
        return remote(ext.at[1, core, piece(index)], ext.at[1, core, piece(index, 32)],
                      diag_send.at[index], diag_recv.at[index], me.cross)

    def pair_copy(kind, index, plane):
        if kind == 1:
            where = ext.at[0, plane, groups_of(index, SIDE)]
        else:
            where = ext.at[1, plane, piece(index, 32 if kind == 2 else 0)]
        sem = (0, PIECES, PIECES + 4)[kind] + index
        return remote(where, where, pair_send.at[sem], pair_recv.at[sem], me.partner)

    @pl.when(has_left)
    def _():
        for index in range(OWN):
            right_copy(index).start()

    @pl.when(bottom)
    def _():
        for part in range(4):
            low_copy(part).start()

    meanwhile()

    def pass_on(index):
        @pl.when(bottom)
        def _():
            diag_copy(index).start()

        pair_copy(0, index, core).start()

    def low_here(part):
        @pl.when(top)
        def _():
            low_copy(part).wait_recv()
            pair_copy(1, part, core).start()

    @pl.when(has_right)
    def _():
        right_copy(0).wait_recv()
        share_copy().start()
        pass_on(0)

    low_here(0)
    low_here(1)

    @pl.when(has_right)
    def _():
        right_copy(1).wait_recv()
        pass_on(1)

    spots_go(2)
    low_here(2)
    low_here(3)

    @pl.when(has_right)
    def _():
        for index in ORDER_IN[2:]:
            if index < OWN:
                right_copy(index).wait_recv()
            else:
                share_copy().wait_recv()
            pass_on(index)

    @pl.when(jnp.logical_and(top, has_right))
    def _():
        for index in ORDER_IN:
            diag_copy(index).wait_recv()
            pair_copy(2, index, core).start()

    @pl.when(has_right)
    def _():
        for index in ORDER_IN:
            pair_copy(0, index, 1 - core).wait_recv()

    @pl.when(top)
    def _():
        for part in range(4):
            pair_copy(1, part, 1 - core).wait_recv()

        @pl.when(has_right)
        def _():
            for index in ORDER_IN:
                pair_copy(2, index, 1 - core).wait_recv()

    def all_sent():
        @pl.when(has_left)
        def _():
            for index in range(OWN):
                right_copy(index).wait_send()

        @pl.when(bottom)
        def _():
            for part in range(4):
                low_copy(part).wait_send()

            @pl.when(has_right)
            def _():
                for index in range(PIECES):
                    diag_copy(index).wait_send()

        @pl.when(has_right)
        def _():
            share_copy().wait_send()
            for index in range(PIECES):
                pair_copy(0, index, core).wait_send()

        @pl.when(top)
        def _():
            for part in range(4):
                pair_copy(1, part, core).wait_send()

            @pl.when(has_right)
            def _():
                for index in range(PIECES):
                    pair_copy(2, index, core).wait_send()

    return all_sent


def spot_chain(me, spots, spot_words, spot_send, spot_recv, word_sem):
    has_right = me.col < 3
    has_left = me.col > 0
    top = me.row == 0
    bottom = me.row == 1

    def spot_copy(step):
        if step in (0, 1, 7):
            where = pl.ds(me.layer, 1)
            other = {0: me.partner, 1: me.far_x, 7: me.far_twin}[step]
            return remote(spots.at[where], spots.at[where], spot_send.at[step], spot_recv.at[step], other)
        if step < 5:
            where = pl.ds(me.z * 4, 4)
            return remote(spots.at[where], spots.at[where], spot_send.at[step], spot_recv.at[step],
                          me.z_peer(step - 1))
        if step == 5:
            return remote(spots.at[pl.ds(0, 16)], spots.at[pl.ds(16, 16)], spot_send.at[5], spot_recv.at[5], me.right)
        return remote(spots.at[pl.ds(0, 32)], spots.at[pl.ds(32, 32)], spot_send.at[6], spot_recv.at[6], me.cross)

    near = pltpu.make_async_copy(spots.at[pl.ds(0, 16)], spot_words.at[pl.ds(0, 16)], word_sem.at[0])
    others = pltpu.make_async_copy(spots.at[pl.ds(16, 48)], spot_words.at[pl.ds(16, 48)], word_sem.at[1])

    def go(stage):
        if stage == 0:
            for step in (1, 7, 0):
                spot_copy(step).start()
        elif stage == 2:
            for step in (0, 1, 7):
                spot_copy(step).wait_recv()
            for step in (2, 3, 4):
                spot_copy(step).start()
        elif stage == 3:
            for step in (2, 3, 4):
                spot_copy(step).wait_recv()
            near.start()

            @pl.when(has_right)
            def _():
                spot_copy(5).start()
        elif stage == 4:
            @pl.when(has_left)
            def _():
                spot_copy(5).wait_recv()

            @pl.when(top)
            def _():
                spot_copy(6).start()
        elif stage == 5:
            @pl.when(bottom)
            def _():
                spot_copy(6).wait_recv()

            others.start()
        else:
            for step in (0, 1, 2, 3, 4, 7):
                spot_copy(step).wait_send()

            @pl.when(has_right)
            def _():
                spot_copy(5).wait_send()

            @pl.when(top)
            def _():
                spot_copy(6).wait_send()

    return go, near, others


def forward(mode, probe, patch, tabs, far):
    pr, pi = probe[0, mode], probe[1, mode]
    tr, ti = patch[0], patch[1]
    er = pr * tr - pi * ti
    ei = pr * ti + pi * tr
    even = side_by_side(er[:, :HALF] + er[:, HALF:], ei[:, :HALF] + ei[:, HALF:])
    odd = side_by_side(er[:, :HALF] - er[:, HALF:], ei[:, :HALF] - ei[:, HALF:])
    ye = on_lanes(even, tabs, EVEN)
    yo = on_lanes(odd, tabs, ODD)
    for parity, which in ((0, EVEN_T), (1, ODD_T)):
        if parity == 0:
            se, so = ye[:HALF] + ye[HALF:], yo[:HALF] + yo[HALF:]
        else:
            se, so = ye[:HALF] - ye[HALF:], yo[:HALF] - yo[HALF:]
        stack = on_top(side_by_side(se[:, :HALF], so[:, :HALF]), side_by_side(se[:, HALF:], so[:, HALF:]))
        far[mode, parity] = on_rows(stack, tabs, which)


def backward_rows(mode, ratio, tabs, far):
    sums = []
    for parity, which in ((0, EVEN), (1, ODD)):
        scale = ratio[parity]
        sums.append(on_rows(far[mode, parity] * on_top(scale, scale), tabs, which))
    far[mode, 0] = sums[0] + sums[1]
    far[mode, 1] = sums[0] - sums[1]


def backward_lanes(half, probe, tabs, far, block):
    even = [side_by_side(far[mode, half, :HALF, :HALF], far[mode, half, HALF:, :HALF]) for mode in range(MODES)]
    odd = [side_by_side(far[mode, half, :HALF, HALF:], far[mode, half, HALF:, HALF:]) for mode in range(MODES)]
    pe = on_lanes(jnp.concatenate(even, axis=0), tabs, EVEN_T)
    po = on_lanes(jnp.concatenate(odd, axis=0), tabs, ODD_T)
    first, second = pe + po, pe - po
    where = slice(half * HALF, half * HALF + HALF)
    cr = ci = None
    for mode in range(MODES):
        part = slice(mode * HALF, mode * HALF + HALF)
        nr = side_by_side(first[part, :HALF], second[part, :HALF])
        ni = side_by_side(first[part, HALF:], second[part, HALF:])
        pr, pi = probe[0, mode, where], probe[1, mode, where]
        tr = pr * nr + pi * ni
        ti = pr * ni - pi * nr
        cr = tr if cr is None else cr + tr
        ci = ti if ci is None else ci + ti
    block[0, where] = cr
    block[1, where] = ci


def rows_from(ref, start, count):
    group = lax.shift_right_arithmetic(start, 3)
    wide = ref[pl.ds(group, count // 8 + 1)].reshape(count + 8, SIDE)
    return pltpu.roll(wide, lax.rem(count + 8 - (start - group * 8), count + 8), 0)[:count]


def inside(value):
    return jnp.clip(value, 0, SIDE - 1)


def grouped(value):
    return value.reshape(value.shape[0] // 8, 8, SIDE)


def sort_amplitudes(amp, tabs, ratio):
    rest = amp[...]
    total = None
    for _ in range(3):
        piece = rest.astype(BF16)
        rest = rest - piece.astype(F32)
        moved = dot(dot(tabs[ORDER_T], piece).astype(BF16), tabs[ORDER])
        total = moved if total is None else total + moved
    ratio[0] = total[:HALF]
    ratio[1] = total[HALF:]


def sum_power(probe, padded, share):
    power = None
    for mode in range(MODES):
        term = probe[0, mode] * probe[0, mode] + probe[1, mode] * probe[1, mode]
        power = term if power is None else power + term
    padded[pl.ds(0, 32)] = jnp.zeros((32, 8, SIDE), F32)
    padded[pl.ds(32, 32)] = grouped(power)
    padded[pl.ds(64, 33)] = jnp.zeros((33, 8, SIDE), F32)
    share[...] = jnp.zeros_like(share)


def cut_patch(row_at, col_at, ext, patch):
    lanes = lax.broadcasted_iota(jnp.int32, (SIDE, SIDE), 1)
    back = lax.rem(SIDE - col_at, SIDE)
    for plane in range(2):
        here = pltpu.roll(rows_from(ext.at[0, plane], row_at, SIDE), back, 1)
        there = pltpu.roll(rows_from(ext.at[1, plane], row_at, SIDE), back, 1)
        patch[plane] = jnp.where(lanes < SIDE - col_at, here, there)


def make_ratio(far, ratio):
    for parity in range(2):
        seen = None
        for mode in range(MODES):
            re, im = far[mode, parity, :HALF], far[mode, parity, HALF:]
            term = re * re + im * im
            seen = term if seen is None else seen + term
        ratio[parity] = ratio[parity] / (jnp.sqrt(seen) + SOFTEN)


TOGETHER = 4


def add_spots(me, group, spots, padded, share):
    up, left = group // 2, group % 2
    known = jnp.logical_and(me.row >= up, me.col >= left)
    first = up * SIDE + me.z * QUART + me.xh * EIGHTH + SIDE
    row_base = (me.row - up) * SIDE
    col_base = (me.col - left) * SIDE
    lanes = lax.broadcasted_iota(jnp.int32, (EIGHTH, SIDE), 1)

    def some(index, carry):
        total = share[...]
        for step in range(TOGETHER):
            spot = group * 16 + index * TOGETHER + step
            start = jnp.where(known, first - inside(spots[spot, 0, 0] - row_base), 0)
            turn = jnp.where(known, inside(spots[spot, 0, 1] - col_base), 0)
            turned = pltpu.roll(rows_from(padded, start, EIGHTH), turn, 1)
            kept = lanes >= turn if left == 0 else lanes < turn
            total = total + jnp.where(kept, turned, 0.0)
        share[...] = total
        return carry

    lax.fori_loop(0, 16 // TOGETHER, some, 0)


def put_tall(value, col_at, tall):
    lanes = lax.broadcasted_iota(jnp.int32, (SIDE, SIDE), 1)
    turned = pltpu.roll(value, col_at, 1)
    tall[0, pl.ds(32, 32)] = grouped(jnp.where(lanes >= col_at, turned, 0.0))
    tall[1, pl.ds(32, 32)] = grouped(jnp.where(lanes < col_at, turned, 0.0))


def whole_kernel(
    offsets, obj_hbm, probe_hbm, amp_hbm, tabs_hbm, out,
    ext, spots, spot_words, probe, amp, tabs, patch, far, ratio, block, padded, share,
    twin_block, tall, low_sum, low_in, right_sum, right_in, total, z_in, far_in,
    load_sem, word_sem,
    h_right_send, h_right_recv, h_share_send, h_share_recv, h_low_send, h_low_recv, h_diag_send, h_diag_recv,
    h_pair_send, h_pair_recv, spot_send, spot_recv,
    pair_send, pair_recv, low_send, low_recv, right_send, right_recv,
    z_send, z_recv, far_send, far_recv, out_send, out_recv, twin_send, twin_recv,
):
    me = Place()
    core = me.core
    loads = [
        pltpu.make_async_copy(obj_hbm.at[0], ext.at[0, 0, pl.ds(0, SIDE // 8)], load_sem.at[0]),
        pltpu.make_async_copy(obj_hbm.at[1], ext.at[0, 1, pl.ds(0, SIDE // 8)], load_sem.at[1]),
        pltpu.make_async_copy(tabs_hbm, tabs, load_sem.at[2]),
        pltpu.make_async_copy(amp_hbm, amp, load_sem.at[3]),
        pltpu.make_async_copy(probe_hbm, probe, load_sem.at[4]),
    ]
    for load in loads:
        load.start()
    lanes = lax.broadcasted_iota(jnp.int32, (1, 1, 128), 2)
    line = jnp.where(lanes == 0, offsets[0, 0], jnp.where(lanes == 1, offsets[0, 1], 0))
    spots[pl.ds(me.layer, 1)] = line
    me.meet()
    loads[0].wait()
    loads[1].wait()

    def meanwhile():
        loads[2].wait()
        loads[3].wait()
        sort_amplitudes(amp, tabs, ratio)
        for source in range(2):
            for side in range(2):
                tall[source, side, pl.ds(0, 32)] = jnp.zeros((32, 8, SIDE), F32)
                tall[source, side, pl.ds(64, 33)] = jnp.zeros((33, 8, SIDE), F32)
        loads[4].wait()
        sum_power(probe, padded, share)

    spots_go, near_words, other_words = spot_chain(me, spots, spot_words, spot_send, spot_recv, word_sem)
    spots_go(0)
    halo_sent = halo(me, ext, h_right_send, h_right_recv, h_share_send, h_share_recv, h_low_send, h_low_recv,
                     h_diag_send, h_diag_recv, h_pair_send, h_pair_recv, meanwhile, spots_go)
    spots_go(3)

    row_at = inside(offsets[0, 0] - me.row * SIDE)
    col_at = inside(offsets[0, 1] - me.col * SIDE)
    cut_patch(row_at, col_at, ext, patch)
    for mode in range(MODES):
        forward(mode, probe, patch, tabs, far)
    spots_go(4)
    make_ratio(far, ratio)
    for mode in range(MODES):
        backward_rows(mode, ratio, tabs, far)
    near_words.wait()
    twin_layer = me.layer + 1 - 2 * core
    twin_row = inside(spot_words[twin_layer, 0, 0] - me.row * SIDE)
    twin_col = inside(spot_words[twin_layer, 0, 1] - me.col * SIDE)

    def pair_copy(half):
        where = pl.ds(half * HALF, HALF)
        return remote(block.at[1 - core, where], twin_block.at[where],
                      pair_send.at[half], pair_recv.at[half], me.partner)

    for half in range(2):
        backward_lanes(half, probe, tabs, far, block)
        pair_copy(half).start()

    has_right = me.col < 3
    has_left = me.col > 0
    top = me.row == 0
    bottom = me.row == 1
    parts = [(me.z + 1 + step) % 4 for step in range(4)]

    def unit(part, half):
        return pl.ds(pl.multiple_of(part * QUART + half * EIGHTH, EIGHTH), EIGHTH)

    def rows_at(step):
        return unit(parts[step // 2], step % 2)

    def low_copy(side, step):
        where = rows_at(step) if side == 1 else rows_of(parts[step])
        return remote(low_sum.at[side, where], low_in.at[side, where],
                      low_send.at[side, step], low_recv.at[side, step], me.cross)

    def right_copy(step):
        where = rows_at(step)
        return remote(right_sum.at[where], right_in.at[where], right_send.at[step], right_recv.at[step], me.right)

    def z_copy(step):
        return remote(total.at[unit(parts[step], me.xh)], z_in.at[step], z_send.at[step], z_recv.at[step],
                      me.z_peer(step + 1))

    def far_copy(step):
        return remote(total.at[unit(parts[step], 1 - me.xh)], far_in.at[step], far_send.at[step], far_recv.at[step],
                      me.at(z=parts[step], xh=1 - me.xh))

    put_tall(block[core], col_at, tall.at[0])
    for half in range(2):
        pair_copy(half).wait_recv()
    put_tall(twin_block[...], twin_col, tall.at[1])

    def both(side, first, count):
        return (rows_from(tall.at[0, side], SIDE + first - row_at, count)
                + rows_from(tall.at[1, side], SIDE + first - twin_row, count))

    def first_of(step):
        return parts[step // 2] * QUART + step % 2 * EIGHTH

    @pl.when(top)
    def _():
        for step in range(8):
            low_sum[1, rows_at(step)] = both(1, SIDE + first_of(step), EIGHTH)
            low_copy(1, step).start()

    for step in range(8):
        right_sum[rows_at(step)] = both(1, first_of(step), EIGHTH)

        @pl.when(jnp.logical_and(top, has_right))
        def _():
            right_copy(step).start()

    @pl.when(top)
    def _():
        for step in range(4):
            low_sum[0, rows_of(parts[step])] = both(0, SIDE + parts[step] * QUART, QUART)
            low_copy(0, step).start()

    for step in range(4):
        total[rows_of(parts[step])] = both(0, parts[step] * QUART, QUART)
    add_spots(me, 0, spot_words, padded, share)

    @pl.when(bottom)
    def _():
        for step in range(8):
            where = rows_at(step)
            low_copy(1, step).wait_recv()
            right_sum[where] = right_sum[where] + low_in[1, where]

            @pl.when(has_right)
            def _():
                right_copy(step).start()

    spots_go(5)
    other_words.wait()
    for group in range(1, 4):
        add_spots(me, group, spot_words, padded, share)

    for step in range(8):
        where = rows_at(step)
        if step % 2 == 0:
            @pl.when(bottom)
            def _():
                low_copy(0, step // 2).wait_recv()
                lower = rows_of(parts[step // 2])
                total[lower] = total[lower] + low_in[0, lower]

        @pl.when(has_left)
        def _():
            right_copy(step).wait_recv()
            total[where] = total[where] + right_in[where]

        @pl.when(me.xh != step % 2)
        def _():
            far_copy(step // 2).start()

        if step < 6:
            @pl.when(me.xh == step % 2)
            def _():
                z_copy(step // 2).start()

    def out_copy(index):
        where = out.at[core, unit(me.z, me.xh)]
        there = me.z_peer(index + 1) if index < 3 else me.at(z=(me.z + index - 3) % 4, xh=1 - me.xh)
        return remote(where, where, out_send.at[index], out_recv.at[index], there)

    def unit_of(index):
        if index < 3:
            return unit((me.z + 3 - index) % 4, me.xh)
        if index < 7:
            return unit((me.z + 7 - index) % 4, 1 - me.xh)
        return unit(me.z, me.xh)

    def twin_copy(index, plane):
        where = out.at[plane, unit_of(index)]
        return remote(where, where, twin_send.at[index], twin_recv.at[index], me.partner)

    mine = unit(me.z, me.xh)
    for step in range(3):
        z_copy(step).wait_recv()
    near_sum = total[mine] + z_in[0] + z_in[1] + z_in[2]
    for step in range(4):
        far_copy(step).wait_recv()
    far_sum = far_in[3] + far_in[0] + far_in[1] + far_in[2]
    own = ext[0, core, pl.ds(me.z * 8 + me.xh * 4, 4)].reshape(EIGHTH, SIDE)
    out[core, mine] = (near_sum + far_sum + DAMPING * own) / (share[...] + DAMPING)
    for index in (5, 4, 6, 3, 1, 0, 2):
        out_copy(index).start()
    twin_copy(7, core).start()
    for index in (0, 2, 1, 3, 4, 6, 5):
        out_copy(index).wait_recv()
        twin_copy(index, core).start()
    for index in (7, 0, 2, 1, 3, 4, 6, 5):
        twin_copy(index, 1 - core).wait_recv()

    for half in range(2):
        pair_copy(half).wait_send()
    for step in range(8):
        twin_copy(step, core).wait_send()
        if step < 7:
            out_copy(step).wait_send()
        if step < 4:
            far_copy(step).wait_send()
        if step < 3:
            z_copy(step).wait_send()

        @pl.when(top)
        def _():
            low_copy(1, step).wait_send()
            if step < 4:
                low_copy(0, step).wait_send()

        @pl.when(has_right)
        def _():
            right_copy(step).wait_send()
    halo_sent()
    spots_go(6)


def body(object_field, probe_modes, amplitudes, offsets):
    sems = pltpu.SemaphoreType.DMA
    return pl.pallas_call(
        whole_kernel,
        out_shape=pltpu.VMEM((2, SIDE, SIDE), F32),
        in_specs=[SMEM_SPEC] + [HBM_SPEC] * 4,
        out_specs=VMEM_SPEC,
        scratch_shapes=[
            pltpu.VMEM((2, 2, 64, 8, SIDE), F32),
            pltpu.VMEM((64, 1, 128), jnp.int32),
            pltpu.SMEM((64, 1, 128), jnp.int32),
            pltpu.VMEM((2, MODES, SIDE, SIDE), F32),
            pltpu.VMEM((SIDE, SIDE), F32),
            pltpu.VMEM((10, SIDE, SIDE), BF16),
            pltpu.VMEM((2, SIDE, SIDE), F32),
            pltpu.VMEM((MODES, 2, SIDE, SIDE), F32),
            pltpu.VMEM((2, HALF, SIDE), F32),
            pltpu.VMEM((2, SIDE, SIDE), F32),
            pltpu.VMEM((97, 8, SIDE), F32),
            pltpu.VMEM((EIGHTH, SIDE), F32),
            pltpu.VMEM((SIDE, SIDE), F32),
            pltpu.VMEM((2, 2, 97, 8, SIDE), F32),
            pltpu.VMEM((2, SIDE, SIDE), F32),
            pltpu.VMEM((2, SIDE, SIDE), F32),
            pltpu.VMEM((SIDE, SIDE), F32),
            pltpu.VMEM((SIDE, SIDE), F32),
            pltpu.VMEM((SIDE, SIDE), F32),
            pltpu.VMEM((3, EIGHTH, SIDE), F32),
            pltpu.VMEM((4, EIGHTH, SIDE), F32),
            sems((5,)), sems((2,)),
            sems((OWN,)), sems((OWN,)), sems((1,)), sems((1,)), sems((4,)), sems((4,)),
            sems((PIECES,)), sems((PIECES,)), sems((2 * PIECES + 4,)), sems((2 * PIECES + 4,)), sems((8,)), sems((8,)),
            sems((2,)), sems((2,)), sems((2, 8)), sems((2, 8)), sems((8,)), sems((8,)),
            sems((3,)), sems((3,)), sems((4,)), sems((4,)), sems((7,)), sems((7,)), sems((8,)), sems((8,)),
        ],
        compiler_params=pltpu.CompilerParams(
            collective_id=0, has_side_effects=True
        ),
        name="whole",
    )(offsets, object_field.reshape(2, 32, 8, SIDE), probe_modes, amplitudes[0], jnp.asarray(tables()))


def solution(mesh):
    placed = (
        P(None, "row", "col"),
        P(),
        P(("row", "col", "layer"), None, None),
        P(("row", "col", "layer"), None),
    )
    return jax.shard_map(
        body, mesh=mesh, in_specs=placed, out_specs=P(None, "row", "col"), check_vma=False
    )
```

```python
import functools
import math

import jax
import jax.numpy as jnp
import numpy as np
from jax import lax
from jax.experimental import pallas as pl
from jax.experimental.pallas import tpu as pltpu
from jax.sharding import PartitionSpec as P

SOFTEN = 0.05
DAMPING = 0.5
MODES = 4
SIDE = 256
HALF = 128
QUART = 64
EIGHTH = 32
F32 = jnp.float32
BF16 = jnp.bfloat16
VMEM_SPEC = pl.BlockSpec(memory_space=pltpu.VMEM)
SMEM_SPEC = pl.BlockSpec(memory_space=pltpu.SMEM)
HBM_SPEC = pl.BlockSpec(memory_space=pltpu.HBM)


def remote(src, dst, send, recv, device):
    return pltpu.make_async_remote_copy(
        src_ref=src,
        dst_ref=dst,
        send_sem=send,
        recv_sem=recv,
        device_id=device,
        device_id_type=pl.DeviceIdType.MESH,
    )


class Place:
    def __init__(self):
        self.row = lax.axis_index("row")
        self.col = lax.axis_index("col")
        layer = lax.axis_index("layer")
        self.layer = layer
        self.z = layer // 4
        self.xh = (layer // 2) % 2
        self.core = layer % 2
        self.partner = self.at(xh=self.xh, core=1 - self.core)
        self.far_x = self.at(xh=1 - self.xh)
        self.far_twin = self.at(xh=1 - self.xh, core=1 - self.core)
        self.cross_xh = (self.xh + self.core) % 2
        self.cross = {"row": 1 - self.row, "layer": self.z * 4 + self.cross_xh * 2 + self.core}
        self.left = {"col": (self.col + 3) % 4}
        self.right = {"col": (self.col + 1) % 4}

    def at(self, z=None, xh=None, core=None):
        z = self.z if z is None else z
        xh = self.xh if xh is None else xh
        core = self.core if core is None else core
        return {"layer": z * 4 + xh * 2 + core}

    def z_peer(self, step):
        return self.at(z=(self.z + step) % 4)

    def meet(self):
        barrier = pltpu.get_barrier_semaphore()
        others = [self.partner, self.far_x, self.far_twin, self.cross, self.left, self.right]
        others += [self.z_peer(step) for step in (1, 2, 3)]
        for other in others:
            pl.semaphore_signal(barrier, inc=1, device_id=other, device_id_type=pl.DeviceIdType.MESH)
        pl.semaphore_wait(barrier, len(others))


def rows_of(part, base=0):
    return pl.ds(pl.multiple_of(base + part * QUART, QUART), QUART)


def groups_of(part, base=0):
    return pl.ds(base // 8 + part * (QUART // 8), QUART // 8)


def tables():
    steps = np.arange(HALF)
    found = []
    for odd in (0, 1):
        phase = (steps[:, None] * (2 * steps[None, :] + odd)) % SIDE
        angle = phase * (2.0 * math.pi / SIDE)
        real, imag = np.cos(angle) / 16.0, -np.sin(angle) / 16.0
        full = np.block([[real, imag], [-imag, real]]).astype(np.float32)
        for table in (full, np.ascontiguousarray(full.T)):
            high = table.astype(jnp.bfloat16)
            low = (table - high.astype(np.float32)).astype(jnp.bfloat16)
            found += [high, low]
    order = np.zeros((SIDE, SIDE), np.float32)
    order[2 * steps, steps] = 1.0
    order[2 * steps + 1, HALF + steps] = 1.0
    found += [order.astype(jnp.bfloat16), np.ascontiguousarray(order.T).astype(jnp.bfloat16)]
    return np.stack(found)


EVEN, EVEN_T, ODD, ODD_T, ORDER, ORDER_T = 0, 2, 4, 6, 8, 9


def dot(left, right):
    return jnp.dot(left, right, preferred_element_type=F32)


def split(value):
    high = value.astype(BF16)
    return high, (value - high.astype(F32)).astype(BF16)


def on_lanes(value, tabs, which):
    high, low = split(value)
    return dot(high, tabs[which]) + dot(low, tabs[which]) + dot(high, tabs[which + 1])


def on_rows(value, tabs, which):
    high, low = split(value)
    return dot(tabs[which], high) + dot(tabs[which], low) + dot(tabs[which + 1], high)


def side_by_side(left, right):
    return jnp.concatenate([left, right], axis=1)


def on_top(upper, lower):
    return jnp.concatenate([upper, lower], axis=0)


OWN = 5
PIECES = 6
ORDER_IN = (0, 1, 2, 3, 4, 5)


def halo(me, ext, right_send, right_recv, share_send, share_recv, low_send, low_recv, diag_send, diag_recv,
         pair_send, pair_recv, meanwhile, spots_go):
    core = me.core
    has_right = me.col < 3
    has_left = me.col > 0
    top = me.row == 0
    bottom = me.row == 1

    odd = me.z % 2
    z_mate = me.at(z=me.z + 1 - 2 * odd)

    def piece(index, base=0):
        if index == 0:
            return pl.ds(base + odd * 5, 5)
        if index < OWN:
            return pl.ds(base + (0, 10, 18, 25, 29)[index], (0, 8, 7, 4, 3)[index])
        return pl.ds(base + (1 - odd) * 5, 5)

    def right_copy(index):
        return remote(ext.at[0, core, piece(index)], ext.at[1, core, piece(index)],
                      right_send.at[index], right_recv.at[index], me.left)

    def share_copy():
        where = ext.at[1, core, piece(0)]
        return remote(where, where, share_send.at[0], share_recv.at[0], z_mate)

    def low_copy(part):
        return remote(ext.at[0, core, groups_of(part)], ext.at[0, core, groups_of(part, SIDE)],
                      low_send.at[part], low_recv.at[part], me.cross)

    def diag_copy(index):
        return remote(ext.at[1, core, piece(index)], ext.at[1, core, piece(index, 32)],
                      diag_send.at[index], diag_recv.at[index], me.cross)

    def pair_copy(kind, index, plane):
        if kind == 1:
            where = ext.at[0, plane, groups_of(index, SIDE)]
        else:
            where = ext.at[1, plane, piece(index, 32 if kind == 2 else 0)]
        sem = (0, PIECES, PIECES + 4)[kind] + index
        return remote(where, where, pair_send.at[sem], pair_recv.at[sem], me.partner)

    @pl.when(has_left)
    def _():
        for index in range(OWN):
            right_copy(index).start()

    @pl.when(bottom)
    def _():
        for part in range(4):
            low_copy(part).start()

    meanwhile()

    def pass_on(index):
        @pl.when(bottom)
        def _():
            diag_copy(index).start()

        pair_copy(0, index, core).start()

    def low_here(part):
        @pl.when(top)
        def _():
            low_copy(part).wait_recv()
            pair_copy(1, part, core).start()

    @pl.when(has_right)
    def _():
        right_copy(0).wait_recv()
        share_copy().start()
        pass_on(0)

    low_here(0)
    low_here(1)

    @pl.when(has_right)
    def _():
        right_copy(1).wait_recv()
        pass_on(1)

    spots_go(2)
    low_here(2)
    low_here(3)

    @pl.when(has_right)
    def _():
        for index in ORDER_IN[2:]:
            if index < OWN:
                right_copy(index).wait_recv()
            else:
                share_copy().wait_recv()
            pass_on(index)

    @pl.when(jnp.logical_and(top, has_right))
    def _():
        for index in ORDER_IN:
            diag_copy(index).wait_recv()
            pair_copy(2, index, core).start()

    @pl.when(has_right)
    def _():
        for index in ORDER_IN:
            pair_copy(0, index, 1 - core).wait_recv()

    @pl.when(top)
    def _():
        for part in range(4):
            pair_copy(1, part, 1 - core).wait_recv()

        @pl.when(has_right)
        def _():
            for index in ORDER_IN:
                pair_copy(2, index, 1 - core).wait_recv()

    def all_sent():
        @pl.when(has_left)
        def _():
            for index in range(OWN):
                right_copy(index).wait_send()

        @pl.when(bottom)
        def _():
            for part in range(4):
                low_copy(part).wait_send()

            @pl.when(has_right)
            def _():
                for index in range(PIECES):
                    diag_copy(index).wait_send()

        @pl.when(has_right)
        def _():
            share_copy().wait_send()
            for index in range(PIECES):
                pair_copy(0, index, core).wait_send()

        @pl.when(top)
        def _():
            for part in range(4):
                pair_copy(1, part, core).wait_send()

            @pl.when(has_right)
            def _():
                for index in range(PIECES):
                    pair_copy(2, index, core).wait_send()

    return all_sent


def spot_chain(me, spots, spot_words, spot_send, spot_recv, word_sem):
    has_right = me.col < 3
    has_left = me.col > 0
    top = me.row == 0
    bottom = me.row == 1

    def spot_copy(step):
        if step in (0, 1, 7):
            where = pl.ds(me.layer, 1)
            other = {0: me.partner, 1: me.far_x, 7: me.far_twin}[step]
            return remote(spots.at[where], spots.at[where], spot_send.at[step], spot_recv.at[step], other)
        if step < 5:
            where = pl.ds(me.z * 4, 4)
            return remote(spots.at[where], spots.at[where], spot_send.at[step], spot_recv.at[step],
                          me.z_peer(step - 1))
        if step == 5:
            return remote(spots.at[pl.ds(0, 16)], spots.at[pl.ds(16, 16)], spot_send.at[5], spot_recv.at[5], me.right)
        return remote(spots.at[pl.ds(0, 32)], spots.at[pl.ds(32, 32)], spot_send.at[6], spot_recv.at[6], me.cross)

    near = pltpu.make_async_copy(spots.at[pl.ds(0, 16)], spot_words.at[pl.ds(0, 16)], word_sem.at[0])
    others = pltpu.make_async_copy(spots.at[pl.ds(16, 48)], spot_words.at[pl.ds(16, 48)], word_sem.at[1])

    def go(stage):
        if stage == 0:
            for step in (1, 7, 0):
                spot_copy(step).start()
        elif stage == 2:
            for step in (0, 1, 7):
                spot_copy(step).wait_recv()
            for step in (2, 3, 4):
                spot_copy(step).start()
        elif stage == 3:
            for step in (2, 3, 4):
                spot_copy(step).wait_recv()
            near.start()

            @pl.when(has_right)
            def _():
                spot_copy(5).start()
        elif stage == 4:
            @pl.when(has_left)
            def _():
                spot_copy(5).wait_recv()

            @pl.when(top)
            def _():
                spot_copy(6).start()
        elif stage == 5:
            @pl.when(bottom)
            def _():
                spot_copy(6).wait_recv()

            others.start()
        else:
            for step in (0, 1, 2, 3, 4, 7):
                spot_copy(step).wait_send()

            @pl.when(has_right)
            def _():
                spot_copy(5).wait_send()

            @pl.when(top)
            def _():
                spot_copy(6).wait_send()

    return go, near, others


def forward(mode, probe, patch, tabs, far):
    pr, pi = probe[0, mode], probe[1, mode]
    tr, ti = patch[0], patch[1]
    er = pr * tr - pi * ti
    ei = pr * ti + pi * tr
    even = side_by_side(er[:, :HALF] + er[:, HALF:], ei[:, :HALF] + ei[:, HALF:])
    odd = side_by_side(er[:, :HALF] - er[:, HALF:], ei[:, :HALF] - ei[:, HALF:])
    ye = on_lanes(even, tabs, EVEN)
    yo = on_lanes(odd, tabs, ODD)
    for parity, which in ((0, EVEN_T), (1, ODD_T)):
        if parity == 0:
            se, so = ye[:HALF] + ye[HALF:], yo[:HALF] + yo[HALF:]
        else:
            se, so = ye[:HALF] - ye[HALF:], yo[:HALF] - yo[HALF:]
        stack = on_top(side_by_side(se[:, :HALF], so[:, :HALF]), side_by_side(se[:, HALF:], so[:, HALF:]))
        far[mode, parity] = on_rows(stack, tabs, which)


def backward_rows(mode, ratio, tabs, far):
    sums = []
    for parity, which in ((0, EVEN), (1, ODD)):
        scale = ratio[parity]
        sums.append(on_rows(far[mode, parity] * on_top(scale, scale), tabs, which))
    far[mode, 0] = sums[0] + sums[1]
    far[mode, 1] = sums[0] - sums[1]


def backward_lanes(half, probe, tabs, far, block):
    even = [side_by_side(far[mode, half, :HALF, :HALF], far[mode, half, HALF:, :HALF]) for mode in range(MODES)]
    odd = [side_by_side(far[mode, half, :HALF, HALF:], far[mode, half, HALF:, HALF:]) for mode in range(MODES)]
    pe = on_lanes(jnp.concatenate(even, axis=0), tabs, EVEN_T)
    po = on_lanes(jnp.concatenate(odd, axis=0), tabs, ODD_T)
    first, second = pe + po, pe - po
    where = slice(half * HALF, half * HALF + HALF)
    cr = ci = None
    for mode in range(MODES):
        part = slice(mode * HALF, mode * HALF + HALF)
        nr = side_by_side(first[part, :HALF], second[part, :HALF])
        ni = side_by_side(first[part, HALF:], second[part, HALF:])
        pr, pi = probe[0, mode, where], probe[1, mode, where]
        tr = pr * nr + pi * ni
        ti = pr * ni - pi * nr
        cr = tr if cr is None else cr + tr
        ci = ti if ci is None else ci + ti
    block[0, where] = cr
    block[1, where] = ci


def rows_from(ref, start, count):
    group = lax.shift_right_arithmetic(start, 3)
    wide = ref[pl.ds(group, count // 8 + 1)].reshape(count + 8, SIDE)
    return pltpu.roll(wide, lax.rem(count + 8 - (start - group * 8), count + 8), 0)[:count]


def inside(value):
    return jnp.clip(value, 0, SIDE - 1)


def grouped(value):
    return value.reshape(value.shape[0] // 8, 8, SIDE)


def sort_amplitudes(amp, tabs, ratio):
    rest = amp[...]
    total = None
    for _ in range(3):
        piece = rest.astype(BF16)
        rest = rest - piece.astype(F32)
        moved = dot(dot(tabs[ORDER_T], piece).astype(BF16), tabs[ORDER])
        total = moved if total is None else total + moved
    ratio[0] = total[:HALF]
    ratio[1] = total[HALF:]


def sum_power(probe, padded, share):
    power = None
    for mode in range(MODES):
        term = probe[0, mode] * probe[0, mode] + probe[1, mode] * probe[1, mode]
        power = term if power is None else power + term
    padded[pl.ds(0, 32)] = jnp.zeros((32, 8, SIDE), F32)
    padded[pl.ds(32, 32)] = grouped(power)
    padded[pl.ds(64, 33)] = jnp.zeros((33, 8, SIDE), F32)
    share[...] = jnp.zeros_like(share)


def cut_patch(row_at, col_at, ext, patch):
    lanes = lax.broadcasted_iota(jnp.int32, (SIDE, SIDE), 1)
    back = lax.rem(SIDE - col_at, SIDE)
    for plane in range(2):
        here = pltpu.roll(rows_from(ext.at[0, plane], row_at, SIDE), back, 1)
        there = pltpu.roll(rows_from(ext.at[1, plane], row_at, SIDE), back, 1)
        patch[plane] = jnp.where(lanes < SIDE - col_at, here, there)


def make_ratio(far, ratio):
    for parity in range(2):
        seen = None
        for mode in range(MODES):
            re, im = far[mode, parity, :HALF], far[mode, parity, HALF:]
            term = re * re + im * im
            seen = term if seen is None else seen + term
        ratio[parity] = ratio[parity] / (jnp.sqrt(seen) + SOFTEN)


TOGETHER = 4


def add_spots(me, group, spots, padded, share):
    up, left = group // 2, group % 2
    known = jnp.logical_and(me.row >= up, me.col >= left)
    first = up * SIDE + me.z * QUART + me.xh * EIGHTH + SIDE
    row_base = (me.row - up) * SIDE
    col_base = (me.col - left) * SIDE
    lanes = lax.broadcasted_iota(jnp.int32, (EIGHTH, SIDE), 1)

    def some(index, carry):
        total = share[...]
        for step in range(TOGETHER):
            spot = group * 16 + index * TOGETHER + step
            start = jnp.where(known, first - inside(spots[spot, 0, 0] - row_base), 0)
            turn = jnp.where(known, inside(spots[spot, 0, 1] - col_base), 0)
            turned = pltpu.roll(rows_from(padded, start, EIGHTH), turn, 1)
            kept = lanes >= turn if left == 0 else lanes < turn
            total = total + jnp.where(kept, turned, 0.0)
        share[...] = total
        return carry

    lax.fori_loop(0, 16 // TOGETHER, some, 0)


def put_tall(value, col_at, tall):
    lanes = lax.broadcasted_iota(jnp.int32, (SIDE, SIDE), 1)
    turned = pltpu.roll(value, col_at, 1)
    tall[0, pl.ds(32, 32)] = grouped(jnp.where(lanes >= col_at, turned, 0.0))
    tall[1, pl.ds(32, 32)] = grouped(jnp.where(lanes < col_at, turned, 0.0))


def whole_kernel(
    offsets, obj_hbm, probe_hbm, amp_hbm, tabs_hbm, out,
    ext, spots, spot_words, probe, amp, tabs, patch, far, ratio, block, padded, share,
    twin_block, tall, low_sum, low_in, right_sum, right_in, total, z_in, far_in,
    load_sem, word_sem,
    h_right_send, h_right_recv, h_share_send, h_share_recv, h_low_send, h_low_recv, h_diag_send, h_diag_recv,
    h_pair_send, h_pair_recv, spot_send, spot_recv,
    pair_send, pair_recv, low_send, low_recv, right_send, right_recv,
    z_send, z_recv, far_send, far_recv, out_send, out_recv, twin_send, twin_recv,
):
    me = Place()
    core = me.core
    loads = [
        pltpu.make_async_copy(obj_hbm.at[0], ext.at[0, 0, pl.ds(0, SIDE // 8)], load_sem.at[0]),
        pltpu.make_async_copy(obj_hbm.at[1], ext.at[0, 1, pl.ds(0, SIDE // 8)], load_sem.at[1]),
        pltpu.make_async_copy(tabs_hbm, tabs, load_sem.at[2]),
        pltpu.make_async_copy(amp_hbm, amp, load_sem.at[3]),
        pltpu.make_async_copy(probe_hbm, probe, load_sem.at[4]),
    ]
    for load in loads:
        load.start()
    lanes = lax.broadcasted_iota(jnp.int32, (1, 1, 128), 2)
    line = jnp.where(lanes == 0, offsets[0, 0], jnp.where(lanes == 1, offsets[0, 1], 0))
    spots[pl.ds(me.layer, 1)] = line
    me.meet()
    loads[0].wait()
    loads[1].wait()

    def meanwhile():
        loads[2].wait()
        loads[3].wait()
        sort_amplitudes(amp, tabs, ratio)
        for source in range(2):
            for side in range(2):
                tall[source, side, pl.ds(0, 32)] = jnp.zeros((32, 8, SIDE), F32)
                tall[source, side, pl.ds(64, 33)] = jnp.zeros((33, 8, SIDE), F32)
        loads[4].wait()
        sum_power(probe, padded, share)

    spots_go, near_words, other_words = spot_chain(me, spots, spot_words, spot_send, spot_recv, word_sem)
    spots_go(0)
    halo_sent = halo(me, ext, h_right_send, h_right_recv, h_share_send, h_share_recv, h_low_send, h_low_recv,
                     h_diag_send, h_diag_recv, h_pair_send, h_pair_recv, meanwhile, spots_go)

    row_at = inside(offsets[0, 0] - me.row * SIDE)
    col_at = inside(offsets[0, 1] - me.col * SIDE)
    cut_patch(row_at, col_at, ext, patch)
    for mode in range(MODES):
        forward(mode, probe, patch, tabs, far)
    spots_go(3)
    make_ratio(far, ratio)
    spots_go(4)
    for mode in range(MODES):
        backward_rows(mode, ratio, tabs, far)
    near_words.wait()
    twin_layer = me.layer + 1 - 2 * core
    twin_row = inside(spot_words[twin_layer, 0, 0] - me.row * SIDE)
    twin_col = inside(spot_words[twin_layer, 0, 1] - me.col * SIDE)

    def pair_copy(half):
        where = pl.ds(half * HALF, HALF)
        return remote(block.at[1 - core, where], twin_block.at[where],
                      pair_send.at[half], pair_recv.at[half], me.partner)

    for half in range(2):
        backward_lanes(half, probe, tabs, far, block)
        pair_copy(half).start()

    has_right = me.col < 3
    has_left = me.col > 0
    top = me.row == 0
    bottom = me.row == 1
    parts = [(me.z + step) % 4 for step in (2, 1, 3, 0)]

    def unit(part, half):
        return pl.ds(pl.multiple_of(part * QUART + half * EIGHTH, EIGHTH), EIGHTH)

    def rows_at(step):
        return unit(parts[step // 2], step % 2)

    def low_copy(side, step):
        where = rows_at(step) if side == 1 else rows_of(parts[step])
        return remote(low_sum.at[side, where], low_in.at[side, where],
                      low_send.at[side, step], low_recv.at[side, step], me.cross)

    def right_copy(step):
        where = rows_at(step)
        return remote(right_sum.at[where], right_in.at[where], right_send.at[step], right_recv.at[step], me.right)

    def z_copy(step):
        return remote(total.at[unit(parts[step], me.xh)], z_in.at[step], z_send.at[step], z_recv.at[step],
                      me.at(z=parts[step]))

    def far_copy(step):
        return remote(total.at[unit(parts[step], 1 - me.xh)], far_in.at[step], far_send.at[step], far_recv.at[step],
                      me.at(z=parts[step], xh=1 - me.xh))

    put_tall(block[core], col_at, tall.at[0])
    for half in range(2):
        pair_copy(half).wait_recv()
    put_tall(twin_block[...], twin_col, tall.at[1])

    def both(side, first, count):
        return (rows_from(tall.at[0, side], SIDE + first - row_at, count)
                + rows_from(tall.at[1, side], SIDE + first - twin_row, count))

    def first_of(step):
        return parts[step // 2] * QUART + step % 2 * EIGHTH

    @pl.when(top)
    def _():
        for step in range(8):
            low_sum[1, rows_at(step)] = both(1, SIDE + first_of(step), EIGHTH)
            low_copy(1, step).start()

    for step in range(8):
        right_sum[rows_at(step)] = both(1, first_of(step), EIGHTH)

        @pl.when(jnp.logical_and(top, has_right))
        def _():
            right_copy(step).start()

    @pl.when(top)
    def _():
        for step in range(4):
            low_sum[0, rows_of(parts[step])] = both(0, SIDE + parts[step] * QUART, QUART)
            low_copy(0, step).start()

    for step in range(4):
        total[rows_of(parts[step])] = both(0, parts[step] * QUART, QUART)
    add_spots(me, 0, spot_words, padded, share)

    @pl.when(bottom)
    def _():
        for step in range(8):
            where = rows_at(step)
            low_copy(1, step).wait_recv()
            right_sum[where] = right_sum[where] + low_in[1, where]

            @pl.when(has_right)
            def _():
                right_copy(step).start()

    spots_go(5)
    other_words.wait()
    for group in range(1, 4):
        add_spots(me, group, spot_words, padded, share)

    for step in range(8):
        where = rows_at(step)
        if step % 2 == 0:
            @pl.when(bottom)
            def _():
                low_copy(0, step // 2).wait_recv()
                lower = rows_of(parts[step // 2])
                total[lower] = total[lower] + low_in[0, lower]

        @pl.when(has_left)
        def _():
            right_copy(step).wait_recv()
            total[where] = total[where] + right_in[where]

        @pl.when(me.xh != step % 2)
        def _():
            far_copy(step // 2).start()

        if step < 6:
            @pl.when(me.xh == step % 2)
            def _():
                z_copy(step // 2).start()

    def out_copy(index):
        where = out.at[core, unit(me.z, me.xh)]
        there = me.z_peer(index + 1) if index < 3 else me.at(z=(me.z + index - 3) % 4, xh=1 - me.xh)
        return remote(where, where, out_send.at[index], out_recv.at[index], there)

    def unit_of(index):
        if index < 3:
            return unit((me.z + 3 - index) % 4, me.xh)
        if index < 7:
            return unit((me.z + 7 - index) % 4, 1 - me.xh)
        return unit(me.z, me.xh)

    def twin_copy(index, plane):
        where = out.at[plane, unit_of(index)]
        return remote(where, where, twin_send.at[index], twin_recv.at[index], me.partner)

    mine = unit(me.z, me.xh)
    for step in range(3):
        z_copy(step).wait_recv()
    near_sum = total[mine] + z_in[0] + z_in[1] + z_in[2]
    for step in range(4):
        far_copy(step).wait_recv()
    far_sum = far_in[3] + far_in[0] + far_in[1] + far_in[2]
    own = ext[0, core, pl.ds(me.z * 8 + me.xh * 4, 4)].reshape(EIGHTH, SIDE)
    out[core, mine] = (near_sum + far_sum + DAMPING * own) / (share[...] + DAMPING)
    for index in (5, 4, 6, 3, 1, 0, 2):
        out_copy(index).start()
    twin_copy(7, core).start()
    for index in (0, 2, 1, 3, 4, 6, 5):
        out_copy(index).wait_recv()
        twin_copy(index, core).start()
    for index in (7, 0, 2, 1, 3, 4, 6, 5):
        twin_copy(index, 1 - core).wait_recv()

    for half in range(2):
        pair_copy(half).wait_send()
    for step in range(8):
        twin_copy(step, core).wait_send()
        if step < 7:
            out_copy(step).wait_send()
        if step < 4:
            far_copy(step).wait_send()
        if step < 3:
            z_copy(step).wait_send()

        @pl.when(top)
        def _():
            low_copy(1, step).wait_send()
            if step < 4:
                low_copy(0, step).wait_send()

        @pl.when(has_right)
        def _():
            right_copy(step).wait_send()
    halo_sent()
    spots_go(6)


def body(object_field, probe_modes, amplitudes, offsets):
    sems = pltpu.SemaphoreType.DMA
    return pl.pallas_call(
        whole_kernel,
        out_shape=pltpu.VMEM((2, SIDE, SIDE), F32),
        in_specs=[SMEM_SPEC] + [HBM_SPEC] * 4,
        out_specs=VMEM_SPEC,
        scratch_shapes=[
            pltpu.VMEM((2, 2, 64, 8, SIDE), F32),
            pltpu.VMEM((64, 1, 128), jnp.int32),
            pltpu.SMEM((64, 1, 128), jnp.int32),
            pltpu.VMEM((2, MODES, SIDE, SIDE), F32),
            pltpu.VMEM((SIDE, SIDE), F32),
            pltpu.VMEM((10, SIDE, SIDE), BF16),
            pltpu.VMEM((2, SIDE, SIDE), F32),
            pltpu.VMEM((MODES, 2, SIDE, SIDE), F32),
            pltpu.VMEM((2, HALF, SIDE), F32),
            pltpu.VMEM((2, SIDE, SIDE), F32),
            pltpu.VMEM((97, 8, SIDE), F32),
            pltpu.VMEM((EIGHTH, SIDE), F32),
            pltpu.VMEM((SIDE, SIDE), F32),
            pltpu.VMEM((2, 2, 97, 8, SIDE), F32),
            pltpu.VMEM((2, SIDE, SIDE), F32),
            pltpu.VMEM((2, SIDE, SIDE), F32),
            pltpu.VMEM((SIDE, SIDE), F32),
            pltpu.VMEM((SIDE, SIDE), F32),
            pltpu.VMEM((SIDE, SIDE), F32),
            pltpu.VMEM((3, EIGHTH, SIDE), F32),
            pltpu.VMEM((4, EIGHTH, SIDE), F32),
            sems((5,)), sems((2,)),
            sems((OWN,)), sems((OWN,)), sems((1,)), sems((1,)), sems((4,)), sems((4,)),
            sems((PIECES,)), sems((PIECES,)), sems((2 * PIECES + 4,)), sems((2 * PIECES + 4,)), sems((8,)), sems((8,)),
            sems((2,)), sems((2,)), sems((2, 8)), sems((2, 8)), sems((8,)), sems((8,)),
            sems((3,)), sems((3,)), sems((4,)), sems((4,)), sems((7,)), sems((7,)), sems((8,)), sems((8,)),
        ],
        compiler_params=pltpu.CompilerParams(
            collective_id=0, has_side_effects=True
        ),
        name="whole",
    )(offsets, object_field.reshape(2, 32, 8, SIDE), probe_modes, amplitudes[0], jnp.asarray(tables()))


def solution(mesh):
    placed = (
        P(None, "row", "col"),
        P(),
        P(("row", "col", "layer"), None, None),
        P(("row", "col", "layer"), None),
    )
    return jax.shard_map(
        body, mesh=mesh, in_specs=placed, out_specs=P(None, "row", "col"), check_vma=False
    )
```
